128 devices in a mesh: hi: 64 (over y_lo, x, z, core), grp: 2 (over y_hi).
Axes of the slice: x: 4, y: 4 (y_hi: 2, y_lo: 2; y = y_hi * 2 + y_lo), z: 4, core: 2. Of those that a mesh axis runs over, the one named last changes fastest.
Arguments:
- rho: float32 [2, 8192, 8192], P(None, ('hi', 'grp')), may hold values from -6 to 9
- perm: int32 [2, 13], replicated, may hold values from 0 to 12, each once within a row
- superop: float32 [2, 2, 16, 16], replicated, may hold values from -0.3 to 1.1
Outputs:
- rho_out: float32 [2, 8192, 8192], P(None, ('hi', 'grp'))
- trace_mean: float32 [], replicated
The draws below stay inside these ranges and needn't reach their ends.
All inputs are finite; a program needn't handle non-finite values.
Results may differ from the reference program's by a relative error of at most 0.0001.
Values sent between devices are 32-bit elements; how exact they have to be, the bound alone decides.
A program may use at most 256 MiB of HBM per device.

```python
import jax
import jax.numpy as jnp
from jax import lax

QUBITS = 13
ROWS = 8192
LAYERS = 2
PAIRS = 2


def draw_rho(key, part):
    noise = jnp.clip(jax.random.normal(key, (2, ROWS, ROWS), jnp.float32), -6.0, 6.0)
    ramp = 1.0 + 2.0 * jnp.arange(ROWS, dtype=jnp.float32) / ROWS
    diagonal = jnp.eye(ROWS, dtype=jnp.float32) * ramp[None, :]
    return noise.at[0].add(diagonal)


def draw_superop(key, part):
    noise = jnp.clip(0.06 * jax.random.normal(key, (LAYERS, 2, 16, 16), jnp.float32), -0.3, 0.3)
    return noise.at[:, 0].add(0.8 * jnp.eye(16, dtype=jnp.float32)[None])


def setup_inputs(seed: int = 0) -> dict:
    seeds = jax.random.split(jax.random.key(seed), 4)
    return {
        "rho": draw_rho(jax.random.fold_in(seeds[3], 71), 0),
        "perm": jax.vmap(lambda own: jax.random.permutation(own, QUBITS))(jax.random.split(seeds[1], LAYERS)).reshape((LAYERS, QUBITS)).astype(jnp.int32),
        "superop": draw_superop(jax.random.fold_in(seeds[3], 71), 0),
    }


def relabel_table(order, count):
    positions = jnp.arange(count, dtype=jnp.int32)
    result = jnp.zeros((count,), jnp.int32)
    for qubit in range(order.shape[0]):
        bit_value = jnp.bitwise_and(jnp.right_shift(positions, qubit), 1)
        result = result + bit_value * jnp.left_shift(jnp.int32(1), order[qubit].astype(jnp.int32))
    return result


def apply_channel(matrix, layer_super, pairs):
    real_part = layer_super[0]
    imag_part = layer_super[1]
    kernel = jnp.stack([jnp.stack([real_part, -imag_part], axis=1), jnp.stack([imag_part, real_part], axis=1)], axis=0)
    kernel = kernel.reshape(2, 4, 4, 2, 4, 4)
    row_count = matrix.shape[1]
    col_count = matrix.shape[2]
    for pair_idx in range(pairs):
        inner = 4 ** pair_idx
        shaped = matrix.reshape(2, row_count // (4 * inner), 4, inner, col_count // (4 * inner), 4, inner)
        shaped = jnp.einsum("ABCrst,rhsictj->AhBicCj", kernel, shaped, precision=lax.Precision.HIGHEST)
        matrix = shaped.reshape(2, row_count, col_count)
    return matrix


def reference(rho, perm, superop):
    matrix = rho
    for layer_idx in range(LAYERS):
        index_table = relabel_table(perm[layer_idx], ROWS)
        matrix = jnp.take(matrix, index_table, axis=1)
        matrix = jnp.take(matrix, index_table, axis=2)
        matrix = apply_channel(matrix, superop[layer_idx], PAIRS)
    trace_mean = jnp.trace(matrix[0]) / ROWS
    return matrix, trace_mean
```

```python
import functools

import jax
import jax.numpy as jnp
from jax import lax
from jax.experimental import pallas as pl
from jax.experimental.pallas import tpu as pltpu
from jax.sharding import Mesh
from jax.sharding import PartitionSpec as P

ROWS = 8192
QUBITS = 13
HI_GRP = ("hi", "grp")
F32 = jnp.float32
BF16 = jnp.bfloat16
SMEM = pltpu.SMEM
VMEM = pltpu.VMEM


def fill(table, weights):
    table[0] = jnp.int32(0)
    for k, weight in enumerate(weights):
        for j in range(1 << k):
            table[(1 << k) + j] = table[j] + weight


def one_shl(amount):
    return jnp.left_shift(jnp.int32(1), amount)


def column_order(perm, order):
    for j in range(4):
        order[j] = perm[0, j]
    count = jnp.int32(4)
    for q in range(QUBITS):
        order[count] = jnp.int32(q)
        mine = perm[0, 0] == q
        for j in range(1, 4):
            mine = mine | (perm[0, j] == q)
        count = count + jnp.where(mine, 0, 1)


def spread(perm, x, out, y, z0, z1, order, tc, te):
    column_order(perm, order)
    top = order[12]

    def weight(q):
        return one_shl(jnp.where(q < top, q, q - 1))

    fill(tc, [weight(order[i]) for i in range(6)])
    fill(te, [weight(order[6 + i]) for i in range(6)])
    step = one_shl(top - 7)

    @pl.loop(0, 32)
    def _(m):
        low = m & (step - 1)
        first = (m - low) * 2 + low
        for part in range(2):
            halves = [
                x[part, :, pl.ds(pl.multiple_of(t * 128, 128), 128)] for t in (first, first + step)
            ]
            start = pl.multiple_of(part * 4096 + m * 128, 128)
            y[pl.ds(start, 128), :] = jnp.concatenate(halves, axis=0).T

    @pl.loop(0, 32)
    def _(pair):
        for k, z in enumerate((z0, z1)):
            e = pair * 2 + k
            base = te[e]
            for c in range(64):
                row = base + tc[c]
                z[pl.ds(c, 1), :] = y[pl.ds(row, 1), :]
                z[pl.ds(64 + c, 1), :] = y[pl.ds(row + 4096, 1), :]
        for k, z in enumerate((z0, z1)):
            e = pair * 2 + k
            turned = z[...].T
            out[e] = turned[:64]
            out[64 + e] = turned[64:]


def split_bf16(value):
    high = value.astype(BF16)
    return high, (value - high.astype(F32)).astype(BF16)


def build_weights(sup, layer, pair, major_is_row, high_ref, low_ref):
    def uv(major, lane):
        minor = jnp.right_shift(lane, 2 * pair) & 3
        return 4 * major + minor if major_is_row else 4 * minor + major

    row = lax.broadcasted_iota(jnp.int32, (512, 16), 0)
    col16 = lax.broadcasted_iota(jnp.int32, (512, 16), 1)
    expand = jnp.where(uv(jnp.right_shift(row, 7), row & 127) == col16, 1.0, 0.0).astype(BF16)
    dims = (((1,), (1,)), ((), ()))
    lane_in = lax.broadcasted_iota(jnp.int32, (512, 128), 0) & 127
    lane_out = lax.broadcasted_iota(jnp.int32, (512, 128), 1)
    keep = 63 & ~(3 << (2 * pair))
    same_rest = (lane_in & keep) == (lane_out & keep)
    part_in = jnp.right_shift(lane_in, 6)
    part_out = jnp.right_shift(lane_out, 6)
    sign = jnp.where(part_out >= part_in, 1.0, -1.0).astype(F32)
    parts = [split_bf16(sup[layer, part]) for part in range(2)]
    for which, ref in enumerate((high_ref, low_ref)):
        half = [
            lax.dot_general(expand, parts[p][which], dims, preferred_element_type=F32).astype(BF16)
            for p in range(2)
        ]
        for block in range(4):
            target = expand[block * 128 : (block + 1) * 128]
            real, imag = (
                lax.dot_general(h, target, dims, preferred_element_type=F32) for h in half
            )
            value = jnp.where(part_in == part_out, real, sign * imag)
            ref[:, block * 128 : (block + 1) * 128] = jnp.where(same_rest, value, 0.0).astype(BF16)


def apply_pair(z, pair, high_ref, low_ref, rows=128):
    steps = 512 // rows

    @pl.loop(0, 4 * steps)
    def _(i):
        other = i // steps
        chunk = i % steps
        first = other * 4 if pair == 0 else other
        stride = 1 if pair == 0 else 4
        places = [
            pl.ds(pl.multiple_of((first + stride * k) * 512 + chunk * rows, rows), rows)
            for k in range(4)
        ]
        value = jnp.concatenate([z[place, :] for place in places], axis=1)
        high, low = split_bf16(value)
        mixed = jnp.dot(high, high_ref[...], preferred_element_type=F32)
        mixed += jnp.dot(low, high_ref[...], preferred_element_type=F32)
        mixed += jnp.dot(high, low_ref[...], preferred_element_type=F32)
        for k, place in enumerate(places):
            z[place, :] = mixed[:, k * 128 : (k + 1) * 128]


def channel(sup, layer, major_is_row, z, high_ref, low_ref):
    for pair in range(2):
        build_weights(sup, layer, pair, major_is_row, high_ref, low_ref)
        apply_pair(z, pair, high_ref, low_ref)


def middle(perm, sup, x, out, z, high, low, inv, rest, ta, tl, th, da, dl, dh):
    count = jnp.int32(0)
    for q in range(QUBITS):
        source = perm[1, q]
        inv[source] = jnp.int32(q)
        rest[count] = jnp.int32(q)
        count = count + jnp.where(source >= 4, 1, 0)
    first_row = [one_shl(perm[0, perm[1, rest[j]]]) for j in range(9)]
    fill(ta, [one_shl(perm[0, j]) for j in range(4)])
    fill(tl, first_row[:5])
    fill(th, first_row[5:])
    fill(da, [one_shl(inv[j]) for j in range(4)])
    fill(dl, [one_shl(rest[j]) for j in range(5)])
    fill(dh, [one_shl(rest[5 + j]) for j in range(4)])

    @pl.loop(0, 256)
    def _(i):
        base = ta[i // 16] + th[i % 16]
        place = pl.multiple_of(i * 32, 32)
        for k in range(32):
            z[pl.ds(place + k, 1), :] = x[pl.ds(base + tl[k], 1), :]

    channel(sup, 0, True, z, high, low)

    @pl.loop(0, 256)
    def _(i):
        base = da[i // 16] + dh[i % 16]
        place = pl.multiple_of(i * 32, 32)
        for k in range(32):
            out[pl.ds(base + dl[k], 1), :] = z[pl.ds(place + k, 1), :]


def gather_back(perm, sup, where, x, out, trace, y, z, b0, b1, high, low, order, inv, ta, tl, th):
    column_order(perm, order)
    for i in range(QUBITS):
        inv[order[i]] = jnp.int32(i)
    weights = [one_shl(inv[perm[0, perm[1, q]]]) for q in range(QUBITS)]
    fill(ta, weights[:4])
    fill(tl, weights[4:9])
    fill(th, weights[9:])

    @pl.loop(0, 64)
    def _(p):
        turned = jnp.concatenate([x[p], x[p + 64]], axis=0).T
        real, imag = turned[:64], turned[64:]
        start = pl.multiple_of(p * 64, 64)
        y[pl.ds(start, 64), :] = jnp.concatenate([real[:, :64], imag[:, :64]], axis=1)
        y[pl.ds(start + 4096, 64), :] = jnp.concatenate([real[:, 64:], imag[:, 64:]], axis=1)

    @pl.loop(0, 256)
    def _(i):
        base = ta[i // 16] + th[i % 16]
        place = pl.multiple_of(i * 32, 32)
        for k in range(32):
            z[pl.ds(place + k, 1), :] = y[pl.ds(base + tl[k], 1), :]

    channel(sup, 1, False, z, high, low)

    @pl.loop(0, 32)
    def _(pair):
        for k, b in enumerate((b0, b1)):
            t = pair * 2 + k
            for low_bits in range(16):
                b[pl.ds(low_bits, 8, stride=16), :] = z[
                    pl.ds(pl.multiple_of(low_bits * 512 + t * 8, 8), 8), :
                ]
        for k, b in enumerate((b0, b1)):
            lanes = pl.ds(pl.multiple_of((pair * 2 + k) * 128, 128), 128)
            turned = b[...].T
            out[0, :, lanes] = turned[:64]
            out[1, :, lanes] = turned[64:]

    me = where[0]
    block = out[0, :, pl.ds(pl.multiple_of((me // 2) * 128, 128), 128)]
    lane = lax.broadcasted_iota(jnp.int32, (64, 128), 1)
    row = lax.broadcasted_iota(jnp.int32, (64, 128), 0)
    kept = jnp.where(lane == row + (me % 2) * 64, block, 0.0)
    trace[...] = jnp.sum(kept, axis=0, keepdims=True)


def call(body, outs, n_smem, n_vmem, scratch, args):
    smem = pl.BlockSpec(memory_space=SMEM)
    vmem = pl.BlockSpec(memory_space=VMEM)
    kinds = [smem if i in n_smem else vmem for i in range(n_vmem)]
    return pl.pallas_call(
        body,
        out_shape=outs,
        in_specs=kinds,
        out_specs=jax.tree.map(lambda _: vmem, outs),
        scratch_shapes=scratch,
        compiler_params=pltpu.CompilerParams(vmem_limit_bytes=60 * 2**20),
    )(*args)


def table(*sizes):
    return [SMEM((n,), jnp.int32) for n in sizes]


def spread_call(perm, x):
    return call(
        spread, jax.ShapeDtypeStruct((128, 64, 128), F32), (0,), 2,
        [VMEM((8192, 128), F32), VMEM((128, 128), F32), VMEM((128, 128), F32)] + table(14, 64, 64),
        (perm, x),
    )


def middle_call(perm, sup, x):
    return call(
        middle, jax.ShapeDtypeStruct((8192, 128), F32), (0,), 3,
        [VMEM((8192, 128), F32), VMEM((512, 512), BF16), VMEM((512, 512), BF16)]
        + table(13, 14, 16, 32, 16, 16, 32, 16),
        (perm, sup, x),
    )


def back_call(perm, sup, where, x):
    return call(
        gather_back,
        (jax.ShapeDtypeStruct((2, 64, 8192), F32), jax.ShapeDtypeStruct((1, 128), F32)),
        (0, 2), 4,
        [VMEM((8192, 128), F32), VMEM((8192, 128), F32), VMEM((128, 128), F32), VMEM((128, 128), F32),
         VMEM((512, 512), BF16), VMEM((512, 512), BF16)]
        + table(14, 13, 16, 32, 16),
        (perm, sup, where, x),
    )


def exchange(value):
    return lax.all_to_all(value, HI_GRP, split_axis=0, concat_axis=0, tiled=True)


def per_device(rho, perm, superop):
    sent = spread_call(perm, rho)
    mid = middle_call(perm, superop, exchange(sent).reshape(8192, 128))
    where = lax.axis_index(HI_GRP).astype(jnp.int32).reshape(1)
    matrix, trace = back_call(perm, superop, where, exchange(mid.reshape(128, 64, 128)))
    return matrix, lax.psum(jnp.sum(trace), HI_GRP) / ROWS


def solution(mesh):
    in_specs = (P(None, HI_GRP, None), P(), P())
    out_specs = (P(None, HI_GRP, None), P())
    return jax.shard_map(
        per_device, mesh=mesh, in_specs=in_specs, out_specs=out_specs, check_vma=False
    )
```

```python
import functools

import jax
import jax.numpy as jnp
from jax import lax
from jax.experimental import pallas as pl
from jax.experimental.pallas import tpu as pltpu
from jax.sharding import Mesh
from jax.sharding import PartitionSpec as P

ROWS = 8192
QUBITS = 13
HI_GRP = ("hi", "grp")
F32 = jnp.float32
BF16 = jnp.bfloat16
SMEM = pltpu.SMEM
VMEM = pltpu.VMEM


def fill(table, weights):
    table[0] = jnp.int32(0)
    for k, weight in enumerate(weights):
        for j in range(1 << k):
            table[(1 << k) + j] = table[j] + weight


def one_shl(amount):
    return jnp.left_shift(jnp.int32(1), amount)


def column_order(perm, order):
    for j in range(4):
        order[j] = perm[0, j]
    count = jnp.int32(4)
    for q in range(QUBITS):
        order[count] = jnp.int32(q)
        mine = perm[0, 0] == q
        for j in range(1, 4):
            mine = mine | (perm[0, j] == q)
        count = count + jnp.where(mine, 0, 1)


def tile_at(vreg):
    return pl.ds(pl.multiple_of(vreg * 8, 8), 8)


def insert_zero(index, bit):
    low = index & (one_shl(bit) - 1)
    return (index - low) * 2 + low


def swap_stage(buf, sub, bit, unroll=8):
    step = 1 << sub
    keep = (lax.broadcasted_iota(jnp.int32, (8, 128), 0) & step) == 0

    @pl.loop(0, 512 // unroll)
    def _(i):
        pairs = []
        for k in range(unroll):
            v = insert_zero(i * unroll + k, bit)
            w = v + one_shl(bit)
            pairs.append((v, w, buf[tile_at(v), :], buf[tile_at(w), :]))
        for v, w, a, b in pairs:
            buf[tile_at(v), :] = jnp.where(keep, a, pltpu.roll(b, step, 0))
            buf[tile_at(w), :] = jnp.where(keep, pltpu.roll(a, 8 - step, 0), b)


def exchange_bits(buf, loc, occ, sub, place):
    swap_stage(buf, sub, place - 3)
    here, there = occ[sub], occ[place]
    occ[sub] = there
    occ[place] = here
    loc[there] = jnp.int32(sub)
    loc[here] = place


def settle_sublanes(buf, loc, occ, wanted, bits):
    for sub in range(3):
        best = jnp.int32(-1)
        for bit in bits:
            best = jnp.where(wanted(bit) & (loc[bit] >= 3), loc[bit], best)

        @pl.when(jnp.logical_not(wanted(occ[sub])) & (best >= 3))
        def _():
            exchange_bits(buf, loc, occ, sub, best)


def spread(perm, x, out, lanes, y, order, loc, occ, tc, te):
    column_order(perm, order)
    top = order[12]
    for q in range(QUBITS):
        place = jnp.where(jnp.int32(q) < top, q, q - 1)
        loc[q] = jnp.where(jnp.int32(q) == top, jnp.int32(13), place)
        occ[place] = jnp.int32(q)
    for q in range(QUBITS):

        @pl.when(jnp.int32(q) != top)
        def _():
            occ[loc[q]] = jnp.int32(q)

    step = one_shl(top - 7)

    @pl.loop(0, 16)
    def _(pair):
        for k in range(2):
            m = pair * 2 + k
            first = insert_zero(m, top - 7)
            for part in range(2):
                halves = [
                    x[part, :, pl.ds(pl.multiple_of(t * 128, 128), 128)]
                    for t in (first, first + step)
                ]
                start = pl.multiple_of(part * 4096 + m * 128, 128)
                y[pl.ds(start, 128), :] = jnp.concatenate(halves, axis=0).T

    def local(bit):
        found = bit == order[0]
        for i in range(1, 6):
            found = found | (bit == order[i])
        return found

    settle_sublanes(y, loc, occ, local, [order[i] for i in range(6)])
    for s in range(3):
        found = jnp.int32(0)
        for i in range(6):
            found = jnp.where(order[i] == occ[s], i, found)
        lanes[s] = found
    count = jnp.int32(3)
    for i in range(6):
        lanes[count] = jnp.int32(i)
        count = count + jnp.where(loc[order[i]] >= 3, 1, 0)
    fill(tc, [one_shl(loc[order[lanes[3 + i]]] - 3) for i in range(3)])
    fill(te, [one_shl(loc[order[6 + i]] - 3) for i in range(6)])

    @pl.loop(0, 16)
    def _(group):
        for k in range(4):
            e = group * 4 + k
            base = te[e]
            tiles = [y[tile_at(base + tc[j] + part * 512), :] for part in range(2) for j in range(8)]
            turned = jnp.concatenate(tiles, axis=0).T
            out[e] = turned[:64]
            out[64 + e] = turned[64:]


def split_bf16(value):
    high = value.astype(BF16)
    return high, (value - high.astype(F32)).astype(BF16)


def build_weights(sup, layer, pair, major_is_row, lanes, high_ref, low_ref):
    def canonical(lane):
        if lanes is None:
            return lane & 63
        total = jnp.zeros_like(lane)
        for k in range(6):
            total = total + jnp.left_shift(jnp.right_shift(lane, k) & 1, lanes[k])
        return total

    def uv(major, lane):
        minor = jnp.right_shift(lane, 2 * pair) & 3
        return 4 * major + minor if major_is_row else 4 * minor + major

    row = lax.broadcasted_iota(jnp.int32, (512, 16), 0)
    col16 = lax.broadcasted_iota(jnp.int32, (512, 16), 1)

    def one_hot(lane):
        hit = uv(jnp.right_shift(row, 7), lane) == col16
        return jnp.where(hit, 1.0, 0.0).astype(BF16)

    expand_out = one_hot(row & 63)
    expand_in = expand_out if lanes is None else one_hot(canonical(row))
    dims = (((1,), (1,)), ((), ()))
    raw_in = lax.broadcasted_iota(jnp.int32, (512, 128), 0) & 127
    lane_in = canonical(raw_in)
    raw_out = lax.broadcasted_iota(jnp.int32, (512, 128), 1)
    keep = 63 & ~(3 << (2 * pair))
    same_rest = (lane_in & keep) == (raw_out & keep)
    part_in = jnp.right_shift(raw_in, 6)
    part_out = jnp.right_shift(raw_out, 6)
    sign = jnp.where(part_out >= part_in, 1.0, -1.0).astype(F32)
    parts = [split_bf16(sup[layer, part]) for part in range(2)]
    for which, ref in enumerate((high_ref, low_ref)):
        half = [
            lax.dot_general(expand_in, parts[p][which], dims, preferred_element_type=F32).astype(BF16)
            for p in range(2)
        ]
        for block in range(4):
            target = expand_out[block * 128 : (block + 1) * 128]
            real, imag = (
                lax.dot_general(h, target, dims, preferred_element_type=F32) for h in half
            )
            value = jnp.where(part_in == part_out, real, sign * imag)
            ref[:, block * 128 : (block + 1) * 128] = jnp.where(same_rest, value, 0.0).astype(BF16)


def apply_pair(z, pair, ta, rv, xh, xl, mixed, high_ref, low_ref):
    @pl.loop(0, 4)
    def _(other):
        first = other * 4 if pair == 0 else other
        stride = 1 if pair == 0 else 4
        bases = [ta[first + stride * k] for k in range(4)]

        @pl.loop(0, 16)
        def _(r):
            for half in range(2):
                v0 = rv[r * 4 + half * 2]
                v1 = rv[r * 4 + half * 2 + 1]
                rows = pl.ds(pl.multiple_of(r * 32 + half * 16, 16), 16)
                for k in range(4):
                    both = [z[tile_at(bases[k] + v), :] for v in (v0, v1)]
                    high, low = split_bf16(jnp.concatenate(both, axis=0))
                    xh[rows, k * 128 : (k + 1) * 128] = high
                    xl[rows, k * 128 : (k + 1) * 128] = low

        total = jnp.dot(xh[...], high_ref[...], preferred_element_type=F32)
        total += jnp.dot(xl[...], high_ref[...], preferred_element_type=F32)
        total += jnp.dot(xh[...], low_ref[...], preferred_element_type=F32)
        mixed[...] = total

        @pl.loop(0, 16)
        def _(r):
            for j in range(4):
                v = rv[r * 4 + j]
                rows = pl.ds(pl.multiple_of(r * 32 + j * 8, 8), 8)
                for k in range(4):
                    z[tile_at(bases[k] + v), :] = mixed[rows, k * 128 : (k + 1) * 128]


def channel(sup, layer, major_is_row, lanes, z, ta, rv, xh, xl, mixed, high_ref, low_ref):
    for pair in range(2):
        build_weights(sup, layer, pair, major_is_row, lanes if pair == 0 else None, high_ref, low_ref)
        apply_pair(z, pair, ta, rv, xh, xl, mixed, high_ref, low_ref)


def middle(perm, lanes, sup, x, out, rows_out, z, xh, xl, mixed, high, low,
           final, outpos, loc, occ, rest, ta, rv, ti, td):
    for q in range(QUBITS):
        bit = perm[0, perm[1, q]]
        final[q] = bit
        outpos[bit] = jnp.int32(q)
        loc[q] = jnp.int32(q)
        occ[q] = jnp.int32(q)
    z[...] = x[...]
    mixes = [perm[0, j] for j in range(4)]

    def mixed_bit(bit):
        found = bit == mixes[0]
        for m in mixes[1:]:
            found = found | (bit == m)
        return found

    everything = [jnp.int32(q) for q in range(QUBITS)]
    stays = lambda bit: outpos[bit] < 6
    settle_sublanes(z, loc, occ, lambda bit: jnp.logical_not(mixed_bit(bit)) & stays(bit), everything)
    settle_sublanes(z, loc, occ, lambda bit: jnp.logical_not(mixed_bit(bit)), everything)
    count = jnp.int32(0)
    for place in range(3, QUBITS):
        rest[count] = jnp.int32(place)
        count = count + jnp.where(mixed_bit(occ[place]), 0, 1)
    fill(ta, [one_shl(loc[m] - 3) for m in mixes])
    fill(rv, [one_shl(rest[j] - 3) for j in range(6)])
    channel(sup, 0, True, lanes, z, ta, rv, xh, xl, mixed, high, low)
    settle_sublanes(z, loc, occ, stays, everything)
    for s in range(3):
        rows_out[s] = outpos[occ[s]]
    count = jnp.int32(3)
    for q in range(6):
        rows_out[count] = jnp.int32(q)
        count = count + jnp.where(loc[final[q]] >= 3, 1, 0)
    fill(ti, [one_shl(loc[final[rows_out[3 + i]]] - 3) for i in range(3)])
    fill(td, [one_shl(loc[final[6 + i]] - 3) for i in range(7)])

    @pl.loop(0, 64)
    def _(i):
        for k in range(2):
            d = i * 2 + k
            base = td[d]
            for j in range(8):
                out[tile_at(d * 8 + j), :] = z[tile_at(base + ti[j]), :]


def gather_back(perm, lanes, where, sup, x, out, trace, y, b0, b1, xh, xl, mixed, high, low,
                order, inv, loc, occ, ta, rv):
    column_order(perm, order)
    for i in range(QUBITS):
        inv[order[i]] = jnp.int32(i)
    for q in range(QUBITS):
        place = inv[perm[0, perm[1, q]]]
        loc[q] = place
        occ[place] = jnp.int32(q)

    @pl.loop(0, 32)
    def _(pair):
        for k in range(2):
            p = pair * 2 + k
            turned = jnp.concatenate([x[p], x[p + 64]], axis=0).T
            real, imag = turned[:64], turned[64:]
            start = pl.multiple_of(p * 64, 64)
            y[pl.ds(start, 64), :] = jnp.concatenate([real[:, :64], imag[:, :64]], axis=1)
            y[pl.ds(start + 4096, 64), :] = jnp.concatenate([real[:, 64:], imag[:, 64:]], axis=1)

    for sub in range(3):
        for other in range(sub + 1, 3):

            @pl.when(loc[4 + sub] == other)
            def _():
                exchange_bits(y, loc, occ, other, jnp.int32(12))

        @pl.when(loc[4 + sub] >= 3)
        def _():
            exchange_bits(y, loc, occ, sub, loc[4 + sub])

    fill(ta, [one_shl(loc[q] - 3) for q in range(4)])
    fill(rv, [one_shl(loc[q] - 3) for q in range(7, QUBITS)])
    channel(sup, 1, False, lanes, y, ta, rv, xh, xl, mixed, high, low)

    @pl.loop(0, 32)
    def _(pair):
        for k, b in enumerate((b0, b1)):
            base = rv[pair * 2 + k]
            for low_bits in range(16):
                b[pl.ds(low_bits, 8, stride=16), :] = y[tile_at(base + ta[low_bits]), :]
        for k, b in enumerate((b0, b1)):
            columns = pl.ds(pl.multiple_of((pair * 2 + k) * 128, 128), 128)
            turned = b[...].T
            out[0, :, columns] = turned[:64]
            out[1, :, columns] = turned[64:]

    me = where[0]
    block = out[0, :, pl.ds(pl.multiple_of((me // 2) * 128, 128), 128)]
    lane = lax.broadcasted_iota(jnp.int32, (64, 128), 1)
    row = lax.broadcasted_iota(jnp.int32, (64, 128), 0)
    kept = jnp.where(lane == row + (me % 2) * 64, block, 0.0)
    folded = kept[0:8]
    for j in range(1, 8):
        folded = folded + kept[8 * j : 8 * j + 8]
    trace[...] = folded


def add_all(x, total, parts, send, recv):
    me = lax.axis_index(HI_GRP)
    devices = parts.shape[0]

    def place(k):
        d = lax.rem(me + k, devices)
        return {"hi": d // 2, "grp": lax.rem(d, 2)}

    barrier = pltpu.get_barrier_semaphore()

    @pl.loop(1, devices)
    def _(k):
        pl.semaphore_signal(
            barrier, inc=1, device_id=place(k), device_id_type=pl.DeviceIdType.MESH
        )

    pl.semaphore_wait(barrier, devices - 1)

    def copy(k):
        return pltpu.make_async_remote_copy(
            src_ref=x,
            dst_ref=parts.at[k],
            send_sem=send.at[k],
            recv_sem=recv.at[k],
            device_id=place(k),
            device_id_type=pl.DeviceIdType.MESH,
        )

    @pl.loop(1, devices)
    def _(k):
        copy(k).start()

    parts[0] = x[...]

    @pl.loop(1, devices)
    def _(k):
        copy(k).wait()

    grand = jnp.sum(parts[...], axis=0)
    total[...] = jnp.sum(jnp.sum(grand, axis=1, keepdims=True), axis=0, keepdims=True) / ROWS


def call(body, outs, out_smem, n_smem, n_args, scratch, args):
    smem = pl.BlockSpec(memory_space=SMEM)
    vmem = pl.BlockSpec(memory_space=VMEM)
    return pl.pallas_call(
        body,
        out_shape=outs,
        in_specs=[smem if i < n_smem else vmem for i in range(n_args)],
        out_specs=tuple(smem if i in out_smem else vmem for i in range(len(outs))),
        scratch_shapes=scratch,
        compiler_params=pltpu.CompilerParams(vmem_limit_bytes=60 * 2**20),
    )(*args)


def table(*sizes):
    return [SMEM((n,), jnp.int32) for n in sizes]


def square(dtype):
    return VMEM((512, 512), dtype)


FULL = VMEM((8192, 128), F32)
BLOCK = VMEM((128, 128), F32)
MAP = jax.ShapeDtypeStruct((8,), jnp.int32)
WORK = [square(BF16), square(BF16), square(F32), square(BF16), square(BF16)]


def spread_call(perm, x):
    return call(
        spread, (jax.ShapeDtypeStruct((128, 64, 128), F32), MAP), (1,), 1, 2,
        [FULL] + table(14, 14, 14, 8, 64), (perm, x),
    )


def middle_call(perm, lanes, sup, x):
    return call(
        middle, (jax.ShapeDtypeStruct((8192, 128), F32), MAP), (1,), 2, 4,
        [FULL] + WORK + table(13, 13, 13, 13, 13, 16, 64, 8, 128), (perm, lanes, sup, x),
    )


def back_call(perm, lanes, where, sup, x):
    return call(
        gather_back,
        (jax.ShapeDtypeStruct((2, 64, 8192), F32), jax.ShapeDtypeStruct((8, 128), F32)),
        (), 3, 5,
        [FULL, BLOCK, BLOCK] + WORK + table(14, 13, 13, 13, 16, 64), (perm, lanes, where, sup, x),
    )


def add_all_call(block, devices):
    vmem = pl.BlockSpec(memory_space=VMEM)
    return pl.pallas_call(
        add_all,
        out_shape=jax.ShapeDtypeStruct((1, 1), F32),
        in_specs=[vmem],
        out_specs=vmem,
        scratch_shapes=[
            VMEM((devices, 8, 128), F32),
            pltpu.SemaphoreType.DMA((devices,)),
            pltpu.SemaphoreType.DMA((devices,)),
        ],
        compiler_params=pltpu.CompilerParams(collective_id=1, has_side_effects=True),
    )(block)


def exchange(value):
    return lax.all_to_all(value, HI_GRP, split_axis=0, concat_axis=0, tiled=True)


def per_device(rho, perm, superop):
    sent, lanes = spread_call(perm, rho)
    mid, rows = middle_call(perm, lanes, superop, exchange(sent).reshape(8192, 128))
    where = lax.axis_index(HI_GRP).astype(jnp.int32).reshape(1)
    matrix, trace = back_call(perm, rows, where, superop, exchange(mid.reshape(128, 64, 128)))
    return matrix, add_all_call(trace, lax.axis_size(HI_GRP)).reshape(())


def solution(mesh):
    in_specs = (P(None, HI_GRP, None), P(), P())
    out_specs = (P(None, HI_GRP, None), P())
    return jax.shard_map(
        per_device, mesh=mesh, in_specs=in_specs, out_specs=out_specs, check_vma=False
    )
```

```python
import functools

import jax
import jax.numpy as jnp
import numpy as np
from jax import lax
from jax.experimental import pallas as pl
from jax.experimental.pallas import tpu as pltpu
from jax.sharding import Mesh
from jax.sharding import PartitionSpec as P

ROWS = 8192
QUBITS = 13
HI_GRP = ("hi", "grp")
F32 = jnp.float32
BF16 = jnp.bfloat16
SMEM = pltpu.SMEM
VMEM = pltpu.VMEM


def fill(table, weights):
    table[0] = jnp.int32(0)
    for k, weight in enumerate(weights):
        for j in range(1 << k):
            table[(1 << k) + j] = table[j] + weight


def one_shl(amount):
    return jnp.left_shift(jnp.int32(1), amount)


def column_order(perm, order):
    for j in range(4):
        order[j] = perm[0, j]
    count = jnp.int32(4)
    for q in range(QUBITS):
        order[count] = jnp.int32(q)
        mine = perm[0, 0] == q
        for j in range(1, 4):
            mine = mine | (perm[0, j] == q)
        count = count + jnp.where(mine, 0, 1)


def tile_at(vreg):
    return pl.ds(pl.multiple_of(vreg * 8, 8), 8)


def insert_zero(index, bit):
    low = index & (one_shl(bit) - 1)
    return (index - low) * 2 + low


def swap_stage(buf, sub, bit, unroll=8):
    step = 1 << sub
    keep = (lax.broadcasted_iota(jnp.int32, (8, 128), 0) & step) == 0

    @pl.loop(0, 512 // unroll)
    def _(i):
        pairs = []
        for k in range(unroll):
            v = insert_zero(i * unroll + k, bit)
            w = v + one_shl(bit)
            pairs.append((v, w, buf[tile_at(v), :], buf[tile_at(w), :]))
        for v, w, a, b in pairs:
            buf[tile_at(v), :] = jnp.where(keep, a, pltpu.roll(b, step, 0))
            buf[tile_at(w), :] = jnp.where(keep, pltpu.roll(a, 8 - step, 0), b)


def exchange_bits(buf, loc, occ, sub, place):
    swap_stage(buf, sub, place - 3)
    here, there = occ[sub], occ[place]
    occ[sub] = there
    occ[place] = here
    loc[there] = jnp.int32(sub)
    loc[here] = place


def settle_sublanes(buf, loc, occ, wanted, bits):
    for sub in range(3):
        best = jnp.int32(-1)
        for bit in bits:
            best = jnp.where(wanted(bit) & (loc[bit] >= 3), loc[bit], best)

        @pl.when(jnp.logical_not(wanted(occ[sub])) & (best >= 3))
        def _():
            exchange_bits(buf, loc, occ, sub, best)


def own_slots(slots, where):
    return [slots[part, where[0]] ^ (64 * part) for part in range(PARTS)]


def spread(perm, slots, where, x, out, lanes, y, order, loc, occ, tc, te):
    column_order(perm, order)
    top = order[12]
    for q in range(QUBITS):
        place = jnp.where(jnp.int32(q) < top, q, q - 1)
        loc[q] = jnp.where(jnp.int32(q) == top, jnp.int32(13), place)
        occ[place] = jnp.int32(q)
    for q in range(QUBITS):

        @pl.when(jnp.int32(q) != top)
        def _():
            occ[loc[q]] = jnp.int32(q)

    step = one_shl(top - 7)

    @pl.loop(0, 16)
    def _(pair):
        for k in range(2):
            m = pair * 2 + k
            first = insert_zero(m, top - 7)
            for part in range(2):
                halves = [
                    x[part, :, pl.ds(pl.multiple_of(t * 128, 128), 128)]
                    for t in (first, first + step)
                ]
                start = pl.multiple_of(part * 4096 + m * 128, 128)
                y[pl.ds(start, 128), :] = jnp.concatenate(halves, axis=0).T

    def local(bit):
        found = bit == order[0]
        for i in range(1, 6):
            found = found | (bit == order[i])
        return found

    settle_sublanes(y, loc, occ, local, [order[i] for i in range(6)])
    for s in range(3):
        found = jnp.int32(0)
        for i in range(6):
            found = jnp.where(order[i] == occ[s], i, found)
        lanes[s] = found
    count = jnp.int32(3)
    for i in range(6):
        lanes[count] = jnp.int32(i)
        count = count + jnp.where(loc[order[i]] >= 3, 1, 0)
    fill(tc, [one_shl(loc[order[lanes[3 + i]]] - 3) for i in range(3)])
    fill(te, [one_shl(loc[order[6 + i]] - 3) for i in range(6)])
    mine = own_slots(slots, where)

    @pl.loop(0, 16)
    def _(group):
        for k in range(4):
            e = group * 4 + k
            base = te[e]
            tiles = [y[tile_at(base + tc[j] + part * 512), :] for part in range(2) for j in range(8)]
            turned = jnp.concatenate(tiles, axis=0).T
            for j in range(16):
                part = j % 8
                v = slots[part, e + 64 * (j // 8)] ^ mine[part]
                out[tile_at(v), :] = turned[8 * j : 8 * j + 8]


def split_bf16(value):
    high = value.astype(BF16)
    return high, (value - high.astype(F32)).astype(BF16)


def build_weights(sup, layer, pair, major_is_row, lanes, high_ref, low_ref):
    def canonical(lane):
        if lanes is None:
            return lane & 63
        total = jnp.zeros_like(lane)
        for k in range(6):
            total = total + jnp.left_shift(jnp.right_shift(lane, k) & 1, lanes[k])
        return total

    def uv(major, lane):
        minor = jnp.right_shift(lane, 2 * pair) & 3
        return 4 * major + minor if major_is_row else 4 * minor + major

    row = lax.broadcasted_iota(jnp.int32, (512, 16), 0)
    col16 = lax.broadcasted_iota(jnp.int32, (512, 16), 1)

    def one_hot(lane):
        hit = uv(jnp.right_shift(row, 7), lane) == col16
        return jnp.where(hit, 1.0, 0.0).astype(BF16)

    expand_out = one_hot(row & 63)
    expand_in = expand_out if lanes is None else one_hot(canonical(row))
    dims = (((1,), (1,)), ((), ()))
    raw_in = lax.broadcasted_iota(jnp.int32, (512, 128), 0) & 127
    lane_in = canonical(raw_in)
    raw_out = lax.broadcasted_iota(jnp.int32, (512, 128), 1)
    keep = 63 & ~(3 << (2 * pair))
    same_rest = (lane_in & keep) == (raw_out & keep)
    part_in = jnp.right_shift(raw_in, 6)
    part_out = jnp.right_shift(raw_out, 6)
    sign = jnp.where(part_out >= part_in, 1.0, -1.0).astype(F32)
    parts = [split_bf16(sup[layer, part]) for part in range(2)]
    for which, ref in enumerate((high_ref, low_ref)):
        half = [
            lax.dot_general(expand_in, parts[p][which], dims, preferred_element_type=F32).astype(BF16)
            for p in range(2)
        ]
        for block in range(4):
            target = expand_out[block * 128 : (block + 1) * 128]
            real, imag = (
                lax.dot_general(h, target, dims, preferred_element_type=F32) for h in half
            )
            value = jnp.where(part_in == part_out, real, sign * imag)
            ref[:, block * 128 : (block + 1) * 128] = jnp.where(same_rest, value, 0.0).astype(BF16)


def apply_pair(z, pair, ta, rv, xh, xl, mixed, high_ref, low_ref):
    @pl.loop(0, 4)
    def _(other):
        first = other * 4 if pair == 0 else other
        stride = 1 if pair == 0 else 4
        bases = [ta[first + stride * k] for k in range(4)]

        @pl.loop(0, 16)
        def _(r):
            for half in range(2):
                v0 = rv[r * 4 + half * 2]
                v1 = rv[r * 4 + half * 2 + 1]
                rows = pl.ds(pl.multiple_of(r * 32 + half * 16, 16), 16)
                for k in range(4):
                    both = [z[tile_at(bases[k] + v), :] for v in (v0, v1)]
                    high, low = split_bf16(jnp.concatenate(both, axis=0))
                    xh[rows, k * 128 : (k + 1) * 128] = high
                    xl[rows, k * 128 : (k + 1) * 128] = low

        total = jnp.dot(xh[...], high_ref[...], preferred_element_type=F32)
        total += jnp.dot(xl[...], high_ref[...], preferred_element_type=F32)
        total += jnp.dot(xh[...], low_ref[...], preferred_element_type=F32)
        mixed[...] = total

        @pl.loop(0, 16)
        def _(r):
            for j in range(4):
                v = rv[r * 4 + j]
                rows = pl.ds(pl.multiple_of(r * 32 + j * 8, 8), 8)
                for k in range(4):
                    z[tile_at(bases[k] + v), :] = mixed[rows, k * 128 : (k + 1) * 128]


def channel(sup, layer, major_is_row, lanes, z, ta, rv, xh, xl, mixed, high_ref, low_ref):
    for pair in range(2):
        build_weights(sup, layer, pair, major_is_row, lanes if pair == 0 else None, high_ref, low_ref)
        apply_pair(z, pair, ta, rv, xh, xl, mixed, high_ref, low_ref)


def trace_share(perm, where, sup, z, loc, outpos, final, order, tu, tc):
    column_order(perm, order)
    me = where[0]

    def place_of(bit):
        found = jnp.int32(0)
        for i in range(QUBITS):
            found = jnp.where(order[i] == bit, i, found)
        return found

    lane = lax.broadcasted_iota(jnp.int32, (16, 128), 1)
    group = jnp.zeros((16, 128), jnp.int32)
    for j in range(4):
        place = place_of(final[j])
        local = jnp.right_shift(lane, jnp.minimum(place, 5)) & 1
        remote_bit = jnp.right_shift(me, jnp.maximum(place - 6, 0)) & 1
        group = group + jnp.left_shift(jnp.where(place < 6, local, remote_bit), j)
    row16 = lax.broadcasted_iota(jnp.int32, (16, 16), 0)
    col16 = lax.broadcasted_iota(jnp.int32, (16, 16), 1)
    hot = jnp.where(lax.broadcasted_iota(jnp.int32, (16, 128), 0) == group, 1.0, 0.0).astype(F32)
    single = []
    for part in range(2):
        s = sup[1, part]
        tau = s[0:1] + s[5:6] + s[10:11] + s[15:16]
        both = []
        for pair in range(2):
            pick = 4 * (jnp.right_shift(row16, 2 * pair) & 3) + (jnp.right_shift(col16, 2 * pair) & 3)
            value = jnp.zeros((16, 16), F32)
            for uv in range(16):
                value = jnp.where(pick == uv, tau[:, uv : uv + 1], value)
            both.append(value)
        single.append(both)
    real = single[0][0] * single[0][1] - single[1][0] * single[1][1]
    imag = single[0][0] * single[1][1] + single[1][0] * single[0][1]
    exact = functools.partial(jnp.dot, precision=lax.Precision.HIGHEST, preferred_element_type=F32)
    weight = jnp.where(lane < 64, exact(real, hot), -exact(imag, hot))

    fill(tu, [one_shl(loc[final[j]]) for j in range(4)])

    def weight_of(bit):
        return jnp.where(outpos[bit] >= 4, one_shl(loc[bit]), 0)

    fill(tc, [weight_of(order[i]) for i in range(6)])
    base = jnp.int32(0)
    for i in range(6, QUBITS):
        base = base + weight_of(order[i]) * (jnp.right_shift(me, i - 6) & 1)
    lane1 = lax.broadcasted_iota(jnp.int32, (1, 128), 1) & 63
    sums = jnp.zeros((1, 128), F32)

    def column(c, rows):
        start = base + tc[c]
        return tuple(
            jnp.where(lane1 == c, z[pl.ds(start + tu[u], 1), :], rows[u]) for u in range(16)
        )

    rows = lax.fori_loop(0, 64, column, tuple(sums for _ in range(16)))
    for u in range(16):
        sums = sums + weight[u : u + 1] * rows[u]
    return sums


def middle(perm, lanes, slots, where, sup, x, out, rows_out, share, z, xh, xl, mixed, high, low,
           final, outpos, loc, occ, rest, ta, rv, ti, td, order, tu, tc):
    for q in range(QUBITS):
        bit = perm[0, perm[1, q]]
        final[q] = bit
        outpos[bit] = jnp.int32(q)
        loc[q] = jnp.int32(q)
        occ[q] = jnp.int32(q)
    mine = own_slots(slots, where)

    @pl.loop(0, 64)
    def _(i):
        for k in range(2):
            d = i * 2 + k
            for part in range(PARTS):
                z[tile_at(d * 8 + part), :] = x[tile_at(slots[part, d] ^ mine[part]), :]

    mixes = [perm[0, j] for j in range(4)]

    def mixed_bit(bit):
        found = bit == mixes[0]
        for m in mixes[1:]:
            found = found | (bit == m)
        return found

    everything = [jnp.int32(q) for q in range(QUBITS)]
    stays = lambda bit: outpos[bit] < 6
    settle_sublanes(z, loc, occ, lambda bit: jnp.logical_not(mixed_bit(bit)) & stays(bit), everything)
    settle_sublanes(z, loc, occ, lambda bit: jnp.logical_not(mixed_bit(bit)), everything)
    count = jnp.int32(0)
    for place in range(3, QUBITS):
        rest[count] = jnp.int32(place)
        count = count + jnp.where(mixed_bit(occ[place]), 0, 1)
    fill(ta, [one_shl(loc[m] - 3) for m in mixes])
    fill(rv, [one_shl(rest[j] - 3) for j in range(6)])
    channel(sup, 0, True, lanes, z, ta, rv, xh, xl, mixed, high, low)
    share[...] = trace_share(perm, where, sup, z, loc, outpos, final, order, tu, tc)
    settle_sublanes(z, loc, occ, stays, everything)
    for s in range(3):
        rows_out[s] = outpos[occ[s]]
    count = jnp.int32(3)
    for q in range(6):
        rows_out[count] = jnp.int32(q)
        count = count + jnp.where(loc[final[q]] >= 3, 1, 0)
    fill(ti, [one_shl(loc[final[rows_out[3 + i]]] - 3) for i in range(3)])
    fill(td, [one_shl(loc[final[6 + i]] - 3) for i in range(7)])

    @pl.loop(0, 64)
    def _(i):
        for k in range(2):
            d = i * 2 + k
            base = td[d]
            for j in range(8):
                out[tile_at(slots[j, d] ^ mine[j]), :] = z[tile_at(base + ti[j]), :]


def gather_back(perm, lanes, slots, where, sup, x, out, y, b0, b1, xh, xl, mixed, high, low,
                order, inv, loc, occ, ta, rv):
    column_order(perm, order)
    for i in range(QUBITS):
        inv[order[i]] = jnp.int32(i)
    for q in range(QUBITS):
        place = inv[perm[0, perm[1, q]]]
        loc[q] = place
        occ[place] = jnp.int32(q)
    mine = own_slots(slots, where)

    @pl.loop(0, 32)
    def _(pair):
        for k in range(2):
            p = pair * 2 + k
            tiles = [
                x[tile_at(slots[j, p + 64 * k] ^ mine[j]), :] for k in range(2) for j in range(PARTS)
            ]
            turned = jnp.concatenate(tiles, axis=0).T
            real, imag = turned[:64], turned[64:]
            start = pl.multiple_of(p * 64, 64)
            y[pl.ds(start, 64), :] = jnp.concatenate([real[:, :64], imag[:, :64]], axis=1)
            y[pl.ds(start + 4096, 64), :] = jnp.concatenate([real[:, 64:], imag[:, 64:]], axis=1)

    for sub in range(3):
        for other in range(sub + 1, 3):

            @pl.when(loc[4 + sub] == other)
            def _():
                exchange_bits(y, loc, occ, other, jnp.int32(12))

        @pl.when(loc[4 + sub] >= 3)
        def _():
            exchange_bits(y, loc, occ, sub, loc[4 + sub])

    fill(ta, [one_shl(loc[q] - 3) for q in range(4)])
    fill(rv, [one_shl(loc[q] - 3) for q in range(7, QUBITS)])
    channel(sup, 1, False, lanes, y, ta, rv, xh, xl, mixed, high, low)

    @pl.loop(0, 32)
    def _(pair):
        for k, b in enumerate((b0, b1)):
            base = rv[pair * 2 + k]
            for low_bits in range(16):
                b[pl.ds(low_bits, 8, stride=16), :] = y[tile_at(base + ta[low_bits]), :]
        for k, b in enumerate((b0, b1)):
            columns = pl.ds(pl.multiple_of((pair * 2 + k) * 128, 128), 128)
            turned = b[...].T
            out[0, :, columns] = turned[:64]
            out[1, :, columns] = turned[64:]


LINKS = 6
PARTS = 8


def part_links(part):
    return [(t, (part + t) % 8) for t in range(8) if (part + t) % 8 < LINKS]


def slot_table():
    low_high = ((4, 5), (6, 0), (2, 3))
    table = np.zeros((PARTS, 128), np.int32)
    for part in range(PARTS):
        place = {link: 1 << (5 - s) for s, (_, link) in enumerate(part_links(part))}
        weight = [0] * 7
        weight[1] = 512
        for axis, (low, high) in enumerate(low_high):
            weight[low] = place[2 * axis]
            weight[high] = place[2 * axis] | place[2 * axis + 1]
        for device in range(128):
            for bit in range(7):
                if device >> bit & 1:
                    table[part, device] ^= weight[bit]
        table[part] += 64 * part
    return table


def swap_all(with_sum, *refs):
    if with_sum:
        x, mine, out, total, shares, share_send, share_recv, *refs = refs
    else:
        x, out, *refs = refs
    held, (send, recv, first_send, first_recv, out_sem) = refs[:7], refs[7:]
    hi = lax.axis_index("hi")
    grp = lax.axis_index("grp")
    bits = [lax.rem(hi // (1 << k), 2) for k in range(6)]

    def flip(k):
        return (1 - 2 * bits[k]) * (1 << k)

    core = {"hi": hi + flip(0), "grp": grp}
    link_device = [
        {"hi": hi + flip(3), "grp": grp},
        {"hi": hi + flip(3) + flip(4), "grp": grp},
        {"hi": hi + flip(5), "grp": grp},
        {"hi": hi + flip(5), "grp": 1 - grp},
        {"hi": hi + flip(1), "grp": grp},
        {"hi": hi + flip(1) + flip(2), "grp": grp},
    ]
    mesh_ids = pl.DeviceIdType.MESH
    barrier = pltpu.get_barrier_semaphore()
    for device in [core] + link_device:
        pl.semaphore_signal(barrier, inc=1, device_id=device, device_id_type=mesh_ids)
    pl.semaphore_wait(barrier, 7)

    def remote(src, dst, send_sem, recv_sem, device):
        return pltpu.make_async_remote_copy(
            src_ref=src, dst_ref=dst, send_sem=send_sem, recv_sem=recv_sem,
            device_id=device, device_id_type=mesh_ids,
        )

    for p in range(PARTS):
        pltpu.make_async_copy(x.at[0, p], held[0].at[0, p], first_recv.at[0, p]).start()
        remote(x.at[1, p], held[0].at[1, p], first_send.at[p], first_recv.at[1, p], core).start()

    def arrived(h, p, s):
        ref = held[s].at[h, p]
        sem = first_recv.at[h, p] if s == 0 else recv.at[h, p, s - 1]
        pltpu.make_async_copy(ref, ref, sem).wait()

    def pick(s, chosen):
        return tuple(chosen[b] for b in range(1, 7) if b != s)

    def cross(h, p, s, link):
        for j in range(s):
            source = {b: slice(None) for b in range(1, 7)}
            for b in range(j + 1, s):
                source[b] = 0
            source[s] = 1
            target = dict(source)
            if j:
                target[j] = 1
            remote(
                held[j].at[(h, p) + pick(j, source)], held[s].at[(h, p) + pick(s, target)],
                send.at[h, p, s - 1], recv.at[h, p, s - 1], link_device[link],
            ).start()

    def deliver(h, p):
        for j in range(7):
            source = {b: slice(None) if b < j else 0 for b in range(1, 7)}
            target = dict(source)
            if j:
                target[j] = 1
            pltpu.make_async_copy(
                held[j].at[(h, p) + pick(j, source)],
                out.at[(h, p) + tuple(target[b] for b in range(1, 7))],
                out_sem.at[h, p],
            ).start()

    done = {p: 0 for p in range(PARTS)}
    if with_sum:
        own = pltpu.make_async_copy(mine, shares.at[0], share_recv.at[7])
        own.start()
        own.wait()

        def double(k):
            return remote(
                shares.at[0 : 1 << k], shares.at[1 << k : 2 << k], share_send.at[k],
                share_recv.at[k], ([core] + link_device)[k],
            )

    for t in range(8):

        @pl.loop(0, 2)
        def _(h):
            for p in range(PARTS):
                link = (p + t) % 8
                if link < LINKS:
                    arrived(h, p, done[p])
                    cross(h, p, done[p] + 1, link)

        if with_sum and t < 7:
            if t:
                double(t - 1).wait()
            double(t).start()
        for p in range(PARTS):
            if (p + t) % 8 < LINKS:
                done[p] += 1

    @pl.loop(0, 2)
    def _(h):
        for p in (0, 7, 1, 2, 3, 4, 5, 6):
            arrived(h, p, 6)
            deliver(h, p)

    if with_sum:
        double(6).wait()
        grand = jnp.sum(shares[...], axis=0)
        total[...] = jnp.sum(grand, axis=1, keepdims=True) / ROWS

    for p in range(PARTS):
        pltpu.make_async_copy(x.at[1, p], x.at[1, p], first_send.at[p]).wait()

    @pl.loop(0, 2)
    def _(h):
        for p in range(PARTS):
            for s in range(1, 7):
                ref = held[s].at[h, p]
                pltpu.make_async_copy(ref, ref, send.at[h, p, s - 1]).wait()
            pltpu.make_async_copy(out.at[h, p], out.at[h, p], out_sem.at[h, p]).wait()


def exchange(value, collective_id, share=None):
    two = (2,) * 6
    whole = jax.ShapeDtypeStruct((2, PARTS) + two + (8, 128), F32)
    dma = pltpu.SemaphoreType.DMA
    anywhere = pl.BlockSpec(memory_space=pltpu.HBM)
    vmem = pl.BlockSpec(memory_space=VMEM)
    extra = share is not None
    scratch = [VMEM((2, PARTS) + two + (8, 128), F32)]
    scratch += [VMEM((2, PARTS) + two[:5] + (8, 128), F32) for _ in range(6)]
    scratch += [dma((2, PARTS, 6)), dma((2, PARTS, 6)), dma((PARTS,)), dma((2, PARTS)), dma((2, PARTS))]
    if extra:
        scratch = [VMEM((128, 1, 128), F32), dma((7,)), dma((8,))] + scratch
    result = pl.pallas_call(
        functools.partial(swap_all, extra),
        out_shape=(whole, jax.ShapeDtypeStruct((1, 1), F32)) if extra else whole,
        in_specs=[anywhere] * (1 + extra),
        out_specs=(anywhere, vmem) if extra else anywhere,
        scratch_shapes=scratch,
        compiler_params=pltpu.CompilerParams(
            collective_id=collective_id, has_side_effects=True, vmem_limit_bytes=40 * 2**20
        ),
    )(*((value.reshape(whole.shape), share) if extra else (value.reshape(whole.shape),)))
    if extra:
        return result[0].reshape(8192, 128), result[1]
    return result.reshape(8192, 128)


def call(body, outs, out_smem, n_smem, n_args, scratch, args):
    smem = pl.BlockSpec(memory_space=SMEM)
    vmem = pl.BlockSpec(memory_space=VMEM)
    return pl.pallas_call(
        body,
        out_shape=outs,
        in_specs=[smem if i < n_smem else vmem for i in range(n_args)],
        out_specs=tuple(smem if i in out_smem else vmem for i in range(len(outs))),
        scratch_shapes=scratch,
        compiler_params=pltpu.CompilerParams(vmem_limit_bytes=60 * 2**20),
    )(*args)


def table(*sizes):
    return [SMEM((n,), jnp.int32) for n in sizes]


def square(dtype):
    return VMEM((512, 512), dtype)


FULL = VMEM((8192, 128), F32)
BLOCK = VMEM((128, 128), F32)
MAP = jax.ShapeDtypeStruct((8,), jnp.int32)
WORK = [square(BF16), square(BF16), square(F32), square(BF16), square(BF16)]


def spread_call(perm, slots, where, x):
    return call(
        spread, (jax.ShapeDtypeStruct((8192, 128), F32), MAP), (1,), 3, 4,
        [FULL] + table(14, 14, 14, 8, 64), (perm, slots, where, x),
    )


def middle_call(perm, lanes, slots, where, sup, x):
    return call(
        middle,
        (jax.ShapeDtypeStruct((8192, 128), F32), MAP, jax.ShapeDtypeStruct((1, 128), F32)),
        (1,), 4, 6,
        [FULL] + WORK + table(13, 13, 13, 13, 13, 16, 64, 8, 128, 14, 16, 64),
        (perm, lanes, slots, where, sup, x),
    )


def back_call(perm, lanes, slots, where, sup, x):
    return call(
        gather_back, (jax.ShapeDtypeStruct((2, 64, 8192), F32),), (), 4, 6,
        [FULL, BLOCK, BLOCK] + WORK + table(14, 13, 13, 13, 16, 64),
        (perm, lanes, slots, where, sup, x),
    )[0]


def per_device(rho, perm, superop):
    slots = jnp.asarray(slot_table())
    where = lax.axis_index(HI_GRP).astype(jnp.int32).reshape(1)
    sent, lanes = spread_call(perm, slots, where, rho)
    mid, rows, share = middle_call(perm, lanes, slots, where, superop, exchange(sent, 0))
    last, total = exchange(mid, 1, share)
    return back_call(perm, rows, slots, where, superop, last), total.reshape(())


def solution(mesh):
    in_specs = (P(None, HI_GRP, None), P(), P())
    out_specs = (P(None, HI_GRP, None), P())
    return jax.shard_map(
        per_device, mesh=mesh, in_specs=in_specs, out_specs=out_specs, check_vma=False
    )
```

```python
import functools

import jax
import jax.numpy as jnp
import numpy as np
from jax import lax
from jax.experimental import pallas as pl
from jax.experimental.pallas import tpu as pltpu
from jax.sharding import Mesh
from jax.sharding import PartitionSpec as P

ROWS = 8192
QUBITS = 13
HI_GRP = ("hi", "grp")
F32 = jnp.float32
BF16 = jnp.bfloat16
SMEM = pltpu.SMEM
VMEM = pltpu.VMEM


def fill(table, weights):
    table[0] = jnp.int32(0)
    for k, weight in enumerate(weights):
        for j in range(1 << k):
            table[(1 << k) + j] = table[j] + weight


def one_shl(amount):
    return jnp.left_shift(jnp.int32(1), amount)


def column_order(perm, order):
    for j in range(4):
        order[j] = perm[0, j]
    count = jnp.int32(4)
    for q in range(QUBITS):
        order[count] = jnp.int32(q)
        mine = perm[0, 0] == q
        for j in range(1, 4):
            mine = mine | (perm[0, j] == q)
        count = count + jnp.where(mine, 0, 1)


def tile_at(row):
    return pl.ds(pl.multiple_of(row, 8), 8)


def insert_zero(index, bit):
    low = index & (one_shl(bit) - 1)
    return (index - low) * 2 + low


def swap_stage(buf, sub, bit, pairs_low, pairs_high):
    step = 1 << sub
    keep = (lax.broadcasted_iota(jnp.int32, (8, 128), 0) & step) == 0
    weights = [8 * one_shl(jnp.int32(k) + jnp.where(k >= bit, 1, 0)) for k in range(9)]
    fill(pairs_low, weights[:3])
    fill(pairs_high, weights[3:])
    far = 8 * one_shl(bit)

    @pl.loop(0, 64)
    def _(i):
        base = pairs_high[i]
        pairs = []
        for k in range(8):
            v = base + pairs_low[k]
            pairs.append((v, v + far, buf[tile_at(v), :], buf[tile_at(v + far), :]))
        for v, w, a, b in pairs:
            buf[tile_at(v), :] = jnp.where(keep, a, pltpu.roll(b, step, 0))
            buf[tile_at(w), :] = jnp.where(keep, pltpu.roll(a, 8 - step, 0), b)


def exchange_bits(buf, loc, occ, sub, place, pairs):
    swap_stage(buf, sub, place - 3, *pairs)
    here, there = occ[sub], occ[place]
    occ[sub] = there
    occ[place] = here
    loc[there] = jnp.int32(sub)
    loc[here] = place


def settle_sublanes(buf, loc, occ, wanted, bits, pairs):
    for sub in range(3):
        best = jnp.int32(-1)
        for bit in bits:
            best = jnp.where(wanted(bit) & (loc[bit] >= 3), loc[bit], best)

        @pl.when(jnp.logical_not(wanted(occ[sub])) & (best >= 3))
        def _():
            exchange_bits(buf, loc, occ, sub, best, pairs)


def own_slots(slots, where):
    return [slots[where[0] * 8 + part] ^ (512 * part) for part in range(PARTS)]


def spread(perm, slots, where, x, out, lanes, y, order, loc, occ, tc, te, *pairs):
    column_order(perm, order)
    top = order[12]
    for q in range(QUBITS):
        place = jnp.where(jnp.int32(q) < top, q, q - 1)
        loc[q] = jnp.where(jnp.int32(q) == top, jnp.int32(13), place)
        occ[place] = jnp.int32(q)
    for q in range(QUBITS):

        @pl.when(jnp.int32(q) != top)
        def _():
            occ[loc[q]] = jnp.int32(q)

    step = one_shl(top - 7)

    @pl.loop(0, 8)
    def _(group):
        for k in range(4):
            m = group * 4 + k
            first = insert_zero(m, top - 7)
            for part in range(2):
                halves = [
                    x[part, :, pl.ds(pl.multiple_of(t * 128, 128), 128)]
                    for t in (first, first + step)
                ]
                start = pl.multiple_of(part * 4096 + m * 128, 128)
                y[pl.ds(start, 128), :] = jnp.concatenate(halves, axis=0).T

    def local(bit):
        found = bit == order[0]
        for i in range(1, 6):
            found = found | (bit == order[i])
        return found

    settle_sublanes(y, loc, occ, local, [order[i] for i in range(6)], pairs)
    for s in range(3):
        found = jnp.int32(0)
        for i in range(6):
            found = jnp.where(order[i] == occ[s], i, found)
        lanes[s] = found
    count = jnp.int32(3)
    for i in range(6):
        lanes[count] = jnp.int32(i)
        count = count + jnp.where(loc[order[i]] >= 3, 1, 0)
    fill(tc, [one_shl(loc[order[lanes[3 + i]]]) for i in range(3)])
    fill(te, [one_shl(loc[order[6 + i]]) for i in range(6)])
    mine = own_slots(slots, where)

    @pl.loop(0, 16)
    def _(group):
        for k in range(4):
            e = group * 4 + k
            base = te[e]
            tiles = [y[tile_at(base + tc[j] + part * 4096), :] for part in range(2) for j in range(8)]
            turned = jnp.concatenate(tiles, axis=0).T
            for j in range(16):
                part = j % 8
                v = slots[e * 8 + 512 * (j // 8) + part] ^ mine[part]
                out[tile_at(v), :] = turned[8 * j : 8 * j + 8]


def split_bf16(value):
    high = value.astype(BF16)
    return high, (value - high.astype(F32)).astype(BF16)


def build_weights(sup, layer, pair, major_is_row, lanes, weights):
    def canonical(lane):
        if lanes is None:
            return lane & 63
        total = jnp.zeros_like(lane)
        for k in range(6):
            total = total + jnp.left_shift(jnp.right_shift(lane, k) & 1, lanes[k])
        return total

    def uv(major, lane):
        minor = jnp.right_shift(lane, 2 * pair) & 3
        return 4 * major + minor if major_is_row else 4 * minor + major

    row = lax.broadcasted_iota(jnp.int32, (512, 16), 0)
    col16 = lax.broadcasted_iota(jnp.int32, (512, 16), 1)

    def one_hot(lane):
        hit = uv(jnp.right_shift(row, 7), lane) == col16
        return jnp.where(hit, 1.0, 0.0).astype(BF16)

    expand_out = one_hot(row & 63)
    expand_in = expand_out if lanes is None else one_hot(canonical(row))
    dims = (((1,), (1,)), ((), ()))
    raw_in = lax.broadcasted_iota(jnp.int32, (512, 128), 0) & 127
    lane_in = canonical(raw_in)
    raw_out = lax.broadcasted_iota(jnp.int32, (512, 128), 1)
    keep = 63 & ~(3 << (2 * pair))
    same_rest = (lane_in & keep) == (raw_out & keep)
    part_in = jnp.right_shift(raw_in, 6)
    part_out = jnp.right_shift(raw_out, 6)
    sign = jnp.where(part_out >= part_in, 1.0, -1.0).astype(F32)
    parts = [split_bf16(sup[layer, part]) for part in range(2)]
    for which, starts in enumerate(((0, 512), (1024,))):
        half = [
            lax.dot_general(expand_in, parts[p][which], dims, preferred_element_type=F32).astype(BF16)
            for p in range(2)
        ]
        for block in range(4):
            target = expand_out[block * 128 : (block + 1) * 128]
            real, imag = (
                lax.dot_general(h, target, dims, preferred_element_type=F32) for h in half
            )
            value = jnp.where(part_in == part_out, real, sign * imag)
            value = jnp.where(same_rest, value, 0.0).astype(BF16)
            for begin in starts:
                weights[begin : begin + 512, block * 128 : (block + 1) * 128] = value


def apply_pair(z, result, pair, ta, rv, xa, xb, weights):
    def bases_of(other):
        first = other * 4 if pair == 0 else other
        return [ta[first + (1 if pair == 0 else 4) * k] for k in range(4)]

    def split_rows(bases, xs, r, start):
        vregs = [rv[r], rv[r + 1]]
        for k in range(4):
            both = [z[tile_at(bases[k] + v), :] for v in vregs]
            high, low = split_bf16(jnp.concatenate(both, axis=0))
            rows = pl.ds(start, 16)
            xs[rows, k * 128 : (k + 1) * 128] = high
            xs[rows, 512 + k * 128 : 512 + (k + 1) * 128] = low
            xs[rows, 1024 + k * 128 : 1024 + (k + 1) * 128] = high

    first = bases_of(0)

    @pl.loop(0, 8)
    def _(i):
        for k in range(4):
            split_rows(first, xa, i * 8 + k * 2, pl.multiple_of(i * 64 + k * 16, 16))

    @pl.loop(0, 2)
    def _(i):
        for k, (xs, spare) in enumerate(((xa, xb), (xb, xa))):
            other = 2 * i + k
            following = bases_of(lax.rem(other + 1, 4))
            bases = bases_of(other)
            for r in range(0, 64, 2):
                split_rows(following, spare, r, 8 * r)
            for half in range(2):
                mixed = jnp.dot(
                    xs[...], weights[:, half * 256 : (half + 1) * 256], preferred_element_type=F32
                )
                for r in range(64):
                    v = rv[r]
                    for q in range(2):
                        result[tile_at(bases[2 * half + q] + v), :] = mixed[
                            8 * r : 8 * r + 8, q * 128 : (q + 1) * 128
                        ]


def channel(sup, layer, major_is_row, lanes, z, spare, ta, rv, xa, xb, weights):
    for pair, (source, result) in enumerate(((z, spare), (spare, z))):
        build_weights(sup, layer, pair, major_is_row, lanes if pair == 0 else None, weights)
        apply_pair(source, result, pair, ta, rv, xa, xb, weights)


def trace_share(perm, where, sup, z, loc, outpos, final, order, tu, tc):
    column_order(perm, order)
    me = where[0]

    def place_of(bit):
        found = jnp.int32(0)
        for i in range(QUBITS):
            found = jnp.where(order[i] == bit, i, found)
        return found

    lane = lax.broadcasted_iota(jnp.int32, (16, 128), 1)
    group = jnp.zeros((16, 128), jnp.int32)
    for j in range(4):
        place = place_of(final[j])
        local = jnp.right_shift(lane, jnp.minimum(place, 5)) & 1
        remote_bit = jnp.right_shift(me, jnp.maximum(place - 6, 0)) & 1
        group = group + jnp.left_shift(jnp.where(place < 6, local, remote_bit), j)
    row16 = lax.broadcasted_iota(jnp.int32, (16, 16), 0)
    col16 = lax.broadcasted_iota(jnp.int32, (16, 16), 1)
    hot = jnp.where(lax.broadcasted_iota(jnp.int32, (16, 128), 0) == group, 1.0, 0.0).astype(F32)
    single = []
    for part in range(2):
        s = sup[1, part]
        tau = s[0:1] + s[5:6] + s[10:11] + s[15:16]
        both = []
        for pair in range(2):
            pick = 4 * (jnp.right_shift(row16, 2 * pair) & 3) + (jnp.right_shift(col16, 2 * pair) & 3)
            value = jnp.zeros((16, 16), F32)
            for uv in range(16):
                value = jnp.where(pick == uv, tau[:, uv : uv + 1], value)
            both.append(value)
        single.append(both)
    real = single[0][0] * single[0][1] - single[1][0] * single[1][1]
    imag = single[0][0] * single[1][1] + single[1][0] * single[0][1]
    exact = functools.partial(jnp.dot, precision=lax.Precision.HIGHEST, preferred_element_type=F32)
    weight = jnp.where(lane < 64, exact(real, hot), -exact(imag, hot))

    fill(tu, [one_shl(loc[final[j]]) for j in range(4)])

    def weight_of(bit):
        return jnp.where(outpos[bit] >= 4, one_shl(loc[bit]), 0)

    fill(tc, [weight_of(order[i]) for i in range(6)])
    base = jnp.int32(0)
    for i in range(6, QUBITS):
        base = base + weight_of(order[i]) * (jnp.right_shift(me, i - 6) & 1)
    lane1 = lax.broadcasted_iota(jnp.int32, (1, 128), 1) & 63
    sums = jnp.zeros((1, 128), F32)

    def column(c, rows):
        start = base + tc[c]
        return tuple(
            jnp.where(lane1 == c, z[pl.ds(start + tu[u], 1), :], rows[u]) for u in range(16)
        )

    rows = lax.fori_loop(0, 64, column, tuple(sums for _ in range(16)))
    for u in range(16):
        sums = sums + weight[u : u + 1] * rows[u]
    return sums


def middle(perm, lanes, slots, where, sup, x, out, rows_out, share, z, spare, xa, xb, weights,
           final, outpos, loc, occ, rest, ta, rv, ti, td, order, tu, tc, *pairs):
    for q in range(QUBITS):
        bit = perm[0, perm[1, q]]
        final[q] = bit
        outpos[bit] = jnp.int32(q)
        loc[q] = jnp.int32(q)
        occ[q] = jnp.int32(q)
    mine = own_slots(slots, where)

    @pl.loop(0, 64)
    def _(i):
        for k in range(2):
            d = i * 2 + k
            for part in range(PARTS):
                z[tile_at(d * 64 + part * 8), :] = x[tile_at(slots[d * 8 + part] ^ mine[part]), :]

    mixes = [perm[0, j] for j in range(4)]

    def mixed_bit(bit):
        found = bit == mixes[0]
        for m in mixes[1:]:
            found = found | (bit == m)
        return found

    everything = [jnp.int32(q) for q in range(QUBITS)]
    stays = lambda bit: outpos[bit] < 6
    settle_sublanes(z, loc, occ, lambda bit: jnp.logical_not(mixed_bit(bit)) & stays(bit), everything, pairs)
    settle_sublanes(z, loc, occ, lambda bit: jnp.logical_not(mixed_bit(bit)), everything, pairs)
    count = jnp.int32(0)
    for place in range(3, QUBITS):
        rest[count] = jnp.int32(place)
        count = count + jnp.where(mixed_bit(occ[place]), 0, 1)
    fill(ta, [one_shl(loc[m]) for m in mixes])
    fill(rv, [one_shl(rest[j]) for j in range(6)])
    channel(sup, 0, True, lanes, z, spare, ta, rv, xa, xb, weights)
    share[...] = trace_share(perm, where, sup, z, loc, outpos, final, order, tu, tc)
    settle_sublanes(z, loc, occ, stays, everything, pairs)
    for s in range(3):
        rows_out[s] = outpos[occ[s]]
    count = jnp.int32(3)
    for q in range(6):
        rows_out[count] = jnp.int32(q)
        count = count + jnp.where(loc[final[q]] >= 3, 1, 0)
    fill(ti, [one_shl(loc[final[rows_out[3 + i]]]) for i in range(3)])
    fill(td, [one_shl(loc[final[6 + i]]) for i in range(7)])

    @pl.loop(0, 64)
    def _(i):
        for k in range(2):
            d = i * 2 + k
            base = td[d]
            for j in range(8):
                out[tile_at(slots[d * 8 + j] ^ mine[j]), :] = z[tile_at(base + ti[j]), :]


def gather_back(perm, lanes, slots, where, sup, x, out, y, spare, xa, xb, weights,
                order, inv, loc, occ, ta, rv, *pairs):
    column_order(perm, order)
    for i in range(QUBITS):
        inv[order[i]] = jnp.int32(i)
    for q in range(QUBITS):
        place = inv[perm[0, perm[1, q]]]
        loc[q] = place
        occ[place] = jnp.int32(q)
    mine = own_slots(slots, where)

    @pl.loop(0, 16)
    def _(group):
        for q in range(4):
            p = group * 4 + q
            tiles = [
                x[tile_at(slots[p * 8 + 512 * k + j] ^ mine[j]), :] for k in range(2) for j in range(PARTS)
            ]
            turned = jnp.concatenate(tiles, axis=0).T
            real, imag = turned[:64], turned[64:]
            start = pl.multiple_of(p * 64, 64)
            y[pl.ds(start, 64), :] = jnp.concatenate([real[:, :64], imag[:, :64]], axis=1)
            y[pl.ds(start + 4096, 64), :] = jnp.concatenate([real[:, 64:], imag[:, 64:]], axis=1)

    for sub in range(3):
        for other in range(sub + 1, 3):

            @pl.when(loc[4 + sub] == other)
            def _():
                exchange_bits(y, loc, occ, other, jnp.int32(12), pairs)

        @pl.when(loc[4 + sub] >= 3)
        def _():
            exchange_bits(y, loc, occ, sub, loc[4 + sub], pairs)

    fill(ta, [one_shl(loc[q]) for q in range(4)])
    fill(rv, [one_shl(loc[q]) for q in range(7, QUBITS)])
    channel(sup, 1, False, lanes, y, spare, ta, rv, xa, xb, weights)

    sublane = lax.broadcasted_iota(jnp.int32, (8, 128), 0)

    @pl.loop(0, 16)
    def _(group):
        for q in range(4):
            t = group * 4 + q
            base = rv[t]
            tiles = [y[tile_at(base + ta[b]), :] for b in range(16)]
            for k in range(3):
                step = 1 << k
                keep = (sublane & step) == 0
                for b in range(16):
                    if not b & step:
                        lower, upper = tiles[b], tiles[b + step]
                        tiles[b] = jnp.where(keep, lower, pltpu.roll(upper, step, 0))
                        tiles[b + step] = jnp.where(keep, pltpu.roll(lower, 8 - step, 0), upper)
            ordered = [tiles[8 * (v % 2) + v // 2] for v in range(16)]
            columns = pl.ds(pl.multiple_of(t * 128, 128), 128)
            turned = jnp.concatenate(ordered, axis=0).T
            out[0, :, columns] = turned[:64]
            out[1, :, columns] = turned[64:]


LINKS = 6
PARTS = 8


def part_links(part):
    return [(t, (part + t) % 8) for t in range(8) if (part + t) % 8 < LINKS]


def slot_table():
    low_high = ((4, 5), (6, 0), (2, 3))
    table = np.zeros((PARTS, 128), np.int32)
    for part in range(PARTS):
        place = {link: 1 << (5 - s) for s, (_, link) in enumerate(part_links(part))}
        weight = [0] * 7
        weight[1] = 512
        for axis, (low, high) in enumerate(low_high):
            weight[low] = place[2 * axis]
            weight[high] = place[2 * axis] | place[2 * axis + 1]
        for device in range(128):
            for bit in range(7):
                if device >> bit & 1:
                    table[part, device] ^= weight[bit]
        table[part] += 64 * part
    return 8 * table.T.reshape(-1)


def swap_all(with_sum, *refs):
    if with_sum:
        x, mine, out, total, shares, share_send, share_recv, *refs = refs
    else:
        x, out, *refs = refs
    held, (send, recv, first_send, first_recv, out_sem) = refs[:7], refs[7:]
    hi = lax.axis_index("hi")
    grp = lax.axis_index("grp")
    bits = [lax.rem(hi // (1 << k), 2) for k in range(6)]

    def flip(k):
        return (1 - 2 * bits[k]) * (1 << k)

    core = {"hi": hi + flip(0), "grp": grp}
    link_device = [
        {"hi": hi + flip(3), "grp": grp},
        {"hi": hi + flip(3) + flip(4), "grp": grp},
        {"hi": hi + flip(5), "grp": grp},
        {"hi": hi + flip(5), "grp": 1 - grp},
        {"hi": hi + flip(1), "grp": grp},
        {"hi": hi + flip(1) + flip(2), "grp": grp},
    ]
    mesh_ids = pl.DeviceIdType.MESH
    barrier = pltpu.get_barrier_semaphore()
    for device in [core] + link_device:
        pl.semaphore_signal(barrier, inc=1, device_id=device, device_id_type=mesh_ids)
    pl.semaphore_wait(barrier, 7)

    def remote(src, dst, send_sem, recv_sem, device):
        return pltpu.make_async_remote_copy(
            src_ref=src, dst_ref=dst, send_sem=send_sem, recv_sem=recv_sem,
            device_id=device, device_id_type=mesh_ids,
        )

    for p in range(PARTS):
        pltpu.make_async_copy(x.at[0, p], held[0].at[0, p], first_recv.at[0, p]).start()
        remote(x.at[1, p], held[0].at[1, p], first_send.at[p], first_recv.at[1, p], core).start()

    def arrived(h, p, s):
        ref = held[s].at[h, p]
        sem = first_recv.at[h, p] if s == 0 else recv.at[h, p, s - 1]
        pltpu.make_async_copy(ref, ref, sem).wait()

    def pick(s, chosen):
        return tuple(chosen[b] for b in range(1, 7) if b != s)

    def cross(h, p, s, link):
        for j in range(s):
            source = {b: slice(None) for b in range(1, 7)}
            for b in range(j + 1, s):
                source[b] = 0
            source[s] = 1
            target = dict(source)
            if j:
                target[j] = 1
            remote(
                held[j].at[(h, p) + pick(j, source)], held[s].at[(h, p) + pick(s, target)],
                send.at[h, p, s - 1], recv.at[h, p, s - 1], link_device[link],
            ).start()

    def deliver(h, p):
        for j in range(7):
            source = {b: slice(None) if b < j else 0 for b in range(1, 7)}
            target = dict(source)
            if j:
                target[j] = 1
            pltpu.make_async_copy(
                held[j].at[(h, p) + pick(j, source)],
                out.at[(h, p) + tuple(target[b] for b in range(1, 7))],
                out_sem.at[h, p],
            ).start()

    done = {p: 0 for p in range(PARTS)}
    if with_sum:
        own = pltpu.make_async_copy(mine, shares.at[0], share_recv.at[7])
        own.start()
        own.wait()

        def double(k):
            return remote(
                shares.at[0 : 1 << k], shares.at[1 << k : 2 << k], share_send.at[k],
                share_recv.at[k], ([core] + link_device)[k],
            )

    for t in range(8):

        @pl.loop(0, 2)
        def _(h):
            for p in range(PARTS):
                link = (p + t) % 8
                if link < LINKS:
                    arrived(h, p, done[p])
                    cross(h, p, done[p] + 1, link)

        if with_sum and t < 7:
            if t:
                double(t - 1).wait()
            double(t).start()
        for p in range(PARTS):
            if (p + t) % 8 < LINKS:
                done[p] += 1

    @pl.loop(0, 2)
    def _(h):
        for p in (0, 7, 1, 2, 3, 4, 5, 6):
            arrived(h, p, 6)
            deliver(h, p)

    if with_sum:
        double(6).wait()
        grand = jnp.sum(shares[...], axis=0)
        total[...] = jnp.sum(grand, axis=1, keepdims=True) / ROWS

    for p in range(PARTS):
        pltpu.make_async_copy(x.at[1, p], x.at[1, p], first_send.at[p]).wait()

    @pl.loop(0, 2)
    def _(h):
        for p in range(PARTS):
            for s in range(1, 7):
                ref = held[s].at[h, p]
                pltpu.make_async_copy(ref, ref, send.at[h, p, s - 1]).wait()
            pltpu.make_async_copy(out.at[h, p], out.at[h, p], out_sem.at[h, p]).wait()


def exchange(value, collective_id, share=None):
    two = (2,) * 6
    whole = jax.ShapeDtypeStruct((2, PARTS) + two + (8, 128), F32)
    dma = pltpu.SemaphoreType.DMA
    anywhere = pl.BlockSpec(memory_space=pltpu.HBM)
    vmem = pl.BlockSpec(memory_space=VMEM)
    extra = share is not None
    scratch = [VMEM((2, PARTS) + two + (8, 128), F32)]
    scratch += [VMEM((2, PARTS) + two[:5] + (8, 128), F32) for _ in range(6)]
    scratch += [dma((2, PARTS, 6)), dma((2, PARTS, 6)), dma((PARTS,)), dma((2, PARTS)), dma((2, PARTS))]
    if extra:
        scratch = [VMEM((128, 1, 128), F32), dma((7,)), dma((8,))] + scratch
    result = pl.pallas_call(
        functools.partial(swap_all, extra),
        out_shape=(whole, jax.ShapeDtypeStruct((1, 1), F32)) if extra else whole,
        in_specs=[anywhere] * (1 + extra),
        out_specs=(anywhere, vmem) if extra else anywhere,
        scratch_shapes=scratch,
        compiler_params=pltpu.CompilerParams(
            collective_id=collective_id, has_side_effects=True, vmem_limit_bytes=60 * 2**20
        ),
    )(*((value.reshape(whole.shape), share) if extra else (value.reshape(whole.shape),)))
    if extra:
        return result[0].reshape(8192, 128), result[1]
    return result.reshape(8192, 128)


def call(body, outs, out_smem, n_smem, n_args, scratch, args):
    smem = pl.BlockSpec(memory_space=SMEM)
    vmem = pl.BlockSpec(memory_space=VMEM)
    return pl.pallas_call(
        body,
        out_shape=outs,
        in_specs=[smem if i < n_smem else vmem for i in range(n_args)],
        out_specs=tuple(smem if i in out_smem else vmem for i in range(len(outs))),
        scratch_shapes=scratch,
        compiler_params=pltpu.CompilerParams(vmem_limit_bytes=60 * 2**20),
    )(*args)


def table(*sizes):
    return [SMEM((n,), jnp.int32) for n in sizes]


FULL = VMEM((8192, 128), F32)
MAP = jax.ShapeDtypeStruct((8,), jnp.int32)
WORK = [FULL, VMEM((512, 1536), BF16), VMEM((512, 1536), BF16), VMEM((1536, 512), BF16)]


def spread_call(perm, slots, where, x):
    return call(
        spread, (jax.ShapeDtypeStruct((8192, 128), F32), MAP), (1,), 3, 4,
        [FULL] + table(14, 14, 14, 8, 64, 8, 64), (perm, slots, where, x),
    )


def middle_call(perm, lanes, slots, where, sup, x):
    return call(
        middle,
        (jax.ShapeDtypeStruct((8192, 128), F32), MAP, jax.ShapeDtypeStruct((1, 128), F32)),
        (1,), 4, 6,
        [FULL] + WORK + table(13, 13, 13, 13, 13, 16, 64, 8, 128, 14, 16, 64, 8, 64),
        (perm, lanes, slots, where, sup, x),
    )


def back_call(perm, lanes, slots, where, sup, x):
    return call(
        gather_back, (jax.ShapeDtypeStruct((2, 64, 8192), F32),), (), 4, 6,
        [FULL] + WORK + table(14, 13, 13, 13, 16, 64, 8, 64),
        (perm, lanes, slots, where, sup, x),
    )[0]


def per_device(rho, perm, superop):
    slots = jnp.asarray(slot_table())
    where = lax.axis_index(HI_GRP).astype(jnp.int32).reshape(1)
    sent, lanes = spread_call(perm, slots, where, rho)
    mid, rows, share = middle_call(perm, lanes, slots, where, superop, exchange(sent, 0))
    last, total = exchange(mid, 1, share)
    return back_call(perm, rows, slots, where, superop, last), total.reshape(())


def solution(mesh):
    in_specs = (P(None, HI_GRP, None), P(), P())
    out_specs = (P(None, HI_GRP, None), P())
    return jax.shard_map(
        per_device, mesh=mesh, in_specs=in_specs, out_specs=out_specs, check_vma=False
    )
```

```python
import functools

import jax
import jax.numpy as jnp
import numpy as np
from jax import lax
from jax.experimental import pallas as pl
from jax.experimental.pallas import tpu as pltpu
from jax.sharding import Mesh
from jax.sharding import PartitionSpec as P

ROWS = 8192
QUBITS = 13
HI_GRP = ("hi", "grp")
F32 = jnp.float32
BF16 = jnp.bfloat16
SMEM = pltpu.SMEM
VMEM = pltpu.VMEM


def fill(table, weights):
    table[0] = jnp.int32(0)
    for k, weight in enumerate(weights):
        for j in range(1 << k):
            table[(1 << k) + j] = table[j] + weight


def one_shl(amount):
    return jnp.left_shift(jnp.int32(1), amount)


def column_order(perm, order):
    for j in range(4):
        order[j] = perm[0, j]
    count = jnp.int32(4)
    for q in range(QUBITS):
        order[count] = jnp.int32(q)
        mine = perm[0, 0] == q
        for j in range(1, 4):
            mine = mine | (perm[0, j] == q)
        count = count + jnp.where(mine, 0, 1)


def tile_at(row):
    return pl.ds(pl.multiple_of(row, 8), 8)


def insert_zero(index, bit):
    low = index & (one_shl(bit) - 1)
    return (index - low) * 2 + low


def swap_rows(lower, upper, sub, keep_lower, keep_upper):
    step = 1 << sub
    return (
        jnp.where(keep_lower, lower, pltpu.roll(upper, step, 0)),
        jnp.where(keep_upper, upper, pltpu.roll(lower, 8 - step, 0)),
    )


def swap_lanes(lower, upper, bit):
    lane = lax.broadcasted_iota(jnp.int32, (8, 128), 1)
    keep = (jnp.right_shift(lane, bit) & 1) == 0
    shift = one_shl(bit) if not isinstance(bit, int) else 1 << bit
    return (
        jnp.where(keep, lower, pltpu.roll(upper, shift, 1)),
        jnp.where(keep, pltpu.roll(lower, 128 - shift, 1), upper),
    )


def swap_lane_pairs(tiles, bits):
    t = list(tiles)
    for k, bit in enumerate(bits):
        step = 1 << k
        for i in range(4):
            if not i & step:
                t[i], t[i + step] = swap_lanes(t[i], t[i + step], bit)
    return t


def plan_sublanes(loc, occ, wanted, bits, places, enabled):
    for sub in range(3):
        best = jnp.int32(-1)
        for bit in bits:
            best = jnp.where(wanted(bit) & (loc[bit] >= 3), loc[bit], best)
        needed = jnp.logical_not(wanted(occ[sub])) & (best >= 3)
        enabled[sub] = jnp.where(needed, 1, 0)
        places[sub] = best

        @pl.when(needed)
        def _():
            here, there = occ[sub], occ[best]
            occ[sub] = there
            occ[best] = here
            loc[there] = jnp.int32(sub)
            loc[here] = best


def regroup(load, dst, places, enabled, others, group_low, group_high, origin=None):
    for sub in range(3):
        free = jnp.int32(3)
        for _ in range(5):
            taken = jnp.bool_(False)
            for k in range(3):
                if k != sub:
                    taken = taken | ((places[k] == free) & ((enabled[k] == 1) | (k < sub)))
            free = free + jnp.where(taken, 1, 0)
        places[sub] = jnp.where(enabled[sub] == 1, places[sub], free)
    count = jnp.int32(0)
    for place in range(3, QUBITS):
        others[count] = jnp.int32(place)
        mine = (places[0] == place) | (places[1] == place) | (places[2] == place)
        count = count + jnp.where(mine, 0, 1)
    fill(group_low, [one_shl(others[k]) for k in range(3)])
    fill(group_high, [one_shl(others[3 + k]) for k in range(4)])
    steps = [one_shl(places[k]) for k in range(3)]
    sublane = lax.broadcasted_iota(jnp.int32, (8, 128), 0)
    masks = []
    for k in range(3):
        bit = jnp.right_shift(sublane, k) & 1
        off = enabled[k] == 0
        masks.append(((bit == 0) | off, (bit == 1) | off))
    if origin is not None:
        index = jnp.zeros((8, 128), jnp.int32)
        for k in range(3):
            index = index + jnp.left_shift(jnp.right_shift(sublane, k) & 1, origin[k])

    @pl.loop(0, 16)
    def _(i):
        high = group_high[i]
        for j in range(8):
            base = high + group_low[j]
            rows = [base]
            for k in range(3):
                rows = rows + [r + steps[k] for r in rows]
            tiles = [load(r) for r in rows]
            if origin is not None:
                tiles = [jnp.take_along_axis(t, index, axis=0) for t in tiles]
            for k in range(3):
                for v in range(8):
                    if not v >> k & 1:
                        w = v + (1 << k)
                        tiles[v], tiles[w] = swap_rows(tiles[v], tiles[w], k, *masks[k])
            for r, t in zip(rows, tiles):
                dst[tile_at(r), :] = t


def spread(perm, slots, where, x, out, lanes, y, order, loc, occ, tc, te, places, enabled, *spare):
    column_order(perm, order)
    top = order[12]
    for q in range(QUBITS):
        place = jnp.where(jnp.int32(q) < top, q, q - 1)
        loc[q] = jnp.where(jnp.int32(q) == top, jnp.int32(13), place)
        occ[place] = jnp.int32(q)
    for q in range(QUBITS):

        @pl.when(jnp.int32(q) != top)
        def _():
            occ[loc[q]] = jnp.int32(q)

    step = one_shl(top - 7)

    @pl.loop(0, 8)
    def _(group):
        for k in range(4):
            m = group * 4 + k
            first = insert_zero(m, top - 7)
            for part in range(2):
                halves = [
                    x[part, :, pl.ds(pl.multiple_of(t * 128, 128), 128)]
                    for t in (first, first + step)
                ]
                start = pl.multiple_of(part * 4096 + m * 128, 128)
                y[pl.ds(start, 128), :] = jnp.concatenate(halves, axis=0).T

    def local(bit):
        found = bit == order[0]
        for i in range(1, 6):
            found = found | (bit == order[i])
        return found

    plan_sublanes(loc, occ, local, [order[i] for i in range(6)], places, enabled)

    @pl.when(enabled[0] + enabled[1] + enabled[2] > 0)
    def _():
        regroup(lambda row: y[tile_at(row), :], y, places, enabled, *spare)

    for s in range(3):
        found = jnp.int32(0)
        for i in range(6):
            found = jnp.where(order[i] == occ[s], i, found)
        lanes[s] = found
    count = jnp.int32(3)
    for i in range(6):
        lanes[count] = jnp.int32(i)
        count = count + jnp.where(loc[order[i]] >= 3, 1, 0)
    fill(tc, [one_shl(loc[order[lanes[3 + i]]]) for i in range(3)])
    fill(te, [one_shl(loc[order[6 + i]]) for i in range(6)])
    me = where[0]

    @pl.loop(0, 16)
    def _(group):
        for k in range(4):
            e = group * 4 + k
            base = te[e]
            tiles = [y[tile_at(base + tc[j] + part * 4096), :] for part in range(2) for j in range(8)]
            turned = jnp.concatenate(tiles, axis=0).T
            apart = (e ^ me) * 8
            starts = (apart, apart ^ 512)
            for j in range(16):
                out[tile_at(slots[starts[j // 8] + j % 8]), :] = turned[8 * j : 8 * j + 8]


def split_bf16(value):
    high = value.astype(BF16)
    return high, (value - high.astype(F32)).astype(BF16)


def build_weights(sup, layer, major_is_row, lanes, weights):
    def canonical(lane):
        total = jnp.zeros_like(lane)
        for k in range(6):
            total = total + jnp.left_shift(jnp.right_shift(lane, k) & 1, lanes[k])
        return total

    row = lax.broadcasted_iota(jnp.int32, (512, 16), 0)
    col16 = lax.broadcasted_iota(jnp.int32, (512, 16), 1)

    def one_hot(pair, lane):
        inner = jnp.right_shift(lane, 2 * pair) & 3
        other = jnp.right_shift(row, 7) if pair else jnp.right_shift(lane, 4) & 3
        uv = 4 * other + inner if major_is_row else 4 * inner + other
        return jnp.where(uv == col16, 1.0, 0.0).astype(BF16)

    dims = (((1,), (1,)), ((), ()))
    parts = [split_bf16(sup[layer, part]) for part in range(2)]
    lane_in = canonical(row)
    source = []
    target = []
    for pair in range(2):
        expand = one_hot(pair, lane_in)
        source.append(
            [
                jnp.concatenate(
                    [
                        lax.dot_general(expand, p, dims, preferred_element_type=F32).astype(BF16)
                        for p in parts[part]
                    ],
                    axis=1,
                )
                for part in range(2)
            ]
        )
        expand = one_hot(pair, row & 63)
        target.append(jnp.concatenate([expand, expand], axis=1))
    part_in = jnp.right_shift(lax.broadcasted_iota(jnp.int32, (512, 128), 0) & 127, 6)
    part_out = jnp.right_shift(lax.broadcasted_iota(jnp.int32, (512, 128), 1), 6)
    for block in range(4):
        columns = slice(block * 128, (block + 1) * 128)
        (r0, i0), (r1, i1) = (
            [
                lax.dot_general(source[pair][part], target[pair][columns], dims, preferred_element_type=F32)
                for part in range(2)
            ]
            for pair in range(2)
        )
        imag = r0 * i1 + i0 * r1
        value = jnp.where(
            part_in == part_out, r0 * r1 - i0 * i1, jnp.where(part_out > part_in, imag, -imag)
        )
        high, low = split_bf16(value)
        weights[0:512, columns] = high
        weights[512:1024, columns] = high
        weights[1024:1536, columns] = low


def channel(z, result, major, rest, lane_bits, xa, xb, weights):
    bases = [major[k] for k in range(4)]

    def split_rows(xs, r, start):
        vregs = [rest[r + q] for q in range(4)]
        for k in range(4):
            tiles = swap_lane_pairs([z[tile_at(bases[k] + v), :] for v in vregs], lane_bits)
            for half in range(2):
                both = jnp.concatenate(tiles[2 * half : 2 * half + 2], axis=0)
                high, low = split_bf16(both)
                rows = pl.ds(start + 16 * half, 16)
                xs[rows, k * 128 : (k + 1) * 128] = high
                xs[rows, 512 + k * 128 : 512 + (k + 1) * 128] = low
                xs[rows, 1024 + k * 128 : 1024 + (k + 1) * 128] = high

    @pl.loop(0, 8)
    def _(i):
        for k in range(2):
            split_rows(xa, i * 8 + k * 4, pl.multiple_of(i * 64 + k * 32, 16))

    @pl.loop(0, 2)
    def _(i):
        for k, (xs, spare) in enumerate(((xa, xb), (xb, xa))):
            block = 2 * i + k
            following = lax.rem(block + 1, 4)
            for r in range(0, 64, 4):
                split_rows(spare, following * 64 + r, 8 * r)
            for half in range(2):
                mixed = jnp.dot(
                    xs[...], weights[:, half * 256 : (half + 1) * 256], preferred_element_type=F32
                )
                for r in range(64):
                    v = rest[block * 64 + r]
                    for q in range(2):
                        result[tile_at(bases[2 * half + q] + v), :] = mixed[
                            8 * r : 8 * r + 8, q * 128 : (q + 1) * 128
                        ]


def find_lane(lanes, which):
    found = jnp.int32(0)
    for k in range(6):
        found = jnp.where(lanes[k] == which, k, found)
    return found


def trace_share(perm, slots, where, sup, out, row_weight, outpos, final, order, tu, tc):
    column_order(perm, order)
    me = where[0]

    def place_of(bit):
        found = jnp.int32(0)
        for i in range(QUBITS):
            found = jnp.where(order[i] == bit, i, found)
        return found

    lane = lax.broadcasted_iota(jnp.int32, (16, 128), 1)
    group = jnp.zeros((16, 128), jnp.int32)
    for j in range(4):
        place = place_of(final[j])
        local = jnp.right_shift(lane, jnp.minimum(place, 5)) & 1
        remote_bit = jnp.right_shift(me, jnp.maximum(place - 6, 0)) & 1
        group = group + jnp.left_shift(jnp.where(place < 6, local, remote_bit), j)
    row16 = lax.broadcasted_iota(jnp.int32, (16, 16), 0)
    col16 = lax.broadcasted_iota(jnp.int32, (16, 16), 1)
    hot = jnp.where(lax.broadcasted_iota(jnp.int32, (16, 128), 0) == group, 1.0, 0.0).astype(F32)
    single = []
    for part in range(2):
        s = sup[1, part]
        tau = s[0:1] + s[5:6] + s[10:11] + s[15:16]
        both = []
        for pair in range(2):
            pick = 4 * (jnp.right_shift(row16, 2 * pair) & 3) + (jnp.right_shift(col16, 2 * pair) & 3)
            value = jnp.zeros((16, 16), F32)
            for uv in range(16):
                value = jnp.where(pick == uv, tau[:, uv : uv + 1], value)
            both.append(value)
        single.append(both)
    real = single[0][0] * single[0][1] - single[1][0] * single[1][1]
    imag = single[0][0] * single[1][1] + single[1][0] * single[0][1]
    exact = functools.partial(jnp.dot, precision=lax.Precision.HIGHEST, preferred_element_type=F32)
    weight = jnp.where(lane < 64, exact(real, hot), -exact(imag, hot))

    fill(tu, [row_weight(final[j]) for j in range(4)])

    def weight_of(bit):
        return jnp.where(outpos[bit] >= 4, row_weight(bit), 0)

    fill(tc, [weight_of(order[i]) for i in range(6)])
    base = jnp.int32(0)
    for i in range(6, QUBITS):
        base = base + weight_of(order[i]) * (jnp.right_shift(me, i - 6) & 1)
    lane1 = lax.broadcasted_iota(jnp.int32, (1, 128), 1) & 63
    sums = jnp.zeros((1, 128), F32)

    def column(c, rows):
        start = base + tc[c]
        found = []
        for u in range(16):
            index = start + tu[u]
            row = slots[jnp.right_shift(index, 3) ^ (me * 8)] + (index & 7)
            found.append(jnp.where(lane1 == c, out[pl.ds(row, 1), :], rows[u]))
        return tuple(found)

    rows = lax.fori_loop(0, 64, column, tuple(sums for _ in range(16)))
    for u in range(16):
        sums = sums + weight[u : u + 1] * rows[u]
    return sums


def middle(perm, lanes, slots, where, sup, x, out, rows_out, share, z, spare, xa, xb, weights,
           final, outpos, loc, occ, rest, major, rv, order, tu, tc, out_of, low_from, low_to,
           high_from, high_to, places, enabled, *groups):
    me = where[0]
    for q in range(QUBITS):
        bit = perm[0, perm[1, q]]
        final[q] = bit
        outpos[bit] = jnp.int32(q)
        loc[q] = jnp.int32(q)
        occ[q] = jnp.int32(q)
    mixes = [perm[0, j] for j in range(4)]

    def mixed_bit(bit):
        found = bit == mixes[0]
        for m in mixes[1:]:
            found = found | (bit == m)
        return found

    everything = [jnp.int32(q) for q in range(QUBITS)]
    stays = lambda bit: outpos[bit] < 6
    best = lambda bit: jnp.logical_not(mixed_bit(bit)) & stays(bit)
    calm = lambda bit: jnp.logical_not(mixed_bit(bit))
    plenty = jnp.int32(0)
    for bit in everything:
        plenty = plenty + jnp.where(best(bit), 1, 0)
    good = lambda bit: jnp.where(plenty >= 3, best(bit), calm(bit))
    plan_sublanes(loc, occ, good, everything, places, enabled)
    mine = me * 8
    regroup(
        lambda row: x[tile_at(slots[jnp.right_shift(row, 3) ^ mine]), :], z, places, enabled, *groups
    )
    count = jnp.int32(0)
    for place in range(3, QUBITS):
        rest[count] = jnp.int32(place)
        count = count + jnp.where(mixed_bit(occ[place]), 0, 1)
    fill(major, [one_shl(loc[m]) for m in mixes[2:]])
    fill(rv, [one_shl(loc[m]) for m in mixes[:2]] + [one_shl(rest[j]) for j in range(6)])
    build_weights(sup, 0, True, lanes, weights)
    channel(z, spare, major, rv, [find_lane(lanes, 4), find_lane(lanes, 5)], xa, xb, weights)
    fixed = lambda bit: stays(bit) & (bit != mixes[0]) & (bit != mixes[1])
    plan_sublanes(loc, occ, fixed, everything, places, enabled)

    @pl.when(enabled[0] + enabled[1] + enabled[2] > 0)
    def _():
        regroup(lambda row: spare[tile_at(row), :], spare, places, enabled, *groups)

    for s in range(3):
        rows_out[s] = outpos[occ[s]]
    count = jnp.int32(3)
    for q in range(6):
        rows_out[count] = jnp.int32(q)
        count = count + jnp.where(loc[final[q]] >= 3, 1, 0)
    for q in range(6, QUBITS):
        out_of[final[q]] = jnp.int32(8 << (q - 6))
    for s in range(3):
        out_of[occ[s]] = jnp.int32(0)
        out_of[final[rows_out[3 + s]]] = jnp.int32(1 << s)
    count = jnp.int32(0)
    for place in range(3, QUBITS):
        rest[count] = jnp.int32(place)
        skip = (loc[mixes[0]] == place) | (loc[mixes[1]] == place)
        count = count + jnp.where(skip, 0, 1)
    fill(low_from, [one_shl(rest[j]) for j in range(3)])
    fill(high_from, [one_shl(rest[3 + j]) for j in range(5)])
    fill(low_to, [out_of[occ[rest[j]]] for j in range(3)])
    fill(high_to, [out_of[occ[rest[3 + j]]] for j in range(5)])
    from_steps = [one_shl(loc[m]) for m in mixes[:2]]
    to_steps = [out_of[m] for m in mixes[:2]]
    from_quad = [0, from_steps[0], from_steps[1], from_steps[0] + from_steps[1]]
    to_quad = [0, to_steps[0], to_steps[1], to_steps[0] + to_steps[1]]

    @pl.loop(0, 32)
    def _(i):
        origin, target = high_from[i], high_to[i]
        for j in range(8):
            start, end = origin + low_from[j], target + low_to[j]
            tiles = swap_lane_pairs([spare[tile_at(start + f), :] for f in from_quad], (4, 5))
            for t, tile in zip(to_quad, tiles):
                out[tile_at(slots[(end + t) ^ mine]), :] = tile

    def row_weight(bit):
        return jnp.where(loc[bit] < 3, one_shl(jnp.minimum(loc[bit], 3)), 8 * out_of[bit])

    share[...] = trace_share(perm, slots, where, sup, out, row_weight, outpos, final, order, tu, tc)


def gather_back(perm, lanes, slots, where, sup, x, out, y, spare, xa, xb, weights,
                order, inv, loc, occ, ta, rv, major, rest, origin, places, enabled, *groups):
    column_order(perm, order)
    for i in range(QUBITS):
        inv[order[i]] = jnp.int32(i)
    for q in range(QUBITS):
        place = inv[perm[0, perm[1, q]]]
        loc[q] = place
        occ[place] = jnp.int32(q)
    me = where[0]

    @pl.loop(0, 16)
    def _(group):
        for q in range(4):
            p = group * 4 + q
            apart = (p ^ me) * 8
            tiles = [
                x[tile_at(slots[start + j]), :] for start in (apart, apart ^ 512) for j in range(PARTS)
            ]
            turned = jnp.concatenate(tiles, axis=0).T
            real, imag = turned[:64], turned[64:]
            start = pl.multiple_of(p * 64, 64)
            y[pl.ds(start, 64), :] = jnp.concatenate([real[:, :64], imag[:, :64]], axis=1)
            y[pl.ds(start + 4096, 64), :] = jnp.concatenate([real[:, 64:], imag[:, 64:]], axis=1)

    for sub in range(3):
        inside = loc[4 + sub] < 3
        enabled[sub] = jnp.where(inside, 0, 1)
        places[sub] = loc[4 + sub]
    for sub in range(3):
        free = jnp.int32(0)
        for _ in range(3):
            taken = jnp.bool_(False)
            for k in range(3):
                taken = taken | ((enabled[k] == 0) & (places[k] == free))
                if k < sub:
                    taken = taken | ((enabled[k] == 1) & (origin[k] == free))
            free = free + jnp.where(taken, 1, 0)
        origin[sub] = jnp.where(enabled[sub] == 1, free, places[sub])
    leaving = [occ[origin[sub]] for sub in range(3)]
    for sub in range(3):

        @pl.when(enabled[sub] == 1)
        def _():
            loc[leaving[sub]] = places[sub]

        loc[4 + sub] = jnp.int32(sub)
    regroup(lambda row: y[tile_at(row), :], y, places, enabled, *groups, origin=origin)
    fill(ta, [one_shl(loc[q]) for q in range(4)])
    fill(rv, [one_shl(loc[q]) for q in range(7, QUBITS)])
    fill(major, [one_shl(loc[q]) for q in range(2, 4)])
    fill(rest, [one_shl(loc[q]) for q in (0, 1, 7, 8, 9, 10, 11, 12)])
    build_weights(sup, 1, False, lanes, weights)
    channel(y, spare, major, rest, [find_lane(lanes, 4), find_lane(lanes, 5)], xa, xb, weights)

    sublane = lax.broadcasted_iota(jnp.int32, (8, 128), 0)

    @pl.loop(0, 16)
    def _(group):
        for q in range(4):
            t = group * 4 + q
            base = rv[t]
            tiles = [spare[tile_at(base + ta[b]), :] for b in range(16)]
            for b in range(0, 16, 4):
                tiles[b : b + 4] = swap_lane_pairs(tiles[b : b + 4], (4, 5))
            for k in range(3):
                step = 1 << k
                keep = (sublane & step) == 0
                for b in range(16):
                    if not b & step:
                        tiles[b], tiles[b + step] = swap_rows(
                            tiles[b], tiles[b + step], k, keep, jnp.logical_not(keep)
                        )
            ordered = [tiles[8 * (v % 2) + v // 2] for v in range(16)]
            columns = pl.ds(pl.multiple_of(t * 128, 128), 128)
            turned = jnp.concatenate(ordered, axis=0).T
            out[0, :, columns] = turned[:64]
            out[1, :, columns] = turned[64:]


LINKS = 6
PARTS = 8


def part_links(part):
    return [(t, (part + t) % 8) for t in range(8) if (part + t) % 8 < LINKS]


def slot_table():
    low_high = ((4, 5), (6, 0), (2, 3))
    table = np.zeros((PARTS, 128), np.int32)
    for part in range(PARTS):
        place = {link: 1 << (5 - s) for s, (_, link) in enumerate(part_links(part))}
        weight = [0] * 7
        weight[1] = 512
        for axis, (low, high) in enumerate(low_high):
            weight[low] = place[2 * axis]
            weight[high] = place[2 * axis] | place[2 * axis + 1]
        for device in range(128):
            for bit in range(7):
                if device >> bit & 1:
                    table[part, device] ^= weight[bit]
        table[part] += 64 * part
    return 8 * table.T.reshape(-1)


def swap_all(with_sum, *refs):
    if with_sum:
        x, mine, out, total, shares, share_send, share_recv, *refs = refs
    else:
        x, out, *refs = refs
    held, (send, recv, first_send, first_recv, out_sem) = refs[:7], refs[7:]
    hi = lax.axis_index("hi")
    grp = lax.axis_index("grp")
    bits = [lax.rem(hi // (1 << k), 2) for k in range(6)]

    def flip(k):
        return (1 - 2 * bits[k]) * (1 << k)

    core = {"hi": hi + flip(0), "grp": grp}
    link_device = [
        {"hi": hi + flip(3), "grp": grp},
        {"hi": hi + flip(3) + flip(4), "grp": grp},
        {"hi": hi + flip(5), "grp": grp},
        {"hi": hi + flip(5), "grp": 1 - grp},
        {"hi": hi + flip(1), "grp": grp},
        {"hi": hi + flip(1) + flip(2), "grp": grp},
    ]
    mesh_ids = pl.DeviceIdType.MESH
    barrier = pltpu.get_barrier_semaphore()
    for device in [core] + link_device:
        pl.semaphore_signal(barrier, inc=1, device_id=device, device_id_type=mesh_ids)
    pl.semaphore_wait(barrier, 7)

    def remote(src, dst, send_sem, recv_sem, device):
        return pltpu.make_async_remote_copy(
            src_ref=src, dst_ref=dst, send_sem=send_sem, recv_sem=recv_sem,
            device_id=device, device_id_type=mesh_ids,
        )

    for p in range(PARTS):
        pltpu.make_async_copy(x.at[0, p], held[0].at[0, p], first_recv.at[0, p]).start()
        remote(x.at[1, p], held[0].at[1, p], first_send.at[p], first_recv.at[1, p], core).start()

    def arrived(h, p, s):
        ref = held[s].at[h, p]
        sem = first_recv.at[h, p] if s == 0 else recv.at[h, p, s - 1]
        pltpu.make_async_copy(ref, ref, sem).wait()

    def pick(s, chosen):
        return tuple(chosen[b] for b in range(1, 7) if b != s)

    def cross(h, p, s, link):
        for j in range(s):
            source = {b: slice(None) for b in range(1, 7)}
            for b in range(j + 1, s):
                source[b] = 0
            source[s] = 1
            target = dict(source)
            if j:
                target[j] = 1
            remote(
                held[j].at[(h, p) + pick(j, source)], held[s].at[(h, p) + pick(s, target)],
                send.at[h, p, s - 1], recv.at[h, p, s - 1], link_device[link],
            ).start()

    def deliver(h, p):
        for j in range(7):
            source = {b: slice(None) if b < j else 0 for b in range(1, 7)}
            target = dict(source)
            if j:
                target[j] = 1
            pltpu.make_async_copy(
                held[j].at[(h, p) + pick(j, source)],
                out.at[(h, p) + tuple(target[b] for b in range(1, 7))],
                out_sem.at[h, p],
            ).start()

    done = {p: 0 for p in range(PARTS)}
    if with_sum:
        own = pltpu.make_async_copy(mine, shares.at[0], share_recv.at[7])
        own.start()
        own.wait()

        def double(k):
            return remote(
                shares.at[0 : 1 << k], shares.at[1 << k : 2 << k], share_send.at[k],
                share_recv.at[k], ([core] + link_device)[k],
            )

    for t in range(8):

        @pl.loop(0, 2)
        def _(h):
            for p in range(PARTS):
                link = (p + t) % 8
                if link < LINKS:
                    arrived(h, p, done[p])
                    cross(h, p, done[p] + 1, link)

        if with_sum and t < 7:
            if t:
                double(t - 1).wait()
            double(t).start()
        for p in range(PARTS):
            if (p + t) % 8 < LINKS:
                done[p] += 1

    @pl.loop(0, 2)
    def _(h):
        for p in (0, 7, 1, 2, 3, 4, 5, 6):
            arrived(h, p, 6)
            deliver(h, p)

    if with_sum:
        double(6).wait()
        grand = jnp.sum(shares[...], axis=0)
        total[...] = jnp.sum(grand, axis=1, keepdims=True) / ROWS

    for p in range(PARTS):
        pltpu.make_async_copy(x.at[1, p], x.at[1, p], first_send.at[p]).wait()

    @pl.loop(0, 2)
    def _(h):
        for p in range(PARTS):
            for s in range(1, 7):
                ref = held[s].at[h, p]
                pltpu.make_async_copy(ref, ref, send.at[h, p, s - 1]).wait()
            pltpu.make_async_copy(out.at[h, p], out.at[h, p], out_sem.at[h, p]).wait()


def exchange(value, collective_id, share=None):
    two = (2,) * 6
    whole = jax.ShapeDtypeStruct((2, PARTS) + two + (8, 128), F32)
    dma = pltpu.SemaphoreType.DMA
    anywhere = pl.BlockSpec(memory_space=pltpu.HBM)
    vmem = pl.BlockSpec(memory_space=VMEM)
    extra = share is not None
    scratch = [VMEM((2, PARTS) + two + (8, 128), F32)]
    scratch += [VMEM((2, PARTS) + two[:5] + (8, 128), F32) for _ in range(6)]
    scratch += [dma((2, PARTS, 6)), dma((2, PARTS, 6)), dma((PARTS,)), dma((2, PARTS)), dma((2, PARTS))]
    if extra:
        scratch = [VMEM((128, 1, 128), F32), dma((7,)), dma((8,))] + scratch
    result = pl.pallas_call(
        functools.partial(swap_all, extra),
        out_shape=(whole, jax.ShapeDtypeStruct((1, 1), F32)) if extra else whole,
        in_specs=[anywhere] * (1 + extra),
        out_specs=(anywhere, vmem) if extra else anywhere,
        scratch_shapes=scratch,
        compiler_params=pltpu.CompilerParams(
            collective_id=collective_id, has_side_effects=True, vmem_limit_bytes=24 * 2**20
        ),
    )(*((value.reshape(whole.shape), share) if extra else (value.reshape(whole.shape),)))
    if extra:
        return result[0].reshape(8192, 128), result[1]
    return result.reshape(8192, 128)


def call(body, outs, out_smem, n_smem, n_args, scratch, args):
    smem = pl.BlockSpec(memory_space=SMEM)
    vmem = pl.BlockSpec(memory_space=VMEM)
    return pl.pallas_call(
        body,
        out_shape=outs,
        in_specs=[smem if i < n_smem else vmem for i in range(n_args)],
        out_specs=tuple(smem if i in out_smem else vmem for i in range(len(outs))),
        scratch_shapes=scratch,
        compiler_params=pltpu.CompilerParams(vmem_limit_bytes=26 * 2**20),
    )(*args)


def table(*sizes):
    return [SMEM((n,), jnp.int32) for n in sizes]


FULL = VMEM((8192, 128), F32)
GROUPS = (3, 3, 14, 8, 16)
MAP = jax.ShapeDtypeStruct((8,), jnp.int32)
WORK = [FULL, VMEM((512, 1536), BF16), VMEM((512, 1536), BF16), VMEM((1536, 512), BF16)]


def spread_call(perm, slots, where, x):
    return call(
        spread, (jax.ShapeDtypeStruct((8192, 128), F32), MAP), (1,), 3, 4,
        [FULL] + table(14, 14, 14, 8, 64, *GROUPS), (perm, slots, where, x),
    )


def middle_call(perm, lanes, slots, where, sup, x):
    return call(
        middle,
        (jax.ShapeDtypeStruct((8192, 128), F32), MAP, jax.ShapeDtypeStruct((1, 128), F32)),
        (1,), 4, 6,
        [FULL] + WORK + table(13, 13, 13, 13, 14, 4, 256, 14, 16, 64, 13, 8, 8, 32, 32, *GROUPS),
        (perm, lanes, slots, where, sup, x),
    )


def back_call(perm, lanes, slots, where, sup, x):
    return call(
        gather_back, (jax.ShapeDtypeStruct((2, 64, 8192), F32),), (), 4, 6,
        [FULL] + WORK + table(14, 13, 13, 13, 16, 64, 4, 256, 3, *GROUPS),
        (perm, lanes, slots, where, sup, x),
    )[0]


def per_device(rho, perm, superop):
    slots = jnp.asarray(slot_table())
    where = lax.axis_index(HI_GRP).astype(jnp.int32).reshape(1)
    sent, lanes = spread_call(perm, slots, where, rho)
    mid, rows, share = middle_call(perm, lanes, slots, where, superop, exchange(sent, 0))
    last, total = exchange(mid, 1, share)
    return back_call(perm, rows, slots, where, superop, last), total.reshape(())


def solution(mesh):
    in_specs = (P(None, HI_GRP, None), P(), P())
    out_specs = (P(None, HI_GRP, None), P())
    return jax.shard_map(
        per_device, mesh=mesh, in_specs=in_specs, out_specs=out_specs, check_vma=False
    )
```

```python
import functools

import jax
import jax.numpy as jnp
import numpy as np
from jax import lax
from jax.experimental import pallas as pl
from jax.experimental.pallas import tpu as pltpu
from jax.sharding import Mesh
from jax.sharding import PartitionSpec as P

ROWS = 8192
QUBITS = 13
HI_GRP = ("hi", "grp")
F32 = jnp.float32
BF16 = jnp.bfloat16
SMEM = pltpu.SMEM
VMEM = pltpu.VMEM


def fill(table, weights):
    table[0] = jnp.int32(0)
    for k, weight in enumerate(weights):
        for j in range(1 << k):
            table[(1 << k) + j] = table[j] + weight


def one_shl(amount):
    return jnp.left_shift(jnp.int32(1), amount)


def column_order(perm, order):
    for j in range(4):
        order[j] = perm[0, j]
    count = jnp.int32(4)
    for q in range(QUBITS):
        order[count] = jnp.int32(q)
        mine = perm[0, 0] == q
        for j in range(1, 4):
            mine = mine | (perm[0, j] == q)
        count = count + jnp.where(mine, 0, 1)


def tile_at(row):
    return pl.ds(pl.multiple_of(row, 8), 8)


def insert_zero(index, bit):
    low = index & (one_shl(bit) - 1)
    return (index - low) * 2 + low


def swap_rows(lower, upper, sub, keep_lower, keep_upper):
    step = 1 << sub
    return (
        jnp.where(keep_lower, lower, pltpu.roll(upper, step, 0)),
        jnp.where(keep_upper, upper, pltpu.roll(lower, 8 - step, 0)),
    )


def plan_sublanes(loc, occ, wanted, bits, places, enabled):
    for sub in range(3):
        best = jnp.int32(-1)
        for bit in bits:
            best = jnp.where(wanted(bit) & (loc[bit] >= 3), loc[bit], best)
        needed = jnp.logical_not(wanted(occ[sub])) & (best >= 3)
        enabled[sub] = jnp.where(needed, 1, 0)
        places[sub] = best

        @pl.when(needed)
        def _():
            here, there = occ[sub], occ[best]
            occ[sub] = there
            occ[best] = here
            loc[there] = jnp.int32(sub)
            loc[here] = best


def regroup(load, dst, places, enabled, others, group_low, group_high, origin=None):
    for sub in range(3):
        free = jnp.int32(3)
        for _ in range(5):
            taken = jnp.bool_(False)
            for k in range(3):
                if k != sub:
                    taken = taken | ((places[k] == free) & ((enabled[k] == 1) | (k < sub)))
            free = free + jnp.where(taken, 1, 0)
        places[sub] = jnp.where(enabled[sub] == 1, places[sub], free)
    count = jnp.int32(0)
    for place in range(3, QUBITS):
        others[count] = jnp.int32(place)
        mine = (places[0] == place) | (places[1] == place) | (places[2] == place)
        count = count + jnp.where(mine, 0, 1)
    fill(group_low, [one_shl(others[k]) for k in range(3)])
    fill(group_high, [one_shl(others[3 + k]) for k in range(4)])
    steps = [one_shl(places[k]) for k in range(3)]
    sublane = lax.broadcasted_iota(jnp.int32, (8, 128), 0)
    masks = []
    for k in range(3):
        bit = jnp.right_shift(sublane, k) & 1
        off = enabled[k] == 0
        masks.append(((bit == 0) | off, (bit == 1) | off))
    if origin is not None:
        index = jnp.zeros((8, 128), jnp.int32)
        for k in range(3):
            index = index + jnp.left_shift(jnp.right_shift(sublane, k) & 1, origin[k])

    @pl.loop(0, 16)
    def _(i):
        high = group_high[i]
        for j in range(8):
            base = high + group_low[j]
            rows = [base]
            for k in range(3):
                rows = rows + [r + steps[k] for r in rows]
            tiles = [load(r) for r in rows]
            if origin is not None:
                tiles = [jnp.take_along_axis(t, index, axis=0) for t in tiles]
            for k in range(3):
                for v in range(8):
                    if not v >> k & 1:
                        w = v + (1 << k)
                        tiles[v], tiles[w] = swap_rows(tiles[v], tiles[w], k, *masks[k])
            for r, t in zip(rows, tiles):
                dst[tile_at(r), :] = t


def spread(perm, slots, where, x, out, lanes, y, z, order, loc, occ, tc, te, places, enabled, *groups):
    column_order(perm, order)
    top = order[12]
    for q in range(QUBITS):
        place = jnp.where(jnp.int32(q) < top, q, q - 1)
        loc[q] = jnp.where(jnp.int32(q) == top, jnp.int32(13), place)
        occ[place] = jnp.int32(q)
    for q in range(QUBITS):

        @pl.when(jnp.int32(q) != top)
        def _():
            occ[loc[q]] = jnp.int32(q)

    step = one_shl(top - 7)

    @pl.loop(0, 8)
    def _(group):
        for k in range(4):
            m = group * 4 + k
            first = insert_zero(m, top - 7)
            for part in range(2):
                halves = [
                    x[part, :, pl.ds(pl.multiple_of(t * 128, 128), 128)]
                    for t in (first, first + step)
                ]
                start = pl.multiple_of(part * 4096 + m * 128, 128)
                y[pl.ds(start, 128), :] = jnp.concatenate(halves, axis=0).T

    def local(bit):
        found = bit == order[0]
        for i in range(1, 6):
            found = found | (bit == order[i])
        return found

    plan_sublanes(loc, occ, local, [order[i] for i in range(6)], places, enabled)

    regroup(lambda row: y[tile_at(row), :], z, places, enabled, *groups)

    for s in range(3):
        found = jnp.int32(0)
        for i in range(6):
            found = jnp.where(order[i] == occ[s], i, found)
        lanes[s] = found
    count = jnp.int32(3)
    for i in range(6):
        lanes[count] = jnp.int32(i)
        count = count + jnp.where(loc[order[i]] >= 3, 1, 0)
    fill(tc, [one_shl(loc[order[lanes[3 + i]]]) for i in range(3)])
    fill(te, [one_shl(loc[order[6 + i]]) for i in range(6)])
    me = where[0]

    @pl.loop(0, 16)
    def _(group):
        for k in range(4):
            e = group * 4 + k
            base = te[e]
            tiles = [z[tile_at(base + tc[j] + part * 4096), :] for part in range(2) for j in range(8)]
            turned = jnp.concatenate(tiles, axis=0).T
            apart = (e ^ me) * 8
            starts = (apart, apart ^ 512)
            for j in range(16):
                out[tile_at(slots[starts[j // 8] + j % 8]), :] = turned[8 * j : 8 * j + 8]


def split_bf16(value):
    high = value.astype(BF16)
    return high, (value - high.astype(F32)).astype(BF16)


def build_weights(sup, layer, pair, major_is_row, lanes, weights):
    def canonical(lane):
        if lanes is None:
            return lane & 63
        total = jnp.zeros_like(lane)
        for k in range(6):
            total = total + jnp.left_shift(jnp.right_shift(lane, k) & 1, lanes[k])
        return total

    def uv(major, lane):
        minor = jnp.right_shift(lane, 2 * pair) & 3
        return 4 * major + minor if major_is_row else 4 * minor + major

    row = lax.broadcasted_iota(jnp.int32, (512, 16), 0)
    col16 = lax.broadcasted_iota(jnp.int32, (512, 16), 1)

    def one_hot(lane):
        hit = uv(jnp.right_shift(row, 7), lane) == col16
        return jnp.where(hit, 1.0, 0.0).astype(BF16)

    expand_out = one_hot(row & 63)
    expand_in = expand_out if lanes is None else one_hot(canonical(row))
    dims = (((1,), (1,)), ((), ()))
    raw_in = lax.broadcasted_iota(jnp.int32, (512, 128), 0) & 127
    lane_in = canonical(raw_in)
    raw_out = lax.broadcasted_iota(jnp.int32, (512, 128), 1)
    keep = 63 & ~(3 << (2 * pair))
    same_rest = (lane_in & keep) == (raw_out & keep)
    part_in = jnp.right_shift(raw_in, 6)
    part_out = jnp.right_shift(raw_out, 6)
    sign = jnp.where(part_out >= part_in, 1.0, -1.0).astype(F32)
    parts = [split_bf16(sup[layer, part]) for part in range(2)]
    for which, starts in enumerate(((0, 512), (1024,))):
        half = [
            lax.dot_general(expand_in, parts[p][which], dims, preferred_element_type=F32).astype(BF16)
            for p in range(2)
        ]
        for block in range(4):
            target = expand_out[block * 128 : (block + 1) * 128]
            real, imag = (
                lax.dot_general(h, target, dims, preferred_element_type=F32) for h in half
            )
            value = jnp.where(part_in == part_out, real, sign * imag)
            value = jnp.where(same_rest, value, 0.0).astype(BF16)
            for begin in starts:
                weights[begin : begin + 512, block * 128 : (block + 1) * 128] = value


def apply_pair(z, result, pair, ta, rv, xa, xb, weights):
    def bases_of(other):
        first = other * 4 if pair == 0 else other
        return [ta[first + (1 if pair == 0 else 4) * k] for k in range(4)]

    def split_rows(bases, xs, r, start):
        vregs = [rv[r], rv[r + 1]]
        for k in range(4):
            both = [z[tile_at(bases[k] + v), :] for v in vregs]
            high, low = split_bf16(jnp.concatenate(both, axis=0))
            rows = pl.ds(start, 16)
            xs[rows, k * 128 : (k + 1) * 128] = high
            xs[rows, 512 + k * 128 : 512 + (k + 1) * 128] = low
            xs[rows, 1024 + k * 128 : 1024 + (k + 1) * 128] = high

    first = bases_of(0)

    @pl.loop(0, 8)
    def _(i):
        for k in range(4):
            split_rows(first, xa, i * 8 + k * 2, pl.multiple_of(i * 64 + k * 16, 16))

    @pl.loop(0, 2)
    def _(i):
        for k, (xs, spare) in enumerate(((xa, xb), (xb, xa))):
            other = 2 * i + k
            following = bases_of(lax.rem(other + 1, 4))
            bases = bases_of(other)
            for r in range(0, 64, 2):
                split_rows(following, spare, r, 8 * r)
            for half in range(2):
                mixed = jnp.dot(
                    xs[...], weights[:, half * 256 : (half + 1) * 256], preferred_element_type=F32
                )
                for r in range(64):
                    v = rv[r]
                    for q in range(2):
                        result[tile_at(bases[2 * half + q] + v), :] = mixed[
                            8 * r : 8 * r + 8, q * 128 : (q + 1) * 128
                        ]


def channel(sup, layer, major_is_row, lanes, z, spare, ta, rv, xa, xb, weights):
    for pair, (source, result) in enumerate(((z, spare), (spare, z))):
        build_weights(sup, layer, pair, major_is_row, lanes if pair == 0 else None, weights)
        apply_pair(source, result, pair, ta, rv, xa, xb, weights)


def trace_share(perm, slots, where, sup, out, row_weight, outpos, final, order, tu, tc):
    column_order(perm, order)
    me = where[0]

    def place_of(bit):
        found = jnp.int32(0)
        for i in range(QUBITS):
            found = jnp.where(order[i] == bit, i, found)
        return found

    lane = lax.broadcasted_iota(jnp.int32, (16, 128), 1)
    group = jnp.zeros((16, 128), jnp.int32)
    for j in range(4):
        place = place_of(final[j])
        local = jnp.right_shift(lane, jnp.minimum(place, 5)) & 1
        remote_bit = jnp.right_shift(me, jnp.maximum(place - 6, 0)) & 1
        group = group + jnp.left_shift(jnp.where(place < 6, local, remote_bit), j)
    row16 = lax.broadcasted_iota(jnp.int32, (16, 16), 0)
    col16 = lax.broadcasted_iota(jnp.int32, (16, 16), 1)
    hot = jnp.where(lax.broadcasted_iota(jnp.int32, (16, 128), 0) == group, 1.0, 0.0).astype(F32)
    single = []
    for part in range(2):
        s = sup[1, part]
        tau = s[0:1] + s[5:6] + s[10:11] + s[15:16]
        both = []
        for pair in range(2):
            pick = 4 * (jnp.right_shift(row16, 2 * pair) & 3) + (jnp.right_shift(col16, 2 * pair) & 3)
            value = jnp.zeros((16, 16), F32)
            for uv in range(16):
                value = jnp.where(pick == uv, tau[:, uv : uv + 1], value)
            both.append(value)
        single.append(both)
    real = single[0][0] * single[0][1] - single[1][0] * single[1][1]
    imag = single[0][0] * single[1][1] + single[1][0] * single[0][1]
    exact = functools.partial(jnp.dot, precision=lax.Precision.HIGHEST, preferred_element_type=F32)
    weight = jnp.where(lane < 64, exact(real, hot), -exact(imag, hot))

    fill(tu, [row_weight(final[j]) for j in range(4)])

    def weight_of(bit):
        return jnp.where(outpos[bit] >= 4, row_weight(bit), 0)

    fill(tc, [weight_of(order[i]) for i in range(6)])
    base = jnp.int32(0)
    for i in range(6, QUBITS):
        base = base + weight_of(order[i]) * (jnp.right_shift(me, i - 6) & 1)
    lane1 = lax.broadcasted_iota(jnp.int32, (1, 128), 1) & 63
    sums = jnp.zeros((1, 128), F32)

    def column(c, rows):
        start = base + tc[c]
        found = []
        for u in range(16):
            index = start + tu[u]
            row = slots[jnp.right_shift(index, 3) ^ (me * 8)] + (index & 7)
            found.append(jnp.where(lane1 == c, out[pl.ds(row, 1), :], rows[u]))
        return tuple(found)

    rows = lax.fori_loop(0, 64, column, tuple(sums for _ in range(16)))
    for u in range(16):
        sums = sums + weight[u : u + 1] * rows[u]
    return sums


def middle(perm, lanes, slots, where, sup, x, out, rows_out, share, z, spare, xa, xb, weights,
           final, outpos, loc, occ, rest, major, rv, order, tu, tc, out_of, low_from, low_to,
           high_from, high_to, places, enabled, *groups):
    me = where[0]
    for q in range(QUBITS):
        bit = perm[0, perm[1, q]]
        final[q] = bit
        outpos[bit] = jnp.int32(q)
        loc[q] = jnp.int32(q)
        occ[q] = jnp.int32(q)
    mixes = [perm[0, j] for j in range(4)]

    def mixed_bit(bit):
        found = bit == mixes[0]
        for m in mixes[1:]:
            found = found | (bit == m)
        return found

    everything = [jnp.int32(q) for q in range(QUBITS)]
    stays = lambda bit: outpos[bit] < 6
    best = lambda bit: jnp.logical_not(mixed_bit(bit)) & stays(bit)
    calm = lambda bit: jnp.logical_not(mixed_bit(bit))
    plenty = jnp.int32(0)
    for bit in everything:
        plenty = plenty + jnp.where(best(bit), 1, 0)
    good = lambda bit: jnp.where(plenty >= 3, best(bit), calm(bit))
    plan_sublanes(loc, occ, good, everything, places, enabled)
    mine = me * 8
    regroup(
        lambda row: x[tile_at(slots[jnp.right_shift(row, 3) ^ mine]), :], z, places, enabled, *groups
    )
    count = jnp.int32(0)
    for place in range(3, QUBITS):
        rest[count] = jnp.int32(place)
        count = count + jnp.where(mixed_bit(occ[place]), 0, 1)
    fill(major, [one_shl(loc[m]) for m in mixes])
    fill(rv, [one_shl(rest[j]) for j in range(6)])
    channel(sup, 0, True, lanes, z, spare, major, rv, xa, xb, weights)
    plan_sublanes(loc, occ, stays, everything, places, enabled)

    @pl.when(enabled[0] + enabled[1] + enabled[2] > 0)
    def _():
        regroup(lambda row: z[tile_at(row), :], z, places, enabled, *groups)

    for s in range(3):
        rows_out[s] = outpos[occ[s]]
    count = jnp.int32(3)
    for q in range(6):
        rows_out[count] = jnp.int32(q)
        count = count + jnp.where(loc[final[q]] >= 3, 1, 0)
    for q in range(6, QUBITS):
        out_of[final[q]] = jnp.int32(8 << (q - 6))
    for s in range(3):
        out_of[occ[s]] = jnp.int32(0)
        out_of[final[rows_out[3 + s]]] = jnp.int32(1 << s)
    fill(low_from, [one_shl(3 + j) for j in range(5)])
    fill(high_from, [one_shl(8 + j) for j in range(5)])
    fill(low_to, [out_of[occ[3 + j]] for j in range(5)])
    fill(high_to, [out_of[occ[8 + j]] for j in range(5)])

    @pl.loop(0, 32)
    def _(i):
        origin, target = high_from[i], high_to[i]
        for j in range(32):
            out[tile_at(slots[(target + low_to[j]) ^ mine]), :] = z[tile_at(origin + 8 * j), :]

    def row_weight(bit):
        return jnp.where(loc[bit] < 3, one_shl(jnp.minimum(loc[bit], 3)), 8 * out_of[bit])

    share[...] = trace_share(perm, slots, where, sup, out, row_weight, outpos, final, order, tu, tc)


def gather_back(perm, lanes, slots, where, sup, x, out, y, spare, xa, xb, weights,
                order, inv, loc, occ, ta, rv, origin, places, enabled, *groups):
    column_order(perm, order)
    for i in range(QUBITS):
        inv[order[i]] = jnp.int32(i)
    for q in range(QUBITS):
        place = inv[perm[0, perm[1, q]]]
        loc[q] = place
        occ[place] = jnp.int32(q)
    me = where[0]
    first_half = lax.broadcasted_iota(jnp.int32, (64, 128), 1) < 64

    @pl.loop(0, 16)
    def _(group):
        for q in range(4):
            p = group * 4 + q
            apart = (p ^ me) * 8
            tiles = [
                x[tile_at(slots[start + j]), :] for start in (apart, apart ^ 512) for j in range(PARTS)
            ]
            turned = jnp.concatenate(tiles, axis=0).T
            real, imag = turned[:64], turned[64:]
            start = pl.multiple_of(p * 64, 64)
            moved = pltpu.roll(jnp.where(first_half, imag, real), 64, 1)
            y[pl.ds(start, 64), :] = jnp.where(first_half, real, moved)
            y[pl.ds(start + 4096, 64), :] = jnp.where(first_half, moved, imag)

    for sub in range(3):
        inside = loc[4 + sub] < 3
        enabled[sub] = jnp.where(inside, 0, 1)
        places[sub] = loc[4 + sub]
    for sub in range(3):
        free = jnp.int32(0)
        for _ in range(3):
            taken = jnp.bool_(False)
            for k in range(3):
                taken = taken | ((enabled[k] == 0) & (places[k] == free))
                if k < sub:
                    taken = taken | ((enabled[k] == 1) & (origin[k] == free))
            free = free + jnp.where(taken, 1, 0)
        origin[sub] = jnp.where(enabled[sub] == 1, free, places[sub])
    leaving = [occ[origin[sub]] for sub in range(3)]
    for sub in range(3):

        @pl.when(enabled[sub] == 1)
        def _():
            loc[leaving[sub]] = places[sub]

        loc[4 + sub] = jnp.int32(sub)
    regroup(lambda row: y[tile_at(row), :], spare, places, enabled, *groups, origin=origin)
    fill(ta, [one_shl(loc[q]) for q in range(4)])
    fill(rv, [one_shl(loc[q]) for q in range(7, QUBITS)])
    channel(sup, 1, False, lanes, spare, y, ta, rv, xa, xb, weights)

    sublane = lax.broadcasted_iota(jnp.int32, (8, 128), 0)

    @pl.loop(0, 16)
    def _(group):
        for q in range(4):
            t = group * 4 + q
            base = rv[t]
            tiles = [spare[tile_at(base + ta[b]), :] for b in range(16)]
            for k in range(3):
                step = 1 << k
                keep = (sublane & step) == 0
                for b in range(16):
                    if not b & step:
                        tiles[b], tiles[b + step] = swap_rows(
                            tiles[b], tiles[b + step], k, keep, jnp.logical_not(keep)
                        )
            ordered = [tiles[8 * (v % 2) + v // 2] for v in range(16)]
            columns = pl.ds(pl.multiple_of(t * 128, 128), 128)
            turned = jnp.concatenate(ordered, axis=0).T
            out[0, :, columns] = turned[:64]
            out[1, :, columns] = turned[64:]


LINKS = 6
PARTS = 8


def part_links(part):
    return [(t, (part + t) % 8) for t in range(8) if (part + t) % 8 < LINKS]


def slot_table():
    low_high = ((4, 5), (6, 0), (2, 3))
    table = np.zeros((PARTS, 128), np.int32)
    for part in range(PARTS):
        place = {link: 1 << (5 - s) for s, (_, link) in enumerate(part_links(part))}
        weight = [0] * 7
        weight[1] = 512
        for axis, (low, high) in enumerate(low_high):
            weight[low] = place[2 * axis]
            weight[high] = place[2 * axis] | place[2 * axis + 1]
        for device in range(128):
            for bit in range(7):
                if device >> bit & 1:
                    table[part, device] ^= weight[bit]
        table[part] += 64 * part
    return 8 * table.T.reshape(-1)


def swap_all(with_sum, *refs):
    if with_sum:
        x, mine, out, total, shares, share_send, share_recv, *refs = refs
    else:
        x, out, *refs = refs
    held, (send, recv, first_send, first_recv, out_sem) = refs[:7], refs[7:]
    hi = lax.axis_index("hi")
    grp = lax.axis_index("grp")
    bits = [lax.rem(hi // (1 << k), 2) for k in range(6)]

    def flip(k):
        return (1 - 2 * bits[k]) * (1 << k)

    core = {"hi": hi + flip(0), "grp": grp}
    link_device = [
        {"hi": hi + flip(3), "grp": grp},
        {"hi": hi + flip(3) + flip(4), "grp": grp},
        {"hi": hi + flip(5), "grp": grp},
        {"hi": hi + flip(5), "grp": 1 - grp},
        {"hi": hi + flip(1), "grp": grp},
        {"hi": hi + flip(1) + flip(2), "grp": grp},
    ]
    mesh_ids = pl.DeviceIdType.MESH
    barrier = pltpu.get_barrier_semaphore()
    for device in [core] + link_device:
        pl.semaphore_signal(barrier, inc=1, device_id=device, device_id_type=mesh_ids)
    pl.semaphore_wait(barrier, 7)

    def remote(src, dst, send_sem, recv_sem, device):
        return pltpu.make_async_remote_copy(
            src_ref=src, dst_ref=dst, send_sem=send_sem, recv_sem=recv_sem,
            device_id=device, device_id_type=mesh_ids,
        )

    for p in range(PARTS):
        pltpu.make_async_copy(x.at[0, p], held[0].at[0, p], first_recv.at[0, p]).start()
        remote(x.at[1, p], held[0].at[1, p], first_send.at[p], first_recv.at[1, p], core).start()

    def arrived(h, p, s):
        ref = held[s].at[h, p]
        sem = first_recv.at[h, p] if s == 0 else recv.at[h, p, s - 1]
        pltpu.make_async_copy(ref, ref, sem).wait()

    def pick(s, chosen):
        return tuple(chosen[b] for b in range(1, 7) if b != s)

    def cross(h, p, s, link):
        for j in range(s):
            source = {b: slice(None) for b in range(1, 7)}
            for b in range(j + 1, s):
                source[b] = 0
            source[s] = 1
            target = dict(source)
            if j:
                target[j] = 1
            remote(
                held[j].at[(h, p) + pick(j, source)], held[s].at[(h, p) + pick(s, target)],
                send.at[h, p, s - 1], recv.at[h, p, s - 1], link_device[link],
            ).start()

    def deliver(h, p):
        for j in range(7):
            source = {b: slice(None) if b < j else 0 for b in range(1, 7)}
            target = dict(source)
            if j:
                target[j] = 1
            pltpu.make_async_copy(
                held[j].at[(h, p) + pick(j, source)],
                out.at[(h, p) + tuple(target[b] for b in range(1, 7))],
                out_sem.at[h, p],
            ).start()

    done = {p: 0 for p in range(PARTS)}
    if with_sum:
        own = pltpu.make_async_copy(mine, shares.at[0], share_recv.at[7])
        own.start()
        own.wait()

        def double(k):
            return remote(
                shares.at[0 : 1 << k], shares.at[1 << k : 2 << k], share_send.at[k],
                share_recv.at[k], ([core] + link_device)[k],
            )

    for t in range(8):

        @pl.loop(0, 2)
        def _(h):
            for p in range(PARTS):
                link = (p + t) % 8
                if link < LINKS:
                    arrived(h, p, done[p])
                    cross(h, p, done[p] + 1, link)

        if with_sum and t < 7:
            if t:
                double(t - 1).wait()
            double(t).start()
        for p in range(PARTS):
            if (p + t) % 8 < LINKS:
                done[p] += 1

    @pl.loop(0, 2)
    def _(h):
        for p in (0, 7, 1, 2, 3, 4, 5, 6):
            arrived(h, p, 6)
            deliver(h, p)

    if with_sum:
        double(6).wait()
        grand = jnp.sum(shares[...], axis=0)
        total[...] = jnp.sum(grand, axis=1, keepdims=True) / ROWS

    for p in range(PARTS):
        pltpu.make_async_copy(x.at[1, p], x.at[1, p], first_send.at[p]).wait()

    @pl.loop(0, 2)
    def _(h):
        for p in range(PARTS):
            for s in range(1, 7):
                ref = held[s].at[h, p]
                pltpu.make_async_copy(ref, ref, send.at[h, p, s - 1]).wait()
            pltpu.make_async_copy(out.at[h, p], out.at[h, p], out_sem.at[h, p]).wait()


def exchange(value, collective_id, share=None):
    two = (2,) * 6
    whole = jax.ShapeDtypeStruct((2, PARTS) + two + (8, 128), F32)
    dma = pltpu.SemaphoreType.DMA
    anywhere = pl.BlockSpec(memory_space=pltpu.HBM)
    vmem = pl.BlockSpec(memory_space=VMEM)
    extra = share is not None
    scratch = [VMEM((2, PARTS) + two + (8, 128), F32)]
    scratch += [VMEM((2, PARTS) + two[:5] + (8, 128), F32) for _ in range(6)]
    scratch += [dma((2, PARTS, 6)), dma((2, PARTS, 6)), dma((PARTS,)), dma((2, PARTS)), dma((2, PARTS))]
    if extra:
        scratch = [VMEM((128, 1, 128), F32), dma((7,)), dma((8,))] + scratch
    result = pl.pallas_call(
        functools.partial(swap_all, extra),
        out_shape=(whole, jax.ShapeDtypeStruct((1, 1), F32)) if extra else whole,
        in_specs=[anywhere] * (1 + extra),
        out_specs=(anywhere, vmem) if extra else anywhere,
        scratch_shapes=scratch,
        compiler_params=pltpu.CompilerParams(
            collective_id=collective_id, has_side_effects=True, vmem_limit_bytes=24 * 2**20
        ),
    )(*((value.reshape(whole.shape), share) if extra else (value.reshape(whole.shape),)))
    if extra:
        return result[0].reshape(8192, 128), result[1]
    return result.reshape(8192, 128)


def call(body, outs, out_smem, n_smem, n_args, scratch, args):
    smem = pl.BlockSpec(memory_space=SMEM)
    vmem = pl.BlockSpec(memory_space=VMEM)
    return pl.pallas_call(
        body,
        out_shape=outs,
        in_specs=[smem if i < n_smem else vmem for i in range(n_args)],
        out_specs=tuple(smem if i in out_smem else vmem for i in range(len(outs))),
        scratch_shapes=scratch,
        compiler_params=pltpu.CompilerParams(vmem_limit_bytes=26 * 2**20),
    )(*args)


def table(*sizes):
    return [SMEM((n,), jnp.int32) for n in sizes]


FULL = VMEM((8192, 128), F32)
GROUPS = (3, 3, 14, 8, 16)
MAP = jax.ShapeDtypeStruct((8,), jnp.int32)
WORK = [FULL, VMEM((512, 1536), BF16), VMEM((512, 1536), BF16), VMEM((1536, 512), BF16)]


def spread_call(perm, slots, where, x):
    return call(
        spread, (jax.ShapeDtypeStruct((8192, 128), F32), MAP), (1,), 3, 4,
        [FULL, FULL] + table(14, 14, 14, 8, 64, *GROUPS), (perm, slots, where, x),
    )


def middle_call(perm, lanes, slots, where, sup, x):
    return call(
        middle,
        (jax.ShapeDtypeStruct((8192, 128), F32), MAP, jax.ShapeDtypeStruct((1, 128), F32)),
        (1,), 4, 6,
        [FULL] + WORK + table(13, 13, 13, 13, 14, 16, 64, 14, 16, 64, 13, 32, 32, 32, 32, *GROUPS),
        (perm, lanes, slots, where, sup, x),
    )


def back_call(perm, lanes, slots, where, sup, x):
    return call(
        gather_back, (jax.ShapeDtypeStruct((2, 64, 8192), F32),), (), 4, 6,
        [FULL] + WORK + table(14, 13, 13, 13, 16, 64, 3, *GROUPS),
        (perm, lanes, slots, where, sup, x),
    )[0]


def per_device(rho, perm, superop):
    slots = jnp.asarray(slot_table())
    where = lax.axis_index(HI_GRP).astype(jnp.int32).reshape(1)
    sent, lanes = spread_call(perm, slots, where, rho)
    mid, rows, share = middle_call(perm, lanes, slots, where, superop, exchange(sent, 0))
    last, total = exchange(mid, 1, share)
    return back_call(perm, rows, slots, where, superop, last), total.reshape(())


def solution(mesh):
    in_specs = (P(None, HI_GRP, None), P(), P())
    out_specs = (P(None, HI_GRP, None), P())
    return jax.shard_map(
        per_device, mesh=mesh, in_specs=in_specs, out_specs=out_specs, check_vma=False
    )
```

```python
import functools

import jax
import jax.numpy as jnp
import numpy as np
from jax import lax
from jax.experimental import pallas as pl
from jax.experimental.pallas import tpu as pltpu
from jax.sharding import Mesh
from jax.sharding import PartitionSpec as P

ROWS = 8192
QUBITS = 13
HI_GRP = ("hi", "grp")
F32 = jnp.float32
BF16 = jnp.bfloat16
SMEM = pltpu.SMEM
VMEM = pltpu.VMEM


def fill(table, weights):
    table[0] = jnp.int32(0)
    for k, weight in enumerate(weights):
        for j in range(1 << k):
            table[(1 << k) + j] = table[j] + weight


def one_shl(amount):
    return jnp.left_shift(jnp.int32(1), amount)


def column_order(perm, order):
    for j in range(4):
        order[j] = perm[0, j]
    count = jnp.int32(4)
    for q in range(QUBITS):
        order[count] = jnp.int32(q)
        mine = perm[0, 0] == q
        for j in range(1, 4):
            mine = mine | (perm[0, j] == q)
        count = count + jnp.where(mine, 0, 1)


def tile_at(row):
    return pl.ds(pl.multiple_of(row, 8), 8)


def insert_zero(index, bit):
    low = index & (one_shl(bit) - 1)
    return (index - low) * 2 + low


def swap_rows(lower, upper, sub, keep_lower, keep_upper):
    step = 1 << sub
    return (
        jnp.where(keep_lower, lower, pltpu.roll(upper, step, 0)),
        jnp.where(keep_upper, upper, pltpu.roll(lower, 8 - step, 0)),
    )


def plan_sublanes(loc, occ, wanted, bits, places, enabled):
    for sub in range(3):
        best = jnp.int32(-1)
        for bit in bits:
            best = jnp.where(wanted(bit) & (loc[bit] >= 3), loc[bit], best)
        needed = jnp.logical_not(wanted(occ[sub])) & (best >= 3)
        enabled[sub] = jnp.where(needed, 1, 0)
        places[sub] = best

        @pl.when(needed)
        def _():
            here, there = occ[sub], occ[best]
            occ[sub] = there
            occ[best] = here
            loc[there] = jnp.int32(sub)
            loc[here] = best


def regroup(load, dst, places, enabled, others, group_low, group_high, origin=None):
    for sub in range(3):
        free = jnp.int32(3)
        for _ in range(5):
            taken = jnp.bool_(False)
            for k in range(3):
                if k != sub:
                    taken = taken | ((places[k] == free) & ((enabled[k] == 1) | (k < sub)))
            free = free + jnp.where(taken, 1, 0)
        places[sub] = jnp.where(enabled[sub] == 1, places[sub], free)
    count = jnp.int32(0)
    for place in range(3, QUBITS):
        others[count] = jnp.int32(place)
        mine = (places[0] == place) | (places[1] == place) | (places[2] == place)
        count = count + jnp.where(mine, 0, 1)
    fill(group_low, [one_shl(others[k]) for k in range(3)])
    fill(group_high, [one_shl(others[3 + k]) for k in range(4)])
    steps = [one_shl(places[k]) for k in range(3)]
    sublane = lax.broadcasted_iota(jnp.int32, (8, 128), 0)
    masks = []
    for k in range(3):
        bit = jnp.right_shift(sublane, k) & 1
        off = enabled[k] == 0
        masks.append(((bit == 0) | off, (bit == 1) | off))
    if origin is not None:
        index = jnp.zeros((8, 128), jnp.int32)
        for k in range(3):
            index = index + jnp.left_shift(jnp.right_shift(sublane, k) & 1, origin[k])

    @pl.loop(0, 16)
    def _(i):
        high = group_high[i]
        for j in range(8):
            base = high + group_low[j]
            rows = [base]
            for k in range(3):
                rows = rows + [r + steps[k] for r in rows]
            tiles = [load(r) for r in rows]
            if origin is not None:
                tiles = [jnp.take_along_axis(t, index, axis=0) for t in tiles]
            for k in range(3):
                for v in range(8):
                    if not v >> k & 1:
                        w = v + (1 << k)
                        tiles[v], tiles[w] = swap_rows(tiles[v], tiles[w], k, *masks[k])
            for r, t in zip(rows, tiles):
                dst[tile_at(r), :] = t


def spread(perm, slots, where, x, out, lanes, y, z, order, loc, occ, tc, te, places, enabled, *groups):
    column_order(perm, order)
    top = order[12]
    for q in range(QUBITS):
        place = jnp.where(jnp.int32(q) < top, q, q - 1)
        loc[q] = jnp.where(jnp.int32(q) == top, jnp.int32(13), place)
        occ[place] = jnp.int32(q)
    for q in range(QUBITS):

        @pl.when(jnp.int32(q) != top)
        def _():
            occ[loc[q]] = jnp.int32(q)

    step = one_shl(top - 7)

    @pl.loop(0, 8)
    def _(group):
        for k in range(4):
            m = group * 4 + k
            first = insert_zero(m, top - 7)
            for part in range(2):
                halves = [
                    x[part, :, pl.ds(pl.multiple_of(t * 128, 128), 128)]
                    for t in (first, first + step)
                ]
                start = pl.multiple_of(part * 4096 + m * 128, 128)
                y[pl.ds(start, 128), :] = jnp.concatenate(halves, axis=0).T

    def local(bit):
        found = bit == order[0]
        for i in range(1, 6):
            found = found | (bit == order[i])
        return found

    plan_sublanes(loc, occ, local, [order[i] for i in range(6)], places, enabled)

    regroup(lambda row: y[tile_at(row), :], z, places, enabled, *groups)

    for s in range(3):
        found = jnp.int32(0)
        for i in range(6):
            found = jnp.where(order[i] == occ[s], i, found)
        lanes[s] = found
    count = jnp.int32(3)
    for i in range(6):
        lanes[count] = jnp.int32(i)
        count = count + jnp.where(loc[order[i]] >= 3, 1, 0)
    fill(tc, [one_shl(loc[order[lanes[3 + i]]]) for i in range(3)])
    fill(te, [one_shl(loc[order[6 + i]]) for i in range(6)])
    me = where[0]

    @pl.loop(0, 16)
    def _(group):
        for k in range(4):
            e = group * 4 + k
            base = te[e]
            tiles = [z[tile_at(base + tc[j] + part * 4096), :] for part in range(2) for j in range(8)]
            turned = jnp.concatenate(tiles, axis=0).T
            apart = (e ^ me) * 8
            starts = (apart, apart ^ 512)
            for j in range(16):
                out[tile_at(slots[starts[j // 8] + j % 8]), :] = turned[8 * j : 8 * j + 8]


def split_bf16(value):
    high = value.astype(BF16)
    return high, (value - high.astype(F32)).astype(BF16)


def build_weights(sup, layer, pair, major_is_row, lanes, weights):
    def canonical(lane):
        if lanes is None:
            return lane & 63
        total = jnp.zeros_like(lane)
        for k in range(6):
            total = total + jnp.left_shift(jnp.right_shift(lane, k) & 1, lanes[k])
        return total

    def uv(major, lane):
        minor = jnp.right_shift(lane, 2 * pair) & 3
        return 4 * major + minor if major_is_row else 4 * minor + major

    row = lax.broadcasted_iota(jnp.int32, (512, 16), 0)
    col16 = lax.broadcasted_iota(jnp.int32, (512, 16), 1)

    def one_hot(lane):
        hit = uv(jnp.right_shift(row, 7), lane) == col16
        return jnp.where(hit, 1.0, 0.0).astype(BF16)

    expand_out = one_hot(row & 63)
    expand_in = expand_out if lanes is None else one_hot(canonical(row))
    dims = (((1,), (1,)), ((), ()))
    raw_in = lax.broadcasted_iota(jnp.int32, (512, 128), 0) & 127
    lane_in = canonical(raw_in)
    raw_out = lax.broadcasted_iota(jnp.int32, (512, 128), 1)
    keep = 63 & ~(3 << (2 * pair))
    same_rest = (lane_in & keep) == (raw_out & keep)
    part_in = jnp.right_shift(raw_in, 6)
    part_out = jnp.right_shift(raw_out, 6)
    sign = jnp.where(part_out >= part_in, 1.0, -1.0).astype(F32)
    parts = [split_bf16(sup[layer, part]) for part in range(2)]
    for which, starts in enumerate(((0, 512), (1024,))):
        half = [
            lax.dot_general(expand_in, parts[p][which], dims, preferred_element_type=F32).astype(BF16)
            for p in range(2)
        ]
        for block in range(4):
            target = expand_out[block * 128 : (block + 1) * 128]
            real, imag = (
                lax.dot_general(h, target, dims, preferred_element_type=F32) for h in half
            )
            value = jnp.where(part_in == part_out, real, sign * imag)
            value = jnp.where(same_rest, value, 0.0).astype(BF16)
            for begin in starts:
                weights[begin : begin + 512, block * 128 : (block + 1) * 128] = value


def apply_pair(z, result, pair, ta, rv, xa, xb, weights):
    def bases_of(other):
        first = other * 4 if pair == 0 else other
        return [ta[first + (1 if pair == 0 else 4) * k] for k in range(4)]

    def split_rows(bases, xs, r, start):
        vregs = [rv[r], rv[r + 1]]
        for k in range(4):
            both = [z[tile_at(bases[k] + v), :] for v in vregs]
            high, low = split_bf16(jnp.concatenate(both, axis=0))
            rows = pl.ds(start, 16)
            xs[rows, k * 128 : (k + 1) * 128] = high
            xs[rows, 512 + k * 128 : 512 + (k + 1) * 128] = low
            xs[rows, 1024 + k * 128 : 1024 + (k + 1) * 128] = high

    first = bases_of(0)

    @pl.loop(0, 8)
    def _(i):
        for k in range(4):
            split_rows(first, xa, i * 8 + k * 2, pl.multiple_of(i * 64 + k * 16, 16))

    @pl.loop(0, 2)
    def _(i):
        for k, (xs, spare) in enumerate(((xa, xb), (xb, xa))):
            other = 2 * i + k
            following = bases_of(lax.rem(other + 1, 4))
            bases = bases_of(other)
            for r in range(0, 64, 2):
                split_rows(following, spare, r, 8 * r)
            for half in range(2):
                mixed = jnp.dot(
                    xs[...], weights[:, half * 256 : (half + 1) * 256], preferred_element_type=F32
                )
                for r in range(64):
                    v = rv[r]
                    for q in range(2):
                        result[tile_at(bases[2 * half + q] + v), :] = mixed[
                            8 * r : 8 * r + 8, q * 128 : (q + 1) * 128
                        ]


def channel(sup, layer, major_is_row, lanes, z, spare, ta, rv, xa, xb, weights):
    for pair, (source, result) in enumerate(((z, spare), (spare, z))):
        build_weights(sup, layer, pair, major_is_row, lanes if pair == 0 else None, weights)
        apply_pair(source, result, pair, ta, rv, xa, xb, weights)


def trace_share(perm, where, sup, z, loc, outpos, final, order, tu, tc):
    column_order(perm, order)
    me = where[0]

    def place_of(bit):
        found = jnp.int32(0)
        for i in range(QUBITS):
            found = jnp.where(order[i] == bit, i, found)
        return found

    lane = lax.broadcasted_iota(jnp.int32, (16, 128), 1)
    group = jnp.zeros((16, 128), jnp.int32)
    for j in range(4):
        place = place_of(final[j])
        local = jnp.right_shift(lane, jnp.minimum(place, 5)) & 1
        remote_bit = jnp.right_shift(me, jnp.maximum(place - 6, 0)) & 1
        group = group + jnp.left_shift(jnp.where(place < 6, local, remote_bit), j)
    row16 = lax.broadcasted_iota(jnp.int32, (16, 16), 0)
    col16 = lax.broadcasted_iota(jnp.int32, (16, 16), 1)
    hot = jnp.where(lax.broadcasted_iota(jnp.int32, (16, 128), 0) == group, 1.0, 0.0).astype(F32)
    single = []
    for part in range(2):
        s = sup[1, part]
        tau = s[0:1] + s[5:6] + s[10:11] + s[15:16]
        both = []
        for pair in range(2):
            pick = 4 * (jnp.right_shift(row16, 2 * pair) & 3) + (jnp.right_shift(col16, 2 * pair) & 3)
            value = jnp.zeros((16, 16), F32)
            for uv in range(16):
                value = jnp.where(pick == uv, tau[:, uv : uv + 1], value)
            both.append(value)
        single.append(both)
    real = single[0][0] * single[0][1] - single[1][0] * single[1][1]
    imag = single[0][0] * single[1][1] + single[1][0] * single[0][1]
    exact = functools.partial(jnp.dot, precision=lax.Precision.HIGHEST, preferred_element_type=F32)
    weight = jnp.where(lane < 64, exact(real, hot), -exact(imag, hot))

    fill(tu, [one_shl(loc[final[j]]) for j in range(4)])

    def weight_of(bit):
        return jnp.where(outpos[bit] >= 4, one_shl(loc[bit]), 0)

    fill(tc, [weight_of(order[i]) for i in range(6)])
    base = jnp.int32(0)
    for i in range(6, QUBITS):
        base = base + weight_of(order[i]) * (jnp.right_shift(me, i - 6) & 1)
    lane1 = lax.broadcasted_iota(jnp.int32, (1, 128), 1) & 63
    sums = jnp.zeros((1, 128), F32)

    def column(c, rows):
        start = base + tc[c]
        return tuple(
            jnp.where(lane1 == c, z[pl.ds(start + tu[u], 1), :], rows[u]) for u in range(16)
        )

    rows = lax.fori_loop(0, 64, column, tuple(sums for _ in range(16)))
    for u in range(16):
        sums = sums + weight[u : u + 1] * rows[u]
    return sums


def middle(perm, lanes, slots, where, sup, x, out, rows_out, share, z, spare, xa, xb, weights,
           final, outpos, loc, occ, rest, major, rv, order, tu, tc, out_of, low_from, low_to,
           high_from, high_to, places, enabled, *groups):
    me = where[0]
    for q in range(QUBITS):
        bit = perm[0, perm[1, q]]
        final[q] = bit
        outpos[bit] = jnp.int32(q)
        loc[q] = jnp.int32(q)
        occ[q] = jnp.int32(q)
    mixes = [perm[0, j] for j in range(4)]

    def mixed_bit(bit):
        found = bit == mixes[0]
        for m in mixes[1:]:
            found = found | (bit == m)
        return found

    everything = [jnp.int32(q) for q in range(QUBITS)]
    stays = lambda bit: outpos[bit] < 6
    best = lambda bit: jnp.logical_not(mixed_bit(bit)) & stays(bit)
    calm = lambda bit: jnp.logical_not(mixed_bit(bit))
    plenty = jnp.int32(0)
    for bit in everything:
        plenty = plenty + jnp.where(best(bit), 1, 0)
    good = lambda bit: jnp.where(plenty >= 3, best(bit), calm(bit))
    plan_sublanes(loc, occ, good, everything, places, enabled)
    mine = me * 8
    regroup(
        lambda row: x[tile_at(slots[jnp.right_shift(row, 3) ^ mine]), :], z, places, enabled, *groups
    )
    count = jnp.int32(0)
    for place in range(3, QUBITS):
        rest[count] = jnp.int32(place)
        count = count + jnp.where(mixed_bit(occ[place]), 0, 1)
    fill(major, [one_shl(loc[m]) for m in mixes])
    fill(rv, [one_shl(rest[j]) for j in range(6)])
    channel(sup, 0, True, lanes, z, spare, major, rv, xa, xb, weights)
    share[...] = trace_share(perm, where, sup, z, loc, outpos, final, order, tu, tc)
    plan_sublanes(loc, occ, stays, everything, places, enabled)

    @pl.when(enabled[0] + enabled[1] + enabled[2] > 0)
    def _():
        regroup(lambda row: z[tile_at(row), :], z, places, enabled, *groups)

    for s in range(3):
        rows_out[s] = outpos[occ[s]]
    count = jnp.int32(3)
    for q in range(6):
        rows_out[count] = jnp.int32(q)
        count = count + jnp.where(loc[final[q]] >= 3, 1, 0)
    for q in range(6, QUBITS):
        out_of[final[q]] = jnp.int32(8 << (q - 6))
    for s in range(3):
        out_of[occ[s]] = jnp.int32(0)
        out_of[final[rows_out[3 + s]]] = jnp.int32(1 << s)
    fill(low_from, [one_shl(3 + j) for j in range(5)])
    fill(high_from, [one_shl(8 + j) for j in range(5)])
    fill(low_to, [out_of[occ[3 + j]] for j in range(5)])
    fill(high_to, [out_of[occ[8 + j]] for j in range(5)])

    @pl.loop(0, 32)
    def _(i):
        origin, target = high_from[i], high_to[i]
        for j in range(32):
            out[tile_at(slots[(target + low_to[j]) ^ mine]), :] = z[tile_at(origin + 8 * j), :]


def gather_back(perm, lanes, slots, where, sup, x, out, y, spare, xa, xb, weights,
                order, inv, loc, occ, ta, rv, origin, places, enabled, *groups):
    column_order(perm, order)
    for i in range(QUBITS):
        inv[order[i]] = jnp.int32(i)
    for q in range(QUBITS):
        place = inv[perm[0, perm[1, q]]]
        loc[q] = place
        occ[place] = jnp.int32(q)
    me = where[0]
    first_half = lax.broadcasted_iota(jnp.int32, (64, 128), 1) < 64

    @pl.loop(0, 16)
    def _(group):
        for q in range(4):
            p = group * 4 + q
            apart = (p ^ me) * 8
            tiles = [
                x[tile_at(slots[start + j]), :] for start in (apart, apart ^ 512) for j in range(PARTS)
            ]
            turned = jnp.concatenate(tiles, axis=0).T
            real, imag = turned[:64], turned[64:]
            start = pl.multiple_of(p * 64, 64)
            moved = pltpu.roll(jnp.where(first_half, imag, real), 64, 1)
            y[pl.ds(start, 64), :] = jnp.where(first_half, real, moved)
            y[pl.ds(start + 4096, 64), :] = jnp.where(first_half, moved, imag)

    for sub in range(3):
        inside = loc[4 + sub] < 3
        enabled[sub] = jnp.where(inside, 0, 1)
        places[sub] = loc[4 + sub]
    for sub in range(3):
        free = jnp.int32(0)
        for _ in range(3):
            taken = jnp.bool_(False)
            for k in range(3):
                taken = taken | ((enabled[k] == 0) & (places[k] == free))
                if k < sub:
                    taken = taken | ((enabled[k] == 1) & (origin[k] == free))
            free = free + jnp.where(taken, 1, 0)
        origin[sub] = jnp.where(enabled[sub] == 1, free, places[sub])
    leaving = [occ[origin[sub]] for sub in range(3)]
    for sub in range(3):

        @pl.when(enabled[sub] == 1)
        def _():
            loc[leaving[sub]] = places[sub]

        loc[4 + sub] = jnp.int32(sub)
    regroup(lambda row: y[tile_at(row), :], spare, places, enabled, *groups, origin=origin)
    fill(ta, [one_shl(loc[q]) for q in range(4)])
    fill(rv, [one_shl(loc[q]) for q in range(7, QUBITS)])
    channel(sup, 1, False, lanes, spare, y, ta, rv, xa, xb, weights)

    sublane = lax.broadcasted_iota(jnp.int32, (8, 128), 0)

    @pl.loop(0, 16)
    def _(group):
        for q in range(4):
            t = group * 4 + q
            base = rv[t]
            tiles = [spare[tile_at(base + ta[b]), :] for b in range(16)]
            for k in range(3):
                step = 1 << k
                keep = (sublane & step) == 0
                for b in range(16):
                    if not b & step:
                        tiles[b], tiles[b + step] = swap_rows(
                            tiles[b], tiles[b + step], k, keep, jnp.logical_not(keep)
                        )
            ordered = [tiles[8 * (v % 2) + v // 2] for v in range(16)]
            columns = pl.ds(pl.multiple_of(t * 128, 128), 128)
            turned = jnp.concatenate(ordered, axis=0).T
            out[0, :, columns] = turned[:64]
            out[1, :, columns] = turned[64:]


LINKS = 6
PARTS = 8


def part_links(part):
    return [(t, (part + t) % 8) for t in range(8) if (part + t) % 8 < LINKS]


def slot_table():
    low_high = ((4, 5), (6, 0), (2, 3))
    table = np.zeros((PARTS, 128), np.int32)
    for part in range(PARTS):
        place = {link: 1 << (5 - s) for s, (_, link) in enumerate(part_links(part))}
        weight = [0] * 7
        weight[1] = 512
        for axis, (low, high) in enumerate(low_high):
            weight[low] = place[2 * axis]
            weight[high] = place[2 * axis] | place[2 * axis + 1]
        for device in range(128):
            for bit in range(7):
                if device >> bit & 1:
                    table[part, device] ^= weight[bit]
        table[part] += 64 * part
    return 8 * table.T.reshape(-1)


def swap_all(with_sum, *refs):
    if with_sum:
        x, mine, out, total, shares, share_send, share_recv, *refs = refs
    else:
        x, out, *refs = refs
    held, (send, recv, first_send, first_recv, out_sem) = refs[:6], refs[6:]
    hi = lax.axis_index("hi")
    grp = lax.axis_index("grp")
    bits = [lax.rem(hi // (1 << k), 2) for k in range(6)]

    def flip(k):
        return (1 - 2 * bits[k]) * (1 << k)

    core = {"hi": hi + flip(0), "grp": grp}
    link_device = [
        {"hi": hi + flip(3), "grp": grp},
        {"hi": hi + flip(3) + flip(4), "grp": grp},
        {"hi": hi + flip(5), "grp": grp},
        {"hi": hi + flip(5), "grp": 1 - grp},
        {"hi": hi + flip(1), "grp": grp},
        {"hi": hi + flip(1) + flip(2), "grp": grp},
    ]
    mesh_ids = pl.DeviceIdType.MESH
    barrier = pltpu.get_barrier_semaphore()
    for device in [core] + link_device:
        pl.semaphore_signal(barrier, inc=1, device_id=device, device_id_type=mesh_ids)
    pl.semaphore_wait(barrier, 7)

    def remote(src, dst, send_sem, recv_sem, device):
        return pltpu.make_async_remote_copy(
            src_ref=src, dst_ref=dst, send_sem=send_sem, recv_sem=recv_sem,
            device_id=device, device_id_type=mesh_ids,
        )

    for p in range(PARTS):
        remote(x.at[1, p], held[0].at[p], first_send.at[p], first_recv.at[p], core).start()

    def drained(ref, sem):
        pltpu.make_async_copy(ref, ref, sem).wait()

    def stage(h, p, s, index=()):
        if s == 0:
            return x.at[(0, p) + index] if h == 0 else held[0].at[(p,) + index]
        return held[s].at[(h, p) + index]

    def landed(h, p):
        return out.at[(h, p) + (slice(None),) * 5 + (1,)]

    def arrived(h, p, s):
        if s:
            drained(stage(h, p, s) if s < 6 else landed(h, p), recv.at[h, p, s - 1])
        elif h:
            drained(stage(h, p, 0), first_recv.at[p])

    def pick(s, chosen):
        return tuple(chosen[b] for b in range(1, 7) if b != s)

    def cross(h, p, s, link):
        for j in range(s):
            source = {b: slice(None) for b in range(1, 7)}
            for b in range(j + 1, s):
                source[b] = 0
            source[s] = 1
            target = dict(source)
            if j:
                target[j] = 1
            place = (h, p) + pick(s, target)
            remote(
                stage(h, p, j, pick(j, source)), held[s].at[place] if s < 6 else out.at[place + (1,)],
                send.at[h, p, s - 1], recv.at[h, p, s - 1], link_device[link],
            ).start()

    def deliver(h, p):
        for j in range(6):
            source = {b: slice(None) if b < j else 0 for b in range(1, 7)}
            target = dict(source)
            if j:
                target[j] = 1
            pltpu.make_async_copy(
                stage(h, p, j, pick(j, source)),
                out.at[(h, p) + tuple(target[b] for b in range(1, 7))],
                out_sem.at[h, p],
            ).start()

    done = {p: 0 for p in range(PARTS)}
    if with_sum:
        own = pltpu.make_async_copy(mine, shares.at[0], share_recv.at[7])
        own.start()
        own.wait()

        def double(k):
            return remote(
                shares.at[0 : 1 << k], shares.at[1 << k : 2 << k], share_send.at[k],
                share_recv.at[k], ([core] + link_device)[k],
            )

    for t in range(8):
        for h in range(2):
            for p in range(PARTS):
                link = (p + t) % 8
                if link < LINKS:
                    arrived(h, p, done[p])
                    cross(h, p, done[p] + 1, link)
                    if done[p] == 5:
                        deliver(h, p)

        if with_sum and t < 7:
            if t:
                double(t - 1).wait()
            double(t).start()
        for p in range(PARTS):
            if (p + t) % 8 < LINKS:
                done[p] += 1

    for h in range(2):
        for p in range(PARTS):
            arrived(h, p, 6)

    if with_sum:
        double(6).wait()
        grand = jnp.sum(shares[...], axis=0)
        total[...] = jnp.sum(grand, axis=1, keepdims=True) / ROWS

    for p in range(PARTS):
        drained(x.at[1, p], first_send.at[p])
    for h in range(2):
        for p in range(PARTS):
            for s in range(1, 7):
                drained(landed(h, p), send.at[h, p, s - 1])
            drained(out.at[h, p, 0], out_sem.at[h, p])


def exchange(value, collective_id, share=None):
    two = (2,) * 6
    whole = jax.ShapeDtypeStruct((2, PARTS) + two + (8, 128), F32)
    dma = pltpu.SemaphoreType.DMA
    anywhere = pl.BlockSpec(memory_space=pltpu.HBM)
    vmem = pl.BlockSpec(memory_space=VMEM)
    extra = share is not None
    scratch = [VMEM((PARTS,) + two + (8, 128), F32)]
    scratch += [VMEM((2, PARTS) + two[:5] + (8, 128), F32) for _ in range(5)]
    scratch += [dma((2, PARTS, 6)), dma((2, PARTS, 6)), dma((PARTS,)), dma((PARTS,)), dma((2, PARTS))]
    if extra:
        scratch = [VMEM((128, 1, 128), F32), dma((7,)), dma((8,))] + scratch
    result = pl.pallas_call(
        functools.partial(swap_all, extra),
        out_shape=(whole, jax.ShapeDtypeStruct((1, 1), F32)) if extra else whole,
        in_specs=[anywhere] * (1 + extra),
        out_specs=(anywhere, vmem) if extra else anywhere,
        scratch_shapes=scratch,
        compiler_params=pltpu.CompilerParams(
            collective_id=collective_id, has_side_effects=True, vmem_limit_bytes=24 * 2**20
        ),
    )(*((value.reshape(whole.shape), share) if extra else (value.reshape(whole.shape),)))
    if extra:
        return result[0].reshape(8192, 128), result[1]
    return result.reshape(8192, 128)


def call(body, outs, out_smem, n_smem, n_args, scratch, args):
    smem = pl.BlockSpec(memory_space=SMEM)
    vmem = pl.BlockSpec(memory_space=VMEM)
    return pl.pallas_call(
        body,
        out_shape=outs,
        in_specs=[smem if i < n_smem else vmem for i in range(n_args)],
        out_specs=tuple(smem if i in out_smem else vmem for i in range(len(outs))),
        scratch_shapes=scratch,
        compiler_params=pltpu.CompilerParams(vmem_limit_bytes=26 * 2**20),
    )(*args)


def table(*sizes):
    return [SMEM((n,), jnp.int32) for n in sizes]


FULL = VMEM((8192, 128), F32)
GROUPS = (3, 3, 14, 8, 16)
MAP = jax.ShapeDtypeStruct((8,), jnp.int32)
WORK = [FULL, VMEM((512, 1536), BF16), VMEM((512, 1536), BF16), VMEM((1536, 512), BF16)]


def spread_call(perm, slots, where, x):
    return call(
        spread, (jax.ShapeDtypeStruct((8192, 128), F32), MAP), (1,), 3, 4,
        [FULL, FULL] + table(14, 14, 14, 8, 64, *GROUPS), (perm, slots, where, x),
    )


def middle_call(perm, lanes, slots, where, sup, x):
    return call(
        middle,
        (jax.ShapeDtypeStruct((8192, 128), F32), MAP, jax.ShapeDtypeStruct((1, 128), F32)),
        (1,), 4, 6,
        [FULL] + WORK + table(13, 13, 13, 13, 14, 16, 64, 14, 16, 64, 13, 32, 32, 32, 32, *GROUPS),
        (perm, lanes, slots, where, sup, x),
    )


def back_call(perm, lanes, slots, where, sup, x):
    return call(
        gather_back, (jax.ShapeDtypeStruct((2, 64, 8192), F32),), (), 4, 6,
        [FULL] + WORK + table(14, 13, 13, 13, 16, 64, 3, *GROUPS),
        (perm, lanes, slots, where, sup, x),
    )[0]


def per_device(rho, perm, superop):
    slots = jnp.asarray(slot_table())
    where = lax.axis_index(HI_GRP).astype(jnp.int32).reshape(1)
    sent, lanes = spread_call(perm, slots, where, rho)
    mid, rows, share = middle_call(perm, lanes, slots, where, superop, exchange(sent, 0))
    last, total = exchange(mid, 1, share)
    return back_call(perm, rows, slots, where, superop, last), total.reshape(())


def solution(mesh):
    in_specs = (P(None, HI_GRP, None), P(), P())
    out_specs = (P(None, HI_GRP, None), P())
    return jax.shard_map(
        per_device, mesh=mesh, in_specs=in_specs, out_specs=out_specs, check_vma=False
    )
```

```python
import functools

import jax
import jax.numpy as jnp
import numpy as np
from jax import lax
from jax.experimental import pallas as pl
from jax.experimental.pallas import tpu as pltpu
from jax.sharding import Mesh
from jax.sharding import PartitionSpec as P

ROWS = 8192
QUBITS = 13
HI_GRP = ("hi", "grp")
F32 = jnp.float32
BF16 = jnp.bfloat16
SMEM = pltpu.SMEM
VMEM = pltpu.VMEM


def fill(table, weights):
    table[0] = jnp.int32(0)
    for k, weight in enumerate(weights):
        for j in range(1 << k):
            table[(1 << k) + j] = table[j] + weight


def one_shl(amount):
    return jnp.left_shift(jnp.int32(1), amount)


def column_order(perm, order):
    for j in range(4):
        order[j] = perm[0, j]
    count = jnp.int32(4)
    for q in range(QUBITS):
        order[count] = jnp.int32(q)
        mine = perm[0, 0] == q
        for j in range(1, 4):
            mine = mine | (perm[0, j] == q)
        count = count + jnp.where(mine, 0, 1)


def tile_at(row):
    return pl.ds(pl.multiple_of(row, 8), 8)


def insert_zero(index, bit):
    low = index & (one_shl(bit) - 1)
    return (index - low) * 2 + low


def swap_rows(lower, upper, sub, keep_lower, keep_upper):
    step = 1 << sub
    return (
        jnp.where(keep_lower, lower, pltpu.roll(upper, step, 0)),
        jnp.where(keep_upper, upper, pltpu.roll(lower, 8 - step, 0)),
    )


def plan_sublanes(loc, occ, wanted, bits, places, enabled):
    for sub in range(3):
        best = jnp.int32(-1)
        for bit in bits:
            best = jnp.where(wanted(bit) & (loc[bit] >= 3), loc[bit], best)
        needed = jnp.logical_not(wanted(occ[sub])) & (best >= 3)
        enabled[sub] = jnp.where(needed, 1, 0)
        places[sub] = best

        @pl.when(needed)
        def _():
            here, there = occ[sub], occ[best]
            occ[sub] = there
            occ[best] = here
            loc[there] = jnp.int32(sub)
            loc[here] = best


def regroup(load, dst, places, enabled, others, group_low, group_high, origin=None):
    for sub in range(3):
        free = jnp.int32(3)
        for _ in range(5):
            taken = jnp.bool_(False)
            for k in range(3):
                if k != sub:
                    taken = taken | ((places[k] == free) & ((enabled[k] == 1) | (k < sub)))
            free = free + jnp.where(taken, 1, 0)
        places[sub] = jnp.where(enabled[sub] == 1, places[sub], free)
    count = jnp.int32(0)
    for place in range(3, QUBITS):
        others[count] = jnp.int32(place)
        mine = (places[0] == place) | (places[1] == place) | (places[2] == place)
        count = count + jnp.where(mine, 0, 1)
    fill(group_low, [one_shl(others[k]) for k in range(3)])
    fill(group_high, [one_shl(others[3 + k]) for k in range(4)])
    steps = [one_shl(places[k]) for k in range(3)]
    sublane = lax.broadcasted_iota(jnp.int32, (8, 128), 0)
    masks = []
    for k in range(3):
        bit = jnp.right_shift(sublane, k) & 1
        off = enabled[k] == 0
        masks.append(((bit == 0) | off, (bit == 1) | off))
    if origin is not None:
        index = jnp.zeros((8, 128), jnp.int32)
        for k in range(3):
            index = index + jnp.left_shift(jnp.right_shift(sublane, k) & 1, origin[k])

    @pl.loop(0, 16)
    def _(i):
        high = group_high[i]
        for j in range(8):
            base = high + group_low[j]
            rows = [base]
            for k in range(3):
                rows = rows + [r + steps[k] for r in rows]
            tiles = [load(r) for r in rows]
            if origin is not None:
                tiles = [jnp.take_along_axis(t, index, axis=0) for t in tiles]
            for k in range(3):
                for v in range(8):
                    if not v >> k & 1:
                        w = v + (1 << k)
                        tiles[v], tiles[w] = swap_rows(tiles[v], tiles[w], k, *masks[k])
            for r, t in zip(rows, tiles):
                dst[tile_at(r), :] = t


def spread(perm, slots, where, x, out, lanes, y, z, order, loc, occ, tc, te, places, enabled, *groups):
    column_order(perm, order)
    top = order[12]
    for q in range(QUBITS):
        place = jnp.where(jnp.int32(q) < top, q, q - 1)
        loc[q] = jnp.where(jnp.int32(q) == top, jnp.int32(13), place)
        occ[place] = jnp.int32(q)
    for q in range(QUBITS):

        @pl.when(jnp.int32(q) != top)
        def _():
            occ[loc[q]] = jnp.int32(q)

    step = one_shl(top - 7)

    @pl.loop(0, 8)
    def _(group):
        for k in range(4):
            m = group * 4 + k
            first = insert_zero(m, top - 7)
            for part in range(2):
                halves = [
                    x[part, :, pl.ds(pl.multiple_of(t * 128, 128), 128)]
                    for t in (first, first + step)
                ]
                start = pl.multiple_of(part * 4096 + m * 128, 128)
                y[pl.ds(start, 128), :] = jnp.concatenate(halves, axis=0).T

    def local(bit):
        found = bit == order[0]
        for i in range(1, 6):
            found = found | (bit == order[i])
        return found

    plan_sublanes(loc, occ, local, [order[i] for i in range(6)], places, enabled)

    regroup(lambda row: y[tile_at(row), :], z, places, enabled, *groups)

    for s in range(3):
        found = jnp.int32(0)
        for i in range(6):
            found = jnp.where(order[i] == occ[s], i, found)
        lanes[s] = found
    count = jnp.int32(3)
    for i in range(6):
        lanes[count] = jnp.int32(i)
        count = count + jnp.where(loc[order[i]] >= 3, 1, 0)
    fill(tc, [one_shl(loc[order[lanes[3 + i]]]) for i in range(3)])
    fill(te, [one_shl(loc[order[6 + i]]) for i in range(6)])
    me = where[0]

    @pl.loop(0, 16)
    def _(group):
        for k in range(4):
            e = group * 4 + k
            base = te[e]
            tiles = [z[tile_at(base + tc[j] + part * 4096), :] for part in range(2) for j in range(8)]
            turned = jnp.concatenate(tiles, axis=0).T
            apart = (e ^ me) * 8
            starts = (apart, apart ^ 512)
            for j in range(16):
                out[tile_at(slots[starts[j // 8] + j % 8]), :] = turned[8 * j : 8 * j + 8]


def split_bf16(value):
    high = value.astype(BF16)
    return high, (value - high.astype(F32)).astype(BF16)


def build_weights(sup, layer, pair, major_is_row, lanes, weights):
    def canonical(lane):
        if lanes is None:
            return lane & 63
        total = jnp.zeros_like(lane)
        for k in range(6):
            total = total + jnp.left_shift(jnp.right_shift(lane, k) & 1, lanes[k])
        return total

    def uv(major, lane):
        minor = jnp.right_shift(lane, 2 * pair) & 3
        return 4 * major + minor if major_is_row else 4 * minor + major

    row = lax.broadcasted_iota(jnp.int32, (512, 16), 0)
    col16 = lax.broadcasted_iota(jnp.int32, (512, 16), 1)

    def one_hot(lane):
        hit = uv(jnp.right_shift(row, 7), lane) == col16
        return jnp.where(hit, 1.0, 0.0).astype(BF16)

    expand_out = one_hot(row & 63)
    expand_in = expand_out if lanes is None else one_hot(canonical(row))
    dims = (((1,), (1,)), ((), ()))
    raw_in = lax.broadcasted_iota(jnp.int32, (512, 128), 0) & 127
    lane_in = canonical(raw_in)
    raw_out = lax.broadcasted_iota(jnp.int32, (512, 128), 1)
    keep = 63 & ~(3 << (2 * pair))
    same_rest = (lane_in & keep) == (raw_out & keep)
    part_in = jnp.right_shift(raw_in, 6)
    part_out = jnp.right_shift(raw_out, 6)
    sign = jnp.where(part_out >= part_in, 1.0, -1.0).astype(F32)
    parts = [split_bf16(sup[layer, part]) for part in range(2)]
    for which, starts in enumerate(((0, 512), (1024,))):
        half = [
            lax.dot_general(expand_in, parts[p][which], dims, preferred_element_type=F32).astype(BF16)
            for p in range(2)
        ]
        for block in range(4):
            target = expand_out[block * 128 : (block + 1) * 128]
            real, imag = (
                lax.dot_general(h, target, dims, preferred_element_type=F32) for h in half
            )
            value = jnp.where(part_in == part_out, real, sign * imag)
            value = jnp.where(same_rest, value, 0.0).astype(BF16)
            for begin in starts:
                weights[begin : begin + 512, block * 128 : (block + 1) * 128] = value


def apply_pair(z, result, pair, ta, rv, xa, xb, weights):
    def bases_of(other):
        first = other * 4 if pair == 0 else other
        return [ta[first + (1 if pair == 0 else 4) * k] for k in range(4)]

    def split_rows(bases, xs, r, start):
        vregs = [rv[r], rv[r + 1]]
        for k in range(4):
            both = [z[tile_at(bases[k] + v), :] for v in vregs]
            high, low = split_bf16(jnp.concatenate(both, axis=0))
            rows = pl.ds(start, 16)
            xs[rows, k * 128 : (k + 1) * 128] = high
            xs[rows, 512 + k * 128 : 512 + (k + 1) * 128] = low
            xs[rows, 1024 + k * 128 : 1024 + (k + 1) * 128] = high

    first = bases_of(0)

    @pl.loop(0, 8)
    def _(i):
        for k in range(4):
            split_rows(first, xa, i * 8 + k * 2, pl.multiple_of(i * 64 + k * 16, 16))

    @pl.loop(0, 2)
    def _(i):
        for k, (xs, spare) in enumerate(((xa, xb), (xb, xa))):
            other = 2 * i + k
            following = bases_of(lax.rem(other + 1, 4))
            bases = bases_of(other)
            for r in range(0, 64, 2):
                split_rows(following, spare, r, 8 * r)
            for half in range(2):
                mixed = jnp.dot(
                    xs[...], weights[:, half * 256 : (half + 1) * 256], preferred_element_type=F32
                )
                for r in range(64):
                    v = rv[r]
                    for q in range(2):
                        result[tile_at(bases[2 * half + q] + v), :] = mixed[
                            8 * r : 8 * r + 8, q * 128 : (q + 1) * 128
                        ]


def channel(z, spare, ta, rv, xa, xb, weights):
    for pair, (source, result) in enumerate(((z, spare), (spare, z))):
        apply_pair(source, result, pair, ta, rv, xa, xb, weights[pair])


def trace_share(perm, where, sup, z, loc, outpos, final, order, tu, tc):
    column_order(perm, order)
    me = where[0]

    def place_of(bit):
        found = jnp.int32(0)
        for i in range(QUBITS):
            found = jnp.where(order[i] == bit, i, found)
        return found

    lane = lax.broadcasted_iota(jnp.int32, (16, 128), 1)
    group = jnp.zeros((16, 128), jnp.int32)
    for j in range(4):
        place = place_of(final[j])
        local = jnp.right_shift(lane, jnp.minimum(place, 5)) & 1
        remote_bit = jnp.right_shift(me, jnp.maximum(place - 6, 0)) & 1
        group = group + jnp.left_shift(jnp.where(place < 6, local, remote_bit), j)
    row16 = lax.broadcasted_iota(jnp.int32, (16, 16), 0)
    col16 = lax.broadcasted_iota(jnp.int32, (16, 16), 1)
    hot = jnp.where(lax.broadcasted_iota(jnp.int32, (16, 128), 0) == group, 1.0, 0.0).astype(F32)
    single = []
    for part in range(2):
        s = sup[1, part]
        tau = s[0:1] + s[5:6] + s[10:11] + s[15:16]
        both = []
        for pair in range(2):
            pick = 4 * (jnp.right_shift(row16, 2 * pair) & 3) + (jnp.right_shift(col16, 2 * pair) & 3)
            value = jnp.zeros((16, 16), F32)
            for uv in range(16):
                value = jnp.where(pick == uv, tau[:, uv : uv + 1], value)
            both.append(value)
        single.append(both)
    real = single[0][0] * single[0][1] - single[1][0] * single[1][1]
    imag = single[0][0] * single[1][1] + single[1][0] * single[0][1]
    exact = functools.partial(jnp.dot, precision=lax.Precision.HIGHEST, preferred_element_type=F32)
    weight = jnp.where(lane < 64, exact(real, hot), -exact(imag, hot))

    fill(tu, [one_shl(loc[final[j]]) for j in range(4)])

    def weight_of(bit):
        return jnp.where(outpos[bit] >= 4, one_shl(loc[bit]), 0)

    fill(tc, [weight_of(order[i]) for i in range(6)])
    base = jnp.int32(0)
    for i in range(6, QUBITS):
        base = base + weight_of(order[i]) * (jnp.right_shift(me, i - 6) & 1)
    lane1 = lax.broadcasted_iota(jnp.int32, (1, 128), 1) & 63
    sums = jnp.zeros((1, 128), F32)

    def column(c, rows):
        start = base + tc[c]
        return tuple(
            jnp.where(lane1 == c, z[pl.ds(start + tu[u], 1), :], rows[u]) for u in range(16)
        )

    rows = lax.fori_loop(0, 64, column, tuple(sums for _ in range(16)))
    for u in range(16):
        sums = sums + weight[u : u + 1] * rows[u]
    return sums


def middle(perm, slots, where, sup, x, w0, w1, out, rows_out, share, z, spare, xa, xb,
           final, outpos, loc, occ, rest, major, rv, order, tu, tc, out_of, low_from, low_to,
           high_from, high_to, places, enabled, *groups):
    me = where[0]
    for q in range(QUBITS):
        bit = perm[0, perm[1, q]]
        final[q] = bit
        outpos[bit] = jnp.int32(q)
        loc[q] = jnp.int32(q)
        occ[q] = jnp.int32(q)
    mixes = [perm[0, j] for j in range(4)]

    def mixed_bit(bit):
        found = bit == mixes[0]
        for m in mixes[1:]:
            found = found | (bit == m)
        return found

    everything = [jnp.int32(q) for q in range(QUBITS)]
    stays = lambda bit: outpos[bit] < 6
    best = lambda bit: jnp.logical_not(mixed_bit(bit)) & stays(bit)
    calm = lambda bit: jnp.logical_not(mixed_bit(bit))
    plenty = jnp.int32(0)
    for bit in everything:
        plenty = plenty + jnp.where(best(bit), 1, 0)
    good = lambda bit: jnp.where(plenty >= 3, best(bit), calm(bit))
    plan_sublanes(loc, occ, good, everything, places, enabled)
    mine = me * 8
    regroup(
        lambda row: x[tile_at(slots[jnp.right_shift(row, 3) ^ mine]), :], z, places, enabled, *groups
    )
    count = jnp.int32(0)
    for place in range(3, QUBITS):
        rest[count] = jnp.int32(place)
        count = count + jnp.where(mixed_bit(occ[place]), 0, 1)
    fill(major, [one_shl(loc[m]) for m in mixes])
    fill(rv, [one_shl(rest[j]) for j in range(6)])
    channel(z, spare, major, rv, xa, xb, (w0, w1))
    share[...] = trace_share(perm, where, sup, z, loc, outpos, final, order, tu, tc)
    plan_sublanes(loc, occ, stays, everything, places, enabled)

    @pl.when(enabled[0] + enabled[1] + enabled[2] > 0)
    def _():
        regroup(lambda row: z[tile_at(row), :], z, places, enabled, *groups)

    for s in range(3):
        rows_out[s] = outpos[occ[s]]
    count = jnp.int32(3)
    for q in range(6):
        rows_out[count] = jnp.int32(q)
        count = count + jnp.where(loc[final[q]] >= 3, 1, 0)
    for q in range(6, QUBITS):
        out_of[final[q]] = jnp.int32(8 << (q - 6))
    for s in range(3):
        out_of[occ[s]] = jnp.int32(0)
        out_of[final[rows_out[3 + s]]] = jnp.int32(1 << s)
    fill(low_from, [one_shl(3 + j) for j in range(5)])
    fill(high_from, [one_shl(8 + j) for j in range(5)])
    fill(low_to, [out_of[occ[3 + j]] for j in range(5)])
    fill(high_to, [out_of[occ[8 + j]] for j in range(5)])

    @pl.loop(0, 32)
    def _(i):
        origin, target = high_from[i], high_to[i]
        for j in range(32):
            out[tile_at(slots[(target + low_to[j]) ^ mine]), :] = z[tile_at(origin + 8 * j), :]


def gather_back(perm, slots, where, x, w0, w1, out, y, spare, xa, xb,
                order, inv, loc, occ, ta, rv, origin, places, enabled, *groups):
    column_order(perm, order)
    for i in range(QUBITS):
        inv[order[i]] = jnp.int32(i)
    for q in range(QUBITS):
        place = inv[perm[0, perm[1, q]]]
        loc[q] = place
        occ[place] = jnp.int32(q)
    me = where[0]
    first_half = lax.broadcasted_iota(jnp.int32, (64, 128), 1) < 64

    @pl.loop(0, 16)
    def _(group):
        for q in range(4):
            p = group * 4 + q
            apart = (p ^ me) * 8
            tiles = [
                x[tile_at(slots[start + j]), :] for start in (apart, apart ^ 512) for j in range(PARTS)
            ]
            turned = jnp.concatenate(tiles, axis=0).T
            real, imag = turned[:64], turned[64:]
            start = pl.multiple_of(p * 64, 64)
            moved = pltpu.roll(jnp.where(first_half, imag, real), 64, 1)
            y[pl.ds(start, 64), :] = jnp.where(first_half, real, moved)
            y[pl.ds(start + 4096, 64), :] = jnp.where(first_half, moved, imag)

    for sub in range(3):
        inside = loc[4 + sub] < 3
        enabled[sub] = jnp.where(inside, 0, 1)
        places[sub] = loc[4 + sub]
    for sub in range(3):
        free = jnp.int32(0)
        for _ in range(3):
            taken = jnp.bool_(False)
            for k in range(3):
                taken = taken | ((enabled[k] == 0) & (places[k] == free))
                if k < sub:
                    taken = taken | ((enabled[k] == 1) & (origin[k] == free))
            free = free + jnp.where(taken, 1, 0)
        origin[sub] = jnp.where(enabled[sub] == 1, free, places[sub])
    leaving = [occ[origin[sub]] for sub in range(3)]
    for sub in range(3):

        @pl.when(enabled[sub] == 1)
        def _():
            loc[leaving[sub]] = places[sub]

        loc[4 + sub] = jnp.int32(sub)
    regroup(lambda row: y[tile_at(row), :], spare, places, enabled, *groups, origin=origin)
    fill(ta, [one_shl(loc[q]) for q in range(4)])
    fill(rv, [one_shl(loc[q]) for q in range(7, QUBITS)])
    channel(spare, y, ta, rv, xa, xb, (w0, w1))

    sublane = lax.broadcasted_iota(jnp.int32, (8, 128), 0)

    @pl.loop(0, 16)
    def _(group):
        for q in range(4):
            t = group * 4 + q
            base = rv[t]
            tiles = [spare[tile_at(base + ta[b]), :] for b in range(16)]
            for k in range(3):
                step = 1 << k
                keep = (sublane & step) == 0
                for b in range(16):
                    if not b & step:
                        tiles[b], tiles[b + step] = swap_rows(
                            tiles[b], tiles[b + step], k, keep, jnp.logical_not(keep)
                        )
            ordered = [tiles[8 * (v % 2) + v // 2] for v in range(16)]
            columns = pl.ds(pl.multiple_of(t * 128, 128), 128)
            turned = jnp.concatenate(ordered, axis=0).T
            out[0, :, columns] = turned[:64]
            out[1, :, columns] = turned[64:]


LINKS = 6
PARTS = 8


def part_links(part):
    return [(t, (part + t) % 8) for t in range(8) if (part + t) % 8 < LINKS]


def slot_table():
    low_high = ((4, 5), (6, 0), (2, 3))
    table = np.zeros((PARTS, 128), np.int32)
    for part in range(PARTS):
        place = {link: 1 << (5 - s) for s, (_, link) in enumerate(part_links(part))}
        weight = [0] * 7
        weight[1] = 512
        for axis, (low, high) in enumerate(low_high):
            weight[low] = place[2 * axis]
            weight[high] = place[2 * axis] | place[2 * axis + 1]
        for device in range(128):
            for bit in range(7):
                if device >> bit & 1:
                    table[part, device] ^= weight[bit]
        table[part] += 64 * part
    return 8 * table.T.reshape(-1)


def swap_all(with_sum, *refs):
    if with_sum:
        x, lanes, sup, mine, out, w0, w1, total, shares, share_send, share_recv, *refs = refs
    else:
        x, lanes, sup, out, w0, w1, *refs = refs
    held, (send, recv, first_send, first_recv, out_sem) = refs[:6], refs[6:]
    hi = lax.axis_index("hi")
    grp = lax.axis_index("grp")
    bits = [lax.rem(hi // (1 << k), 2) for k in range(6)]

    def flip(k):
        return (1 - 2 * bits[k]) * (1 << k)

    core = {"hi": hi + flip(0), "grp": grp}
    link_device = [
        {"hi": hi + flip(3), "grp": grp},
        {"hi": hi + flip(3) + flip(4), "grp": grp},
        {"hi": hi + flip(5), "grp": grp},
        {"hi": hi + flip(5), "grp": 1 - grp},
        {"hi": hi + flip(1), "grp": grp},
        {"hi": hi + flip(1) + flip(2), "grp": grp},
    ]
    mesh_ids = pl.DeviceIdType.MESH
    barrier = pltpu.get_barrier_semaphore()
    for device in [core] + link_device:
        pl.semaphore_signal(barrier, inc=1, device_id=device, device_id_type=mesh_ids)
    pl.semaphore_wait(barrier, 7)

    def remote(src, dst, send_sem, recv_sem, device):
        return pltpu.make_async_remote_copy(
            src_ref=src, dst_ref=dst, send_sem=send_sem, recv_sem=recv_sem,
            device_id=device, device_id_type=mesh_ids,
        )

    for p in range(PARTS):
        remote(x.at[1, p], held[0].at[p], first_send.at[p], first_recv.at[p], core).start()

    def drained(ref, sem):
        pltpu.make_async_copy(ref, ref, sem).wait()

    def stage(h, p, s, index=()):
        if s == 0:
            return x.at[(0, p) + index] if h == 0 else held[0].at[(p,) + index]
        return held[s].at[(h, p) + index]

    def landed(h, p):
        return out.at[(h, p) + (slice(None),) * 5 + (1,)]

    def arrived(h, p, s):
        if s:
            drained(stage(h, p, s) if s < 6 else landed(h, p), recv.at[h, p, s - 1])
        elif h:
            drained(stage(h, p, 0), first_recv.at[p])

    def pick(s, chosen):
        return tuple(chosen[b] for b in range(1, 7) if b != s)

    def cross(h, p, s, link):
        for j in range(s):
            source = {b: slice(None) for b in range(1, 7)}
            for b in range(j + 1, s):
                source[b] = 0
            source[s] = 1
            target = dict(source)
            if j:
                target[j] = 1
            place = (h, p) + pick(s, target)
            remote(
                stage(h, p, j, pick(j, source)), held[s].at[place] if s < 6 else out.at[place + (1,)],
                send.at[h, p, s - 1], recv.at[h, p, s - 1], link_device[link],
            ).start()

    def deliver(h, p):
        for j in range(6):
            source = {b: slice(None) if b < j else 0 for b in range(1, 7)}
            target = dict(source)
            if j:
                target[j] = 1
            pltpu.make_async_copy(
                stage(h, p, j, pick(j, source)),
                out.at[(h, p) + tuple(target[b] for b in range(1, 7))],
                out_sem.at[h, p],
            ).start()

    done = {p: 0 for p in range(PARTS)}
    if with_sum:
        own = pltpu.make_async_copy(mine, shares.at[0], share_recv.at[7])
        own.start()
        own.wait()

        def double(k):
            return remote(
                shares.at[0 : 1 << k], shares.at[1 << k : 2 << k], share_send.at[k],
                share_recv.at[k], ([core] + link_device)[k],
            )

    for t in range(8):
        for h in range(2):
            for p in range(PARTS):
                link = (p + t) % 8
                if link < LINKS:
                    arrived(h, p, done[p])
                    cross(h, p, done[p] + 1, link)
                    if done[p] == 5:
                        deliver(h, p)

        if t < 2:
            build_weights(
                sup, int(with_sum), t, not with_sum, None if t else lanes, w1 if t else w0
            )
        if with_sum and t < 7:
            if t:
                double(t - 1).wait()
            double(t).start()
        for p in range(PARTS):
            if (p + t) % 8 < LINKS:
                done[p] += 1

    for h in range(2):
        for p in range(PARTS):
            arrived(h, p, 6)

    if with_sum:
        double(6).wait()
        grand = jnp.sum(shares[...], axis=0)
        total[...] = jnp.sum(grand, axis=1, keepdims=True) / ROWS

    for p in range(PARTS):
        drained(x.at[1, p], first_send.at[p])
    for h in range(2):
        for p in range(PARTS):
            for s in range(1, 7):
                drained(landed(h, p), send.at[h, p, s - 1])
            drained(out.at[h, p, 0], out_sem.at[h, p])


def exchange(value, collective_id, lanes, sup, share=None):
    two = (2,) * 6
    whole = jax.ShapeDtypeStruct((2, PARTS) + two + (8, 128), F32)
    dma = pltpu.SemaphoreType.DMA
    anywhere = pl.BlockSpec(memory_space=pltpu.HBM)
    vmem = pl.BlockSpec(memory_space=VMEM)
    extra = share is not None
    scratch = [VMEM((PARTS,) + two + (8, 128), F32)]
    scratch += [VMEM((2, PARTS) + two[:5] + (8, 128), F32) for _ in range(5)]
    scratch += [dma((2, PARTS, 6)), dma((2, PARTS, 6)), dma((PARTS,)), dma((PARTS,)), dma((2, PARTS))]
    if extra:
        scratch = [VMEM((128, 1, 128), F32), dma((7,)), dma((8,))] + scratch
    matrix = jax.ShapeDtypeStruct((1536, 512), BF16)
    smem = pl.BlockSpec(memory_space=SMEM)
    outs = (whole, matrix, matrix) + ((jax.ShapeDtypeStruct((1, 1), F32),) if extra else ())
    result = pl.pallas_call(
        functools.partial(swap_all, extra),
        out_shape=outs,
        in_specs=[anywhere, smem, vmem] + [anywhere] * extra,
        out_specs=(anywhere, vmem, vmem) + (vmem,) * extra,
        scratch_shapes=scratch,
        compiler_params=pltpu.CompilerParams(
            collective_id=collective_id, has_side_effects=True, vmem_limit_bytes=24 * 2**20
        ),
    )(value.reshape(whole.shape), lanes, sup, *((share,) if extra else ()))
    return result[0].reshape(8192, 128), *result[1:]


def call(body, outs, out_smem, n_smem, n_args, scratch, args):
    smem = pl.BlockSpec(memory_space=SMEM)
    vmem = pl.BlockSpec(memory_space=VMEM)
    return pl.pallas_call(
        body,
        out_shape=outs,
        in_specs=[smem if i < n_smem else vmem for i in range(n_args)],
        out_specs=tuple(smem if i in out_smem else vmem for i in range(len(outs))),
        scratch_shapes=scratch,
        compiler_params=pltpu.CompilerParams(vmem_limit_bytes=26 * 2**20),
    )(*args)


def table(*sizes):
    return [SMEM((n,), jnp.int32) for n in sizes]


FULL = VMEM((8192, 128), F32)
GROUPS = (3, 3, 14, 8, 16)
MAP = jax.ShapeDtypeStruct((8,), jnp.int32)
WORK = [FULL, VMEM((512, 1536), BF16), VMEM((512, 1536), BF16)]


def spread_call(perm, slots, where, x):
    return call(
        spread, (jax.ShapeDtypeStruct((8192, 128), F32), MAP), (1,), 3, 4,
        [FULL, FULL] + table(14, 14, 14, 8, 64, *GROUPS), (perm, slots, where, x),
    )


def middle_call(perm, slots, where, sup, x, w0, w1):
    return call(
        middle,
        (jax.ShapeDtypeStruct((8192, 128), F32), MAP, jax.ShapeDtypeStruct((1, 128), F32)),
        (1,), 3, 7,
        [FULL] + WORK + table(13, 13, 13, 13, 14, 16, 64, 14, 16, 64, 13, 32, 32, 32, 32, *GROUPS),
        (perm, slots, where, sup, x, w0, w1),
    )


def back_call(perm, slots, where, x, w0, w1):
    return call(
        gather_back, (jax.ShapeDtypeStruct((2, 64, 8192), F32),), (), 3, 6,
        [FULL] + WORK + table(14, 13, 13, 13, 16, 64, 3, *GROUPS),
        (perm, slots, where, x, w0, w1),
    )[0]


def per_device(rho, perm, superop):
    slots = jnp.asarray(slot_table())
    where = lax.axis_index(HI_GRP).astype(jnp.int32).reshape(1)
    sent, lanes = spread_call(perm, slots, where, rho)
    first = exchange(sent, 0, lanes, superop)
    mid, rows, share = middle_call(perm, slots, where, superop, *first)
    *last, total = exchange(mid, 1, rows, superop, share)
    return back_call(perm, slots, where, *last), total.reshape(())


def solution(mesh):
    in_specs = (P(None, HI_GRP, None), P(), P())
    out_specs = (P(None, HI_GRP, None), P())
    return jax.shard_map(
        per_device, mesh=mesh, in_specs=in_specs, out_specs=out_specs, check_vma=False
    )
```

```python
import functools

import jax
import jax.numpy as jnp
import numpy as np
from jax import lax
from jax.experimental import pallas as pl
from jax.experimental.pallas import tpu as pltpu
from jax.sharding import Mesh
from jax.sharding import PartitionSpec as P

ROWS = 8192
QUBITS = 13
HI_GRP = ("hi", "grp")
F32 = jnp.float32
BF16 = jnp.bfloat16
SMEM = pltpu.SMEM
VMEM = pltpu.VMEM


def fill(table, weights):
    table[0] = jnp.int32(0)
    for k, weight in enumerate(weights):
        for j in range(1 << k):
            table[(1 << k) + j] = table[j] + weight


def one_shl(amount):
    return jnp.left_shift(jnp.int32(1), amount)


def column_order(perm, order):
    for j in range(4):
        order[j] = perm[0, j]
    count = jnp.int32(4)
    for q in range(QUBITS):
        order[count] = jnp.int32(q)
        mine = perm[0, 0] == q
        for j in range(1, 4):
            mine = mine | (perm[0, j] == q)
        count = count + jnp.where(mine, 0, 1)


def tile_at(row):
    return pl.ds(pl.multiple_of(row, 8), 8)


def insert_zero(index, bit):
    low = index & (one_shl(bit) - 1)
    return (index - low) * 2 + low


def swap_rows(lower, upper, sub, keep_lower, keep_upper):
    step = 1 << sub
    return (
        jnp.where(keep_lower, lower, pltpu.roll(upper, step, 0)),
        jnp.where(keep_upper, upper, pltpu.roll(lower, 8 - step, 0)),
    )


def plan_sublanes(loc, occ, wanted, bits, places, enabled):
    for sub in range(3):
        best = jnp.int32(-1)
        for bit in bits:
            best = jnp.where(wanted(bit) & (loc[bit] >= 3), loc[bit], best)
        needed = jnp.logical_not(wanted(occ[sub])) & (best >= 3)
        enabled[sub] = jnp.where(needed, 1, 0)
        places[sub] = best

        @pl.when(needed)
        def _():
            here, there = occ[sub], occ[best]
            occ[sub] = there
            occ[best] = here
            loc[there] = jnp.int32(sub)
            loc[here] = best


def regroup(load, dst, places, enabled, others, group_low, group_high, origin=None):
    for sub in range(3):
        free = jnp.int32(3)
        for _ in range(5):
            taken = jnp.bool_(False)
            for k in range(3):
                if k != sub:
                    taken = taken | ((places[k] == free) & ((enabled[k] == 1) | (k < sub)))
            free = free + jnp.where(taken, 1, 0)
        places[sub] = jnp.where(enabled[sub] == 1, places[sub], free)
    count = jnp.int32(0)
    for place in range(3, QUBITS):
        others[count] = jnp.int32(place)
        mine = (places[0] == place) | (places[1] == place) | (places[2] == place)
        count = count + jnp.where(mine, 0, 1)
    fill(group_low, [one_shl(others[k]) for k in range(3)])
    fill(group_high, [one_shl(others[3 + k]) for k in range(4)])
    steps = [one_shl(places[k]) for k in range(3)]
    sublane = lax.broadcasted_iota(jnp.int32, (8, 128), 0)
    masks = []
    for k in range(3):
        bit = jnp.right_shift(sublane, k) & 1
        off = enabled[k] == 0
        masks.append(((bit == 0) | off, (bit == 1) | off))
    if origin is not None:
        index = jnp.zeros((8, 128), jnp.int32)
        for k in range(3):
            index = index + jnp.left_shift(jnp.right_shift(sublane, k) & 1, origin[k])

    @pl.loop(0, 16)
    def _(i):
        high = group_high[i]
        for j in range(8):
            base = high + group_low[j]
            rows = [base]
            for k in range(3):
                rows = rows + [r + steps[k] for r in rows]
            tiles = [load(r) for r in rows]
            if origin is not None:
                tiles = [jnp.take_along_axis(t, index, axis=0) for t in tiles]
            for k in range(3):
                for v in range(8):
                    if not v >> k & 1:
                        w = v + (1 << k)
                        tiles[v], tiles[w] = swap_rows(tiles[v], tiles[w], k, *masks[k])
            for r, t in zip(rows, tiles):
                dst[tile_at(r), :] = t


def spread(perm, slots, where, x, out, lanes, y, z, order, loc, occ, tc, te, places, enabled, *groups):
    column_order(perm, order)
    top = order[12]
    for q in range(QUBITS):
        place = jnp.where(jnp.int32(q) < top, q, q - 1)
        loc[q] = jnp.where(jnp.int32(q) == top, jnp.int32(13), place)
        occ[place] = jnp.int32(q)
    for q in range(QUBITS):

        @pl.when(jnp.int32(q) != top)
        def _():
            occ[loc[q]] = jnp.int32(q)

    step = one_shl(top - 7)

    @pl.loop(0, 8)
    def _(group):
        for k in range(4):
            m = group * 4 + k
            first = insert_zero(m, top - 7)
            for part in range(2):
                halves = [
                    x[part, :, pl.ds(pl.multiple_of(t * 128, 128), 128)]
                    for t in (first, first + step)
                ]
                start = pl.multiple_of(part * 4096 + m * 128, 128)
                y[pl.ds(start, 128), :] = jnp.concatenate(halves, axis=0).T

    def local(bit):
        found = bit == order[0]
        for i in range(1, 6):
            found = found | (bit == order[i])
        return found

    plan_sublanes(loc, occ, local, [order[i] for i in range(6)], places, enabled)

    regroup(lambda row: y[tile_at(row), :], z, places, enabled, *groups)

    for s in range(3):
        found = jnp.int32(0)
        for i in range(6):
            found = jnp.where(order[i] == occ[s], i, found)
        lanes[s] = found
    count = jnp.int32(3)
    for i in range(6):
        lanes[count] = jnp.int32(i)
        count = count + jnp.where(loc[order[i]] >= 3, 1, 0)
    fill(tc, [one_shl(loc[order[lanes[3 + i]]]) for i in range(3)])
    fill(te, [one_shl(loc[order[6 + i]]) for i in range(6)])
    me = where[0]

    @pl.loop(0, 16)
    def _(group):
        for k in range(4):
            e = group * 4 + k
            base = te[e]
            tiles = [z[tile_at(base + tc[j] + part * 4096), :] for part in range(2) for j in range(8)]
            turned = jnp.concatenate(tiles, axis=0).T
            apart = (e ^ me) * 8
            starts = (apart, apart ^ 512)
            for j in range(16):
                out[tile_at(slots[starts[j // 8] + j % 8]), :] = turned[8 * j : 8 * j + 8]


def split_bf16(value):
    high = value.astype(BF16)
    return high, (value - high.astype(F32)).astype(BF16)


def build_weights(sup, layer, pair, major_is_row, lanes, weights):
    def canonical(lane):
        if lanes is None:
            return lane & 63
        total = jnp.zeros_like(lane)
        for k in range(6):
            total = total + jnp.left_shift(jnp.right_shift(lane, k) & 1, lanes[k])
        return total

    def uv(major, lane):
        minor = jnp.right_shift(lane, 2 * pair) & 3
        return 4 * major + minor if major_is_row else 4 * minor + major

    row = lax.broadcasted_iota(jnp.int32, (512, 16), 0)
    col16 = lax.broadcasted_iota(jnp.int32, (512, 16), 1)

    def one_hot(lane):
        hit = uv(jnp.right_shift(row, 7), lane) == col16
        return jnp.where(hit, 1.0, 0.0).astype(BF16)

    expand_out = one_hot(row & 63)
    expand_in = expand_out if lanes is None else one_hot(canonical(row))
    dims = (((1,), (1,)), ((), ()))
    raw_in = lax.broadcasted_iota(jnp.int32, (512, 128), 0) & 127
    lane_in = canonical(raw_in)
    raw_out = lax.broadcasted_iota(jnp.int32, (512, 128), 1)
    keep = 63 & ~(3 << (2 * pair))
    same_rest = (lane_in & keep) == (raw_out & keep)
    part_in = jnp.right_shift(raw_in, 6)
    part_out = jnp.right_shift(raw_out, 6)
    sign = jnp.where(part_out >= part_in, 1.0, -1.0).astype(F32)
    parts = [split_bf16(sup[layer, part]) for part in range(2)]
    for which, starts in enumerate(((0, 512), (1024,))):
        half = [
            lax.dot_general(expand_in, parts[p][which], dims, preferred_element_type=F32).astype(BF16)
            for p in range(2)
        ]
        for block in range(4):
            target = expand_out[block * 128 : (block + 1) * 128]
            real, imag = (
                lax.dot_general(h, target, dims, preferred_element_type=F32) for h in half
            )
            value = jnp.where(part_in == part_out, real, sign * imag)
            value = jnp.where(same_rest, value, 0.0).astype(BF16)
            for begin in starts:
                weights[begin : begin + 512, block * 128 : (block + 1) * 128] = value


def apply_pair(z, result, pair, ta, rv, xa, xb, weights):
    def bases_of(other):
        first = other * 4 if pair == 0 else other
        return [ta[first + (1 if pair == 0 else 4) * k] for k in range(4)]

    def split_rows(bases, xs, r, start):
        vregs = [rv[r], rv[r + 1]]
        for k in range(4):
            both = [z[tile_at(bases[k] + v), :] for v in vregs]
            high, low = split_bf16(jnp.concatenate(both, axis=0))
            rows = pl.ds(start, 16)
            xs[rows, k * 128 : (k + 1) * 128] = high
            xs[rows, 512 + k * 128 : 512 + (k + 1) * 128] = low
            xs[rows, 1024 + k * 128 : 1024 + (k + 1) * 128] = high

    first = bases_of(0)

    @pl.loop(0, 8)
    def _(i):
        for k in range(4):
            split_rows(first, xa, i * 8 + k * 2, pl.multiple_of(i * 64 + k * 16, 16))

    @pl.loop(0, 2)
    def _(i):
        for k, (xs, spare) in enumerate(((xa, xb), (xb, xa))):
            other = 2 * i + k
            following = bases_of(lax.rem(other + 1, 4))
            bases = bases_of(other)
            for r in range(0, 64, 2):
                split_rows(following, spare, r, 8 * r)
            for half in range(2):
                mixed = jnp.dot(
                    xs[...], weights[:, half * 256 : (half + 1) * 256], preferred_element_type=F32
                )
                for r in range(64):
                    v = rv[r]
                    for q in range(2):
                        result[tile_at(bases[2 * half + q] + v), :] = mixed[
                            8 * r : 8 * r + 8, q * 128 : (q + 1) * 128
                        ]


def channel(z, spare, ta, rv, xa, xb, weights):
    for pair, (source, result) in enumerate(((z, spare), (spare, z))):
        apply_pair(source, result, pair, ta, rv, xa, xb, weights[pair])


def trace_share(perm, where, sup, z, loc, outpos, final, order, tu, tc):
    column_order(perm, order)
    me = where[0]

    def place_of(bit):
        found = jnp.int32(0)
        for i in range(QUBITS):
            found = jnp.where(order[i] == bit, i, found)
        return found

    lane = lax.broadcasted_iota(jnp.int32, (16, 128), 1)
    group = jnp.zeros((16, 128), jnp.int32)
    for j in range(4):
        place = place_of(final[j])
        local = jnp.right_shift(lane, jnp.minimum(place, 5)) & 1
        remote_bit = jnp.right_shift(me, jnp.maximum(place - 6, 0)) & 1
        group = group + jnp.left_shift(jnp.where(place < 6, local, remote_bit), j)
    row16 = lax.broadcasted_iota(jnp.int32, (16, 16), 0)
    col16 = lax.broadcasted_iota(jnp.int32, (16, 16), 1)
    hot = jnp.where(lax.broadcasted_iota(jnp.int32, (16, 128), 0) == group, 1.0, 0.0).astype(F32)
    single = []
    for part in range(2):
        s = sup[1, part]
        tau = s[0:1] + s[5:6] + s[10:11] + s[15:16]
        both = []
        for pair in range(2):
            pick = 4 * (jnp.right_shift(row16, 2 * pair) & 3) + (jnp.right_shift(col16, 2 * pair) & 3)
            value = jnp.zeros((16, 16), F32)
            for uv in range(16):
                value = jnp.where(pick == uv, tau[:, uv : uv + 1], value)
            both.append(value)
        single.append(both)
    real = single[0][0] * single[0][1] - single[1][0] * single[1][1]
    imag = single[0][0] * single[1][1] + single[1][0] * single[0][1]
    exact = functools.partial(jnp.dot, precision=lax.Precision.HIGHEST, preferred_element_type=F32)
    weight = jnp.where(lane < 64, exact(real, hot), -exact(imag, hot))

    fill(tu, [one_shl(loc[final[j]]) for j in range(4)])

    def weight_of(bit):
        return jnp.where(outpos[bit] >= 4, one_shl(loc[bit]), 0)

    fill(tc, [weight_of(order[i]) for i in range(6)])
    base = jnp.int32(0)
    for i in range(6, QUBITS):
        base = base + weight_of(order[i]) * (jnp.right_shift(me, i - 6) & 1)
    lane1 = lax.broadcasted_iota(jnp.int32, (1, 128), 1) & 63
    sums = jnp.zeros((1, 128), F32)

    def column(c, rows):
        start = base + tc[c]
        return tuple(
            jnp.where(lane1 == c, z[pl.ds(start + tu[u], 1), :], rows[u]) for u in range(16)
        )

    rows = lax.fori_loop(0, 64, column, tuple(sums for _ in range(16)))
    for u in range(16):
        sums = sums + weight[u : u + 1] * rows[u]
    return sums


def middle(perm, slots, where, sup, x, w0, w1, out, rows_out, share, z, spare, xa, xb,
           final, outpos, loc, occ, rest, major, rv, order, tu, tc, out_of, low_from, low_to,
           high_from, high_to, places, enabled, *groups):
    me = where[0]
    for q in range(QUBITS):
        bit = perm[0, perm[1, q]]
        final[q] = bit
        outpos[bit] = jnp.int32(q)
        loc[q] = jnp.int32(q)
        occ[q] = jnp.int32(q)
    mixes = [perm[0, j] for j in range(4)]

    def mixed_bit(bit):
        found = bit == mixes[0]
        for m in mixes[1:]:
            found = found | (bit == m)
        return found

    everything = [jnp.int32(q) for q in range(QUBITS)]
    stays = lambda bit: outpos[bit] < 6
    best = lambda bit: jnp.logical_not(mixed_bit(bit)) & stays(bit)
    calm = lambda bit: jnp.logical_not(mixed_bit(bit))
    plenty = jnp.int32(0)
    for bit in everything:
        plenty = plenty + jnp.where(best(bit), 1, 0)
    good = lambda bit: jnp.where(plenty >= 3, best(bit), calm(bit))
    plan_sublanes(loc, occ, good, everything, places, enabled)
    mine = me * 8
    regroup(
        lambda row: x[tile_at(slots[jnp.right_shift(row, 3) ^ mine]), :], z, places, enabled, *groups
    )
    count = jnp.int32(0)
    for place in range(3, QUBITS):
        rest[count] = jnp.int32(place)
        count = count + jnp.where(mixed_bit(occ[place]), 0, 1)
    fill(major, [one_shl(loc[m]) for m in mixes])
    fill(rv, [one_shl(rest[j]) for j in range(6)])
    channel(z, spare, major, rv, xa, xb, (w0, w1))
    share[...] = trace_share(perm, where, sup, z, loc, outpos, final, order, tu, tc)
    plan_sublanes(loc, occ, stays, everything, places, enabled)

    @pl.when(enabled[0] + enabled[1] + enabled[2] > 0)
    def _():
        regroup(lambda row: z[tile_at(row), :], z, places, enabled, *groups)

    for s in range(3):
        rows_out[s] = outpos[occ[s]]
    count = jnp.int32(3)
    for q in range(6):
        rows_out[count] = jnp.int32(q)
        count = count + jnp.where(loc[final[q]] >= 3, 1, 0)
    for q in range(6, QUBITS):
        out_of[final[q]] = jnp.int32(8 << (q - 6))
    for s in range(3):
        out_of[occ[s]] = jnp.int32(0)
        out_of[final[rows_out[3 + s]]] = jnp.int32(1 << s)
    fill(low_from, [one_shl(3 + j) for j in range(5)])
    fill(high_from, [one_shl(8 + j) for j in range(5)])
    fill(low_to, [out_of[occ[3 + j]] for j in range(5)])
    fill(high_to, [out_of[occ[8 + j]] for j in range(5)])

    @pl.loop(0, 32)
    def _(i):
        origin, target = high_from[i], high_to[i]
        for j in range(32):
            out[tile_at(slots[(target + low_to[j]) ^ mine]), :] = z[tile_at(origin + 8 * j), :]


def gather_back(perm, slots, where, x, w0, w1, out, y, spare, xa, xb, ready, done,
                order, inv, loc, occ, ta, rv, origin, places, enabled, *groups):
    column_order(perm, order)
    for i in range(QUBITS):
        inv[order[i]] = jnp.int32(i)
    for q in range(QUBITS):
        place = inv[perm[0, perm[1, q]]]
        loc[q] = place
        occ[place] = jnp.int32(q)
    me = where[0]
    first_half = lax.broadcasted_iota(jnp.int32, (64, 128), 1) < 64

    @pl.loop(0, 16)
    def _(group):
        for q in range(4):
            p = group * 4 + q
            apart = (p ^ me) * 8
            tiles = [
                x[tile_at(slots[start + j]), :] for start in (apart, apart ^ 512) for j in range(PARTS)
            ]
            turned = jnp.concatenate(tiles, axis=0).T
            real, imag = turned[:64], turned[64:]
            start = pl.multiple_of(p * 64, 64)
            moved = pltpu.roll(jnp.where(first_half, imag, real), 64, 1)
            y[pl.ds(start, 64), :] = jnp.where(first_half, real, moved)
            y[pl.ds(start + 4096, 64), :] = jnp.where(first_half, moved, imag)

    for sub in range(3):
        inside = loc[4 + sub] < 3
        enabled[sub] = jnp.where(inside, 0, 1)
        places[sub] = loc[4 + sub]
    for sub in range(3):
        free = jnp.int32(0)
        for _ in range(3):
            taken = jnp.bool_(False)
            for k in range(3):
                taken = taken | ((enabled[k] == 0) & (places[k] == free))
                if k < sub:
                    taken = taken | ((enabled[k] == 1) & (origin[k] == free))
            free = free + jnp.where(taken, 1, 0)
        origin[sub] = jnp.where(enabled[sub] == 1, free, places[sub])
    leaving = [occ[origin[sub]] for sub in range(3)]
    for sub in range(3):

        @pl.when(enabled[sub] == 1)
        def _():
            loc[leaving[sub]] = places[sub]

        loc[4 + sub] = jnp.int32(sub)
    regroup(lambda row: y[tile_at(row), :], spare, places, enabled, *groups, origin=origin)
    fill(ta, [one_shl(loc[q]) for q in range(4)])
    fill(rv, [one_shl(loc[q]) for q in range(7, QUBITS)])
    channel(spare, y, ta, rv, xa, xb, (w0, w1))

    sublane = lax.broadcasted_iota(jnp.int32, (8, 128), 0)

    def leave(group):
        columns = pl.ds(pl.multiple_of(group * 512, 512), 512)
        return pltpu.make_async_copy(ready.at[:, :, columns], out.at[:, :, columns], done)

    @pl.loop(0, 16)
    def _(group):
        for q in range(4):
            t = group * 4 + q
            base = rv[t]
            tiles = [spare[tile_at(base + ta[b]), :] for b in range(16)]
            for k in range(3):
                step = 1 << k
                keep = (sublane & step) == 0
                for b in range(16):
                    if not b & step:
                        tiles[b], tiles[b + step] = swap_rows(
                            tiles[b], tiles[b + step], k, keep, jnp.logical_not(keep)
                        )
            ordered = [tiles[8 * (v % 2) + v // 2] for v in range(16)]
            columns = pl.ds(pl.multiple_of(t * 128, 128), 128)
            turned = jnp.concatenate(ordered, axis=0).T
            ready[0, :, columns] = turned[:64]
            ready[1, :, columns] = turned[64:]

        @pl.when(group > 0)
        def _():
            leave(group - 1).start()

    leave(15).start()
    pltpu.make_async_copy(ready, out, done).wait()


LINKS = 6
PARTS = 8


def part_links(part):
    return [(t, (part + t) % 8) for t in range(8) if (part + t) % 8 < LINKS]


def slot_table():
    low_high = ((4, 5), (6, 0), (2, 3))
    table = np.zeros((PARTS, 128), np.int32)
    for part in range(PARTS):
        place = {link: 1 << (5 - s) for s, (_, link) in enumerate(part_links(part))}
        weight = [0] * 7
        weight[1] = 512
        for axis, (low, high) in enumerate(low_high):
            weight[low] = place[2 * axis]
            weight[high] = place[2 * axis] | place[2 * axis + 1]
        for device in range(128):
            for bit in range(7):
                if device >> bit & 1:
                    table[part, device] ^= weight[bit]
        table[part] += 64 * part
    return 8 * table.T.reshape(-1)


def swap_all(with_sum, *refs):
    if with_sum:
        x, lanes, sup, mine, out, w0, w1, total, shares, share_send, share_recv, *refs = refs
    else:
        x, lanes, sup, out, w0, w1, *refs = refs
    held, (send, recv, first_send, first_recv, out_sem) = refs[:6], refs[6:]
    hi = lax.axis_index("hi")
    grp = lax.axis_index("grp")
    bits = [lax.rem(hi // (1 << k), 2) for k in range(6)]

    def flip(k):
        return (1 - 2 * bits[k]) * (1 << k)

    core = {"hi": hi + flip(0), "grp": grp}
    link_device = [
        {"hi": hi + flip(3), "grp": grp},
        {"hi": hi + flip(3) + flip(4), "grp": grp},
        {"hi": hi + flip(5), "grp": grp},
        {"hi": hi + flip(5), "grp": 1 - grp},
        {"hi": hi + flip(1), "grp": grp},
        {"hi": hi + flip(1) + flip(2), "grp": grp},
    ]
    mesh_ids = pl.DeviceIdType.MESH
    barrier = pltpu.get_barrier_semaphore()
    for device in [core] + link_device:
        pl.semaphore_signal(barrier, inc=1, device_id=device, device_id_type=mesh_ids)
    pl.semaphore_wait(barrier, 7)

    def remote(src, dst, send_sem, recv_sem, device):
        return pltpu.make_async_remote_copy(
            src_ref=src, dst_ref=dst, send_sem=send_sem, recv_sem=recv_sem,
            device_id=device, device_id_type=mesh_ids,
        )

    for p in range(PARTS):
        remote(x.at[1, p], held[0].at[p], first_send.at[p], first_recv.at[p], core).start()

    def drained(ref, sem):
        pltpu.make_async_copy(ref, ref, sem).wait()

    def stage(h, p, s, index=()):
        if s == 0:
            return x.at[(0, p) + index] if h == 0 else held[0].at[(p,) + index]
        return held[s].at[(h, p) + index]

    def landed(h, p):
        return out.at[(h, p) + (slice(None),) * 5 + (1,)]

    def arrived(h, p, s):
        if s:
            drained(stage(h, p, s) if s < 6 else landed(h, p), recv.at[h, p, s - 1])
        elif h:
            drained(stage(h, p, 0), first_recv.at[p])

    def pick(s, chosen):
        return tuple(chosen[b] for b in range(1, 7) if b != s)

    def cross(h, p, s, link):
        for j in range(s):
            source = {b: slice(None) for b in range(1, 7)}
            for b in range(j + 1, s):
                source[b] = 0
            source[s] = 1
            target = dict(source)
            if j:
                target[j] = 1
            place = (h, p) + pick(s, target)
            remote(
                stage(h, p, j, pick(j, source)), held[s].at[place] if s < 6 else out.at[place + (1,)],
                send.at[h, p, s - 1], recv.at[h, p, s - 1], link_device[link],
            ).start()

    def deliver(h, p):
        for j in range(6):
            source = {b: slice(None) if b < j else 0 for b in range(1, 7)}
            target = dict(source)
            if j:
                target[j] = 1
            pltpu.make_async_copy(
                stage(h, p, j, pick(j, source)),
                out.at[(h, p) + tuple(target[b] for b in range(1, 7))],
                out_sem.at[h, p],
            ).start()

    done = {p: 0 for p in range(PARTS)}
    if with_sum:
        own = pltpu.make_async_copy(mine, shares.at[0], share_recv.at[7])
        own.start()
        own.wait()

        def double(k):
            return remote(
                shares.at[0 : 1 << k], shares.at[1 << k : 2 << k], share_send.at[k],
                share_recv.at[k], ([core] + link_device)[k],
            )

    for t in range(8):
        for h in range(2):
            for p in range(PARTS):
                link = (p + t) % 8
                if link < LINKS:
                    arrived(h, p, done[p])
                    cross(h, p, done[p] + 1, link)
                    if done[p] == 5:
                        deliver(h, p)

        if t < 2:
            build_weights(
                sup, int(with_sum), t, not with_sum, None if t else lanes, w1 if t else w0
            )
        if with_sum and t < 7:
            if t:
                double(t - 1).wait()
            double(t).start()
        for p in range(PARTS):
            if (p + t) % 8 < LINKS:
                done[p] += 1

    for h in range(2):
        for p in range(PARTS):
            arrived(h, p, 6)

    if with_sum:
        double(6).wait()
        grand = jnp.sum(shares[...], axis=0)
        total[...] = jnp.sum(grand, axis=1, keepdims=True) / ROWS

    for p in range(PARTS):
        drained(x.at[1, p], first_send.at[p])
    for h in range(2):
        for p in range(PARTS):
            for s in range(1, 7):
                drained(landed(h, p), send.at[h, p, s - 1])
            drained(out.at[h, p, 0], out_sem.at[h, p])


def exchange(value, collective_id, lanes, sup, share=None):
    two = (2,) * 6
    whole = jax.ShapeDtypeStruct((2, PARTS) + two + (8, 128), F32)
    dma = pltpu.SemaphoreType.DMA
    anywhere = pl.BlockSpec(memory_space=pltpu.HBM)
    vmem = pl.BlockSpec(memory_space=VMEM)
    extra = share is not None
    scratch = [VMEM((PARTS,) + two + (8, 128), F32)]
    scratch += [VMEM((2, PARTS) + two[:5] + (8, 128), F32) for _ in range(5)]
    scratch += [dma((2, PARTS, 6)), dma((2, PARTS, 6)), dma((PARTS,)), dma((PARTS,)), dma((2, PARTS))]
    if extra:
        scratch = [VMEM((128, 1, 128), F32), dma((7,)), dma((8,))] + scratch
    matrix = jax.ShapeDtypeStruct((1536, 512), BF16)
    smem = pl.BlockSpec(memory_space=SMEM)
    outs = (whole, matrix, matrix) + ((jax.ShapeDtypeStruct((1, 1), F32),) if extra else ())
    result = pl.pallas_call(
        functools.partial(swap_all, extra),
        out_shape=outs,
        in_specs=[anywhere, smem, vmem] + [anywhere] * extra,
        out_specs=(anywhere, vmem, vmem) + (vmem,) * extra,
        scratch_shapes=scratch,
        compiler_params=pltpu.CompilerParams(
            collective_id=collective_id, has_side_effects=True, vmem_limit_bytes=24 * 2**20
        ),
    )(value.reshape(whole.shape), lanes, sup, *((share,) if extra else ()))
    return result[0].reshape(8192, 128), *result[1:]


def call(body, outs, out_smem, n_smem, n_args, scratch, args, out_space=VMEM):
    smem = pl.BlockSpec(memory_space=SMEM)
    vmem = pl.BlockSpec(memory_space=VMEM)
    return pl.pallas_call(
        body,
        out_shape=outs,
        in_specs=[smem if i < n_smem else vmem for i in range(n_args)],
        out_specs=tuple(
            smem if i in out_smem else pl.BlockSpec(memory_space=out_space) for i in range(len(outs))
        ),
        scratch_shapes=scratch,
        compiler_params=pltpu.CompilerParams(vmem_limit_bytes=26 * 2**20),
    )(*args)


def table(*sizes):
    return [SMEM((n,), jnp.int32) for n in sizes]


FULL = VMEM((8192, 128), F32)
GROUPS = (3, 3, 14, 8, 16)
MAP = jax.ShapeDtypeStruct((8,), jnp.int32)
WORK = [FULL, VMEM((512, 1536), BF16), VMEM((512, 1536), BF16)]


def spread_call(perm, slots, where, x):
    return call(
        spread, (jax.ShapeDtypeStruct((8192, 128), F32), MAP), (1,), 3, 4,
        [FULL, FULL] + table(14, 14, 14, 8, 64, *GROUPS), (perm, slots, where, x),
    )


def middle_call(perm, slots, where, sup, x, w0, w1):
    return call(
        middle,
        (jax.ShapeDtypeStruct((8192, 128), F32), MAP, jax.ShapeDtypeStruct((1, 128), F32)),
        (1,), 3, 7,
        [FULL] + WORK + table(13, 13, 13, 13, 14, 16, 64, 14, 16, 64, 13, 32, 32, 32, 32, *GROUPS),
        (perm, slots, where, sup, x, w0, w1),
    )


def back_call(perm, slots, where, x, w0, w1):
    return call(
        gather_back, (jax.ShapeDtypeStruct((2, 64, 8192), F32),), (), 3, 6,
        [FULL] + WORK + [VMEM((2, 64, 8192), F32), pltpu.SemaphoreType.DMA]
        + table(14, 13, 13, 13, 16, 64, 3, *GROUPS),
        (perm, slots, where, x, w0, w1), out_space=pltpu.HBM,
    )[0]


def per_device(rho, perm, superop):
    slots = jnp.asarray(slot_table())
    where = lax.axis_index(HI_GRP).astype(jnp.int32).reshape(1)
    sent, lanes = spread_call(perm, slots, where, rho)
    first = exchange(sent, 0, lanes, superop)
    mid, rows, share = middle_call(perm, slots, where, superop, *first)
    *last, total = exchange(mid, 1, rows, superop, share)
    return back_call(perm, slots, where, *last), total.reshape(())


def solution(mesh):
    in_specs = (P(None, HI_GRP, None), P(), P())
    out_specs = (P(None, HI_GRP, None), P())
    return jax.shard_map(
        per_device, mesh=mesh, in_specs=in_specs, out_specs=out_specs, check_vma=False
    )
```
